256 devices in a mesh: rep: 2 (over core), dp: 128 (over x, y, z).
Axes of the slice: x: 4, y: 4, z: 8, core: 2. Of those that a mesh axis runs over, the one named last changes fastest.
Arguments:
- g_w_gate: bfloat16 [256, 2, 512, 1408], P(('rep', 'dp')), parts along dimension 0
- g_w_up: bfloat16 [256, 2, 512, 1408], P(('rep', 'dp')), parts along dimension 0
- g_w_down: bfloat16 [256, 2, 1408, 512], P(('rep', 'dp')), parts along dimension 0
- w_gate: bfloat16 [2, 512, 1408], replicated
- w_up: bfloat16 [2, 512, 1408], replicated
- w_down: bfloat16 [2, 1408, 512], replicated
- m_w_gate: float32 [2, 512, 1408], P(None, 'dp')
- m_w_up: float32 [2, 512, 1408], P(None, 'dp')
- m_w_down: float32 [2, 1408, 512], P(None, 'dp')
- v_w_gate: float32 [2, 512, 1408], P(None, 'dp')
- v_w_up: float32 [2, 512, 1408], P(None, 'dp')
- v_w_down: float32 [2, 1408, 512], P(None, 'dp')
Outputs:
- output 1: bfloat16 [4, 512, 1408], P('rep'), parts along dimension 0
- output 2: bfloat16 [4, 512, 1408], P('rep'), parts along dimension 0
- output 3: bfloat16 [4, 1408, 512], P('rep'), parts along dimension 0
- output 4: float32 [4, 512, 1408], P('rep', 'dp'), parts along dimension 0
- output 5: float32 [4, 512, 1408], P('rep', 'dp'), parts along dimension 0
- output 6: float32 [4, 1408, 512], P('rep', 'dp'), parts along dimension 0
- output 7: float32 [4, 512, 1408], P('rep', 'dp'), parts along dimension 0
- output 8: float32 [4, 512, 1408], P('rep', 'dp'), parts along dimension 0
- output 9: float32 [4, 1408, 512], P('rep', 'dp'), parts along dimension 0
There are 2 independent parts. The reference program is written for one: setup_inputs(seed, part) draws one part's arguments, and reference() takes and returns one part's arrays. A program takes and returns all parts, laid end to end along the dimension named above; an argument that names none is the same for every part.
All inputs are finite; a program needn't handle non-finite values.
Results may differ from the reference program's by a relative error of at most 0.022.
Values are sent between devices in bfloat16 or wider.
A program may use at most 768 MiB of HBM per device.

```python
import jax
import jax.numpy as jnp
from jax import lax

DEVICES = 128
D = 512
FF = 1408
LAYERS = 2
NAMES = ("w_gate", "w_up", "w_down")
SHAPES = {"w_gate": (LAYERS, D, FF), "w_up": (LAYERS, D, FF), "w_down": (LAYERS, FF, D)}


def setup_inputs(seed: int = 0, part: int = 0) -> dict:
    kz, *keys = jax.random.split(jax.random.key(seed), 1 + 5 * len(NAMES))
    loud = 2.0 ** jax.random.uniform(kz, (), jnp.float32, -1.0, 1.0)
    drawn = {}
    for name, key, both in zip(NAMES, keys[:3], keys[3:6], strict=True):
        own = jax.random.normal(jax.random.fold_in(key, part), (DEVICES, *SHAPES[name]), jnp.float32)
        shared = jax.random.normal(jax.random.fold_in(both, part), SHAPES[name], jnp.float32)
        drawn["g_" + name] = (loud * (0.7 * shared / DEVICES + 0.7 * own * DEVICES**-0.5)).astype(jnp.bfloat16)
    for name, key in zip(NAMES, keys[6:9], strict=True):
        drawn[name] = (jax.random.normal(key, SHAPES[name], jnp.float32) * SHAPES[name][1] ** -0.5).astype(jnp.bfloat16)
    for name, key in zip(NAMES, keys[9:12], strict=True):
        drawn["m_" + name] = loud * 0.5 * jax.random.normal(key, SHAPES[name], jnp.float32)
    for name, key in zip(NAMES, keys[12:15], strict=True):
        drawn["v_" + name] = loud * loud * jax.random.uniform(key, SHAPES[name], jnp.float32, 0.5, 1.5)
    return drawn


def adamw(w, m, v, g):
    m = 0.9 * m + 0.1 * g
    v = 0.95 * v + 0.05 * g * g
    step = m * lax.rsqrt(v + 1e-8) + 0.1 * w
    return (w - 0.02 * step).astype(jnp.bfloat16), m, v


def clipped(gradients, sum_of_squares, count):
    factor = jnp.minimum(1.0, 0.5 * lax.rsqrt(sum_of_squares / count + 1e-30))
    return [g * factor for g in gradients]


def reference(g_w_gate, g_w_up, g_w_down, w_gate, w_up, w_down, m_w_gate, m_w_up, m_w_down, v_w_gate, v_w_up, v_w_down):
    def total(terms):
        return lax.scan(lambda so_far, term: (so_far + term.astype(jnp.float32), None), jnp.zeros(terms.shape[1:], jnp.float32), terms)[0]

    gradients = [total(terms).astype(jnp.bfloat16).astype(jnp.float32) for terms in (g_w_gate, g_w_up, g_w_down)]
    gradients = clipped(gradients, sum(jnp.sum(g * g) for g in gradients), sum(g.size for g in gradients))
    new = [
        adamw(w.astype(jnp.float32), m, v, g)
        for w, m, v, g in zip((w_gate, w_up, w_down), (m_w_gate, m_w_up, m_w_down), (v_w_gate, v_w_up, v_w_down), gradients, strict=True)
    ]
    return tuple(one[which] for which in range(3) for one in new)
```

```python
import functools

import jax
import jax.numpy as jnp
from jax import lax
from jax.experimental import pallas as pl
from jax.experimental.pallas import tpu as pltpu
from jax.sharding import PartitionSpec as P

X, Y, Z = 4, 4, 8
F = 1408
COUNT = 3 * 2 * 512 * F
SEMS = 256
LOADS = 32
f32, bf16 = jnp.float32, jnp.bfloat16
BOTH = (0, 1)
WAYS = (1, -1)
LONG = ((0, 1), (1, -1))
SHORT = ((1, 1), (0, -1))


def chains(n):
    return [(*one, n // 2) for one in LONG] + [(*one, n // 2 - 1) for one in SHORT]


def slots(n):
    return {key: i for i, key in enumerate((h, s, t) for h, s, length in chains(n) for t in range(1, length + 1))}


def sixteen(i):
    return pl.ds(pl.multiple_of(i * 16, 16), 16)


def loop(n, body):
    def step(i, carry):
        body(i)
        return carry

    lax.fori_loop(0, n, step, 0)


def kernel(gg, gu, gd, wg, wu, wd, mg, mu, md, vg, vu, vd, *rest):
    (og, ou, od, omg, omu, omd, ovg, ovu, ovd) = rest[:9]
    (G, GD, L1, F1, B1, L2, F2, ZS, ZF, ZL, LZ, FD, BD, LDX, DS, YS, YF, YL, NS, NL, WG, WD, WZ, YW, ssem, rsem, lsem, osem) = rest[9:]
    d = lax.axis_index("dp")
    x, y, z = d // 32, (d // 8) % 4, d % 8
    place = {"x": (x, 4), "y": (y, 4), "z": (z, 8)}

    def at(axis, k):
        p, n = place[axis]
        return lax.rem(p + (k + n) % n, n)

    def device(axis, k):
        p = at(axis, k)
        return {"dp": {"x": p * 32 + y * 8 + z, "y": x * 32 + p * 8 + z, "z": x * 32 + y * 8 + p}[axis]}

    used = [0]
    pending = []

    def send(src, dst, axis, k):
        i = used[0]
        used[0] += 1
        copy = pltpu.make_async_remote_copy(
            src_ref=src, dst_ref=dst, send_sem=ssem.at[i], recv_sem=rsem.at[i],
            device_id=device(axis, k), device_id_type=pl.DeviceIdType.MESH,
        )
        copy.start()
        pending.append(copy)
        return copy

    loads = {}

    def load(key, src, dst):
        copy = pltpu.make_async_copy(src, dst, lsem.at[len(loads)])
        copy.start()
        loads[key] = copy

    stores = []

    def store(src, dst):
        copy = pltpu.make_async_copy(src, dst, osem.at[len(stores)])
        copy.start()
        stores.append(copy)

    class Scatter:
        def __init__(self, axis, own, landing, add, need=None):
            self.axis, self.own, self.landing, self.add, self.need = axis, own, landing, add, need
            self.n = place[axis][1]
            self.length = {(h, s): length for h, s, length in chains(self.n)}
            self.slot = slots(self.n)
            self.copies = {}

        def at(self, h, s, t):
            return self.landing.at[self.slot[h, s, t]]

        def first(self, h, s):
            k = s * self.length[h, s]
            if self.need:
                self.need(h, k)
            self.copies[h, s, 1] = send(self.own(h, k), self.at(h, s, 1), self.axis, s)

        def start(self):
            for h, s, _ in chains(self.n):
                self.first(h, s)

        def arrive(self, h, s, t):
            self.copies[h, s, t].wait_recv()
            if t < self.length[h, s]:
                k = s * (self.length[h, s] - t)
                if self.need:
                    self.need(h, k)
                self.add(self.at(h, s, t), h, k)
                self.copies[h, s, t + 1] = send(self.at(h, s, t), self.at(h, s, t + 1), self.axis, s)

        def last(self, h):
            for s in WAYS:
                self.arrive(h, s, self.length[h, s])
            return [self.at(h, s, self.length[h, s]) for s in WAYS]

    class Gather:
        def __init__(self, axis, part):
            self.axis, self.part = axis, part
            self.n = place[axis][1]
            self.length = {(h, s): length for h, s, length in chains(self.n)}
            self.copies = {}

        def push(self, h, s, t):
            ref = self.part(h, -s * (t - 1))
            self.copies[h, s, t] = send(ref, ref, self.axis, s)

        def start(self):
            for h, s, _ in chains(self.n):
                self.push(h, s, 1)

        def arrive(self, h, s, t):
            self.copies[h, s, t].wait_recv()
            if t < self.length[h, s]:
                self.push(h, s, t + 1)
            return -s * t

    def load_wide(f, h, k):
        if f == 0:
            load((f, h, k), (gg, gu)[h].at[0, at("x", k)], G.at[h, 0, at("x", k)])
        else:
            load((f, h, k), (gg, gu)[h].at[1, :, at("y", k)], G.at[h, 1, :, at("y", k)])

    def load_down(h, k):
        load((2, h, k % 8), gd.at[h, at("z", k)], GD.at[h, at("z", k)])

    for f in BOTH:
        for h in BOTH:
            load_wide(f, h, 2)
    for h in BOTH:
        load_down(h, 4)
    for f in BOTH:
        for h, k in ((1, 1), (0, 3)):
            load_wide(f, h, k)
    for h, k in ((1, 3), (0, 5), (0, 3), (1, 5), (1, 2), (0, 6), (0, 2), (1, 6)):
        load_down(h, k)
    for f in BOTH:
        for h, k in ((0, 1), (1, 3)):
            load_wide(f, h, k)
    for h, k in ((0, 1), (1, 7), (1, 1), (0, 7)):
        load_down(h, k)
    for f in BOTH:
        for h in BOTH:
            load_wide(f, h, 0)
    for h in BOTH:
        load_down(h, 0)
    ready = set()

    def need(f, n):
        def wait(h, k):
            key = (f, h, k % n)
            if key not in ready:
                ready.add(key)
                loads[key].wait()

        return wait

    partners = [(a, k) for a, n in (("x", 4), ("y", 4), ("z", 8)) for k in range(1, n)]
    barrier = pltpu.get_barrier_semaphore()
    for a, k in partners:
        pl.semaphore_signal(barrier, inc=1, device_id=device(a, k), device_id_type=pl.DeviceIdType.MESH)
    pl.semaphore_wait(barrier, len(partners))

    def wide(f):
        def own(h, k):
            return G.at[h, 0, at("x", k)] if f == 0 else G.at[h, 1, :, at("y", k)]

        return own

    def add_wide(f):
        def add(got, h, k):
            own = wide(f)(h, k)

            def body(i):
                rows = (i // 2, sixteen(i % 2))
                got[rows] = (got[rows].astype(f32) + own[rows].astype(f32)).astype(bf16)

            loop(8, body)

        return add

    def add_down(got, h, k):
        own = GD.at[h, at("z", k)]

        def body(i):
            got[i] = (got[i].astype(f32) + own[i].astype(f32)).astype(bf16)

        loop(4, body)

    first = [Scatter("xy"[f], wide(f), L1.at[f], add_wide(f), need(f, 4)) for f in BOTH]
    down = Scatter("z", lambda h, k: GD.at[h, at("z", k)], LZ, add_down, need(2, 8))

    def end_wide(f, h):
        a, b = first[f].last(h)
        need(f, 4)(h, 0)
        own = wide(f)(h, 0)

        def body(i):
            rows = (i // 2, sixteen(i % 2))
            total = own[rows].astype(f32) + a[rows].astype(f32) + b[rows].astype(f32)
            F1[(f, h, *rows)] = total
            B1[(f, h, *rows)] = total.astype(bf16)

        loop(8, body)

    def end_down(h):
        a, b = down.last(h)
        need(2, 8)(h, 0)
        own = GD.at[h, at("z", 0)]

        def body(i):
            total = own[i].astype(f32) + a[i].astype(f32) + b[i].astype(f32)
            FD[h, i] = total
            BD[h, i] = total.astype(bf16)

        loop(4, body)

    def add_second(f):
        axis = "yx"[f]

        def add(got, h, k):
            own = F1.at[f, h, at(axis, k)]

            def body(i):
                rows = (sixteen(i),)
                got[rows] = (got[rows].astype(f32) + own[rows]).astype(bf16)

            loop(2, body)

        return add

    def second_own(f):
        axis = "yx"[f]
        return lambda h, k: B1.at[f, h, at(axis, k)]

    def add_down_second(got, h, k):
        got[...] = (got[...].astype(f32) + FD[h, at("x", k)]).astype(bf16)

    second = [Scatter("yx"[f], second_own(f), L2.at[f], add_second(f)) for f in BOTH]
    down_second = Scatter("x", lambda h, k: BD.at[h, at("x", k)], LDX, add_down_second)

    def end_second(f, h):
        a, b = second[f].last(h)
        own = F1.at[f, h, at("yx"[f], 0)]

        def body(i):
            rows = (sixteen(i),)
            F2[(f, h, *rows)] = own[rows] + a[rows].astype(f32) + b[rows].astype(f32)

        loop(2, body)

    def arrive_pair(ring, t, short=False):
        for h, s in SHORT if short else LONG:
            ring.arrive(h, s, t)

    for f in BOTH:
        for h, s in LONG:
            first[f].first(h, s)
    for h, s in LONG:
        down.first(h, s)
    for f in BOTH:
        for h, s in SHORT:
            first[f].first(h, s)
    for h, s in SHORT:
        down.first(h, s)
    arrive_pair(down, 1)
    arrive_pair(down, 1, True)
    arrive_pair(first[0], 1)
    arrive_pair(first[1], 1)
    arrive_pair(down, 2)
    arrive_pair(down, 2, True)
    arrive_pair(down, 3)
    for f in BOTH:
        for h in BOTH:
            end_wide(f, h)
        second[f].start()
    for h in BOTH:
        end_down(h)
    down_second.start()
    for f in BOTH:
        arrive_pair(second[f], 1)
    arrive_pair(down_second, 1)
    for f in BOTH:
        for h in BOTH:
            end_second(f, h)

    for h in BOTH:
        for j in range(4):
            t0, t1 = (F2[f, h, 8 * j : 8 * j + 8, :] for f in BOTH)
            for i, block in enumerate((jnp.concatenate([t0[:4], t1[:4]], 0), jnp.concatenate([t0[4:], t1[4:]], 0))):
                ZF[2 * j + i, h] = block
                ZS[2 * j + i, h] = block.astype(bf16)
    far = (4, 3, 5, 2, 6, 1, 7)
    third = {k: send(ZS.at[at("z", k)], ZL.at[k], "z", k) for k in far}

    for h in BOTH:
        a, b = down_second.last(h)
        DS[h, :88] = FD[h, at("x", 0)] + a[...].astype(f32) + b[...].astype(f32)
        DS[h, 88:] = jnp.zeros((8, 256), f32)
        for j in range(4):
            block = DS[h, 22 * j : 22 * j + 24, :]
            YF[j, h] = block
            YS[j, h] = block.astype(bf16)
    third_down = {k: send(YS.at[at("y", k)], YL.at[k], "y", k) for k in (2, 1, 3)}

    for k in (1, 3, 2):
        third_down[k].wait_recv()
    real = lax.broadcasted_iota(jnp.int32, (24, 256), 0) < 22
    squares = jnp.zeros((), f32)
    g_down = []
    for h in BOTH:
        total = YF[y, h]
        for k in (1, 2, 3):
            total = total + YL[k, h].astype(f32)
        total = jnp.where(real, total, 0.0).astype(bf16).astype(f32)
        g_down.append(total)
        squares += jnp.sum(total * total)
    for k in reversed(far):
        third[k].wait_recv()
    g_wide = []
    for h in BOTH:
        total = ZF[z, h]
        for k in range(1, 8):
            total = total + ZL[k, h].astype(f32)
        total = total.astype(bf16).astype(f32)
        g_wide.append(total)
        squares += jnp.sum(total * total)

    total = jnp.full((8, 128), squares, f32)
    for i, (a, n) in enumerate((("x", 4), ("y", 4), ("z", 8))):
        NS[i] = total
        copies = [send(NS.at[i], NL.at[i, k], a, k) for k in range(1, n)]
        for copy in copies:
            copy.wait_recv()
        for k in range(1, n):
            total = total + NL[i, k]
    factor = jnp.minimum(1.0, 0.5 * lax.rsqrt(total / COUNT + 1e-30))[0:1, 0:1]

    def adamw(w, m, v, g):
        m = 0.9 * m + 0.1 * g
        v = 0.95 * v + 0.05 * g * g
        return (w - 0.02 * (m * lax.rsqrt(v + 1e-8) + 0.1 * w)).astype(bf16), m, v

    for h, (w_, m_, v_, om, ov) in enumerate(((wg, mg, vg, omg, ovg), (wu, mu, vu, omu, ovu))):
        w, m, v = (jnp.concatenate([r[0].astype(f32), r[1].astype(f32)], 0) for r in (w_, m_, v_))
        w, m, v = adamw(w, m, v, g_wide[h] * factor)
        WZ[z, h] = w
        for layer in BOTH:
            om[layer] = m[4 * layer : 4 * layer + 4]
            ov[layer] = v[4 * layer : 4 * layer + 4]
    g = jnp.concatenate(g_down, 1) * factor
    for h in BOTH:
        DS[h, :24] = jnp.zeros((24, 256), f32)
    for layer in BOTH:
        w, m, v = adamw(wd[layer].astype(f32), md[layer], vd[layer], g[11 * layer : 11 * layer + 11])
        omd[layer], ovd[layer] = m, v
        for h in BOTH:
            DS[h, 11 * layer : 11 * layer + 11, :] = w[:, 256 * h : 256 * h + 256].astype(f32)
    for h in BOTH:
        YW[y, h] = DS[h, :24].astype(bf16)

    wide_z = {k: send(WZ.at[z], WZ.at[z], "z", k) for k in far}
    down_y = {k: send(YW.at[y], YW.at[y], "y", k) for k in (2, 1, 3)}
    for k in (1, 3, 2):
        down_y[k].wait_recv()
    for h in BOTH:
        for j in range(4):
            DS[h, 22 * j : 22 * j + 24, :] = YW[j, h].astype(f32)
        WD[h, z, x] = DS[h, :88].astype(bf16)
    down_x = Gather("x", lambda h, k: WD.at[h, z, at("x", k)])
    down_x.start()
    for k in reversed(far):
        wide_z[k].wait_recv()
    for h in BOTH:
        for layer in BOTH:
            rows = slice(4 * layer, 4 * layer + 4)
            for j in range(2):
                parts = [WZ[4 * j + i, h].astype(f32)[rows] for i in range(4)]
                WG[h, layer, x, y, 16 * j : 16 * j + 16, :] = jnp.concatenate(parts, 0).astype(bf16)
    near = [Gather("y", lambda h, k: WG.at[h, 0, x, at("y", k)]), Gather("x", lambda h, k: WG.at[h, 1, at("x", k), y])]
    for ring in near:
        ring.start()
    arrive_pair(down_x, 1)
    arrive_pair(down_x, 1, True)
    arrive_pair(down_x, 2)
    down_z = Gather("z", lambda h, k: WD.at[h, at("z", k)])
    down_z.start()

    def put_wide(f, h, k):
        out = (og, ou)[h]
        if f == 0:
            store(WG.at[h, 0, at("x", k)], out.at[0, at("x", k)])
        else:
            store(WG.at[h, 1, :, at("y", k)], out.at[1, :, at("y", k)])

    def put_down(h, k):
        store(WD.at[h, at("z", k)], od.at[h, at("z", k)])

    for ring in near:
        arrive_pair(ring, 1)
    for ring in near:
        arrive_pair(ring, 1, True)
    far_rings = [Gather("x", lambda h, k: WG.at[h, 0, at("x", k)]), Gather("y", lambda h, k: WG.at[h, 1, :, at("y", k)])]
    for f in BOTH:
        arrive_pair(near[f], 2)
        far_rings[f].start()
    for h in BOTH:
        put_down(h, 0)
        for f in BOTH:
            put_wide(f, h, 0)

    def down_arrive(t, short=False):
        for h, s in SHORT if short else LONG:
            put_down(h, down_z.arrive(h, s, t))

    def wide_arrive(t, short=False):
        for f in BOTH:
            for h, s in SHORT if short else LONG:
                put_wide(f, h, far_rings[f].arrive(h, s, t))

    down_arrive(1)
    down_arrive(1, True)
    down_arrive(2)
    wide_arrive(1)
    down_arrive(2, True)
    down_arrive(3)
    wide_arrive(1, True)
    down_arrive(3, True)
    down_arrive(4)
    wide_arrive(2)
    for copy in pending:
        copy.wait_send()
    for copy in stores:
        copy.wait()


def step_kernel(*args):
    hbm, vmem = pl.BlockSpec(memory_space=pl.ANY), pl.BlockSpec(memory_space=pltpu.VMEM)
    wide, deep = (2, 4, F), (2, 11, 512)
    unit, half = (4, 32, F), (4, 88, 256)
    pair, square, whole_down = (2, 2), (4, *unit), (2, 8, *half)
    blocks, small, tile = (8, 2, 8, F), (4, 2, 24, 256), (8, 128)
    shape = jax.ShapeDtypeStruct
    return pl.pallas_call(
        kernel,
        out_shape=(
            shape((2, *square), bf16), shape((2, *square), bf16), shape(whole_down, bf16),
            shape(wide, f32), shape(wide, f32), shape(deep, f32), shape(wide, f32), shape(wide, f32), shape(deep, f32),
        ),
        in_specs=[hbm] * 3 + [vmem] * 9,
        out_specs=(hbm,) * 3 + (vmem,) * 6,
        scratch_shapes=[
            pltpu.VMEM((*pair, *square), bf16),
            pltpu.VMEM(whole_down, bf16),
            pltpu.VMEM((2, 6, *unit), bf16),
            pltpu.VMEM((*pair, *unit), f32),
            pltpu.VMEM((*pair, *unit), bf16),
            pltpu.VMEM((2, 6, *unit[1:]), bf16),
            pltpu.VMEM((*pair, *unit[1:]), f32),
            pltpu.VMEM(blocks, bf16),
            pltpu.VMEM(blocks, f32),
            pltpu.VMEM(blocks, bf16),
            pltpu.VMEM((14, *half), bf16),
            pltpu.VMEM((2, *half), f32),
            pltpu.VMEM((2, *half), bf16),
            pltpu.VMEM((6, *half[1:]), bf16),
            pltpu.VMEM((2, 96, 256), f32),
            pltpu.VMEM(small, bf16),
            pltpu.VMEM(small, f32),
            pltpu.VMEM(small, bf16),
            pltpu.VMEM((3, *tile), f32),
            pltpu.VMEM((3, 8, *tile), f32),
            pltpu.VMEM((*pair, *square), bf16),
            pltpu.VMEM(whole_down, bf16),
            pltpu.VMEM(blocks, bf16),
            pltpu.VMEM(small, bf16),
            pltpu.SemaphoreType.DMA((SEMS,)),
            pltpu.SemaphoreType.DMA((SEMS,)),
            pltpu.SemaphoreType.DMA((LOADS,)),
            pltpu.SemaphoreType.DMA((LOADS,)),
        ],
        compiler_params=pltpu.CompilerParams(collective_id=0, has_side_effects=True, vmem_limit_bytes=60 * 2**20),
        name="clipped_step",
    )(*args)


def solution(mesh):
    def step(gg, gu, gd, wg, wu, wd, *moments):
        gg, gu = (g.reshape(2, 4, 4, 32, F) for g in (gg, gu))
        gd = gd.reshape(2, 4, 4, 8, 11, 2, 256).transpose(5, 3, 1, 2, 0, 4, 6).reshape(2, 8, 4, 88, 256)
        me = lax.axis_index("dp")
        own = [lax.dynamic_slice_in_dim(w, me * n, n, 1) for w, n in ((wg, 4), (wu, 4), (wd, 11))]
        og, ou, od, *rest = step_kernel(gg, gu, gd, *own, *moments)
        og, ou = (o.reshape(2, 512, F) for o in (og, ou))
        od = od.reshape(2, 8, 4, 4, 2, 11, 256).transpose(4, 2, 3, 1, 5, 0, 6).reshape(2, F, 512)
        return (og, ou, od, *rest)

    all_of, cut = P(None, None, None), P(None, "dp", None)
    return jax.shard_map(
        step,
        mesh=mesh,
        in_specs=(P(("rep", "dp"), None, None, None),) * 3 + (all_of,) * 3 + (cut,) * 6,
        out_specs=(P("rep", None, None),) * 3 + (P("rep", "dp", None),) * 6,
        check_vma=False,
    )
```

```python
import functools

import jax
import jax.numpy as jnp
from jax import lax
from jax.experimental import pallas as pl
from jax.experimental.pallas import tpu as pltpu
from jax.sharding import PartitionSpec as P

X, Y, Z = 4, 4, 8
F = 1408
COUNT = 3 * 2 * 512 * F
SEMS = 256
LOADS = 32
ROWS = 704
f32, bf16 = jnp.float32, jnp.bfloat16
BOTH = (0, 1)
WAYS = (1, -1)
LONG = ((0, 1), (1, -1))
SHORT = ((1, 1), (0, -1))


def chains(n):
    return [(*one, n // 2) for one in LONG] + [(*one, n // 2 - 1) for one in SHORT]


def slots(n):
    return {key: i for i, key in enumerate((h, s, t) for h, s, length in chains(n) for t in range(1, length + 1))}


def sixteen(i):
    return pl.ds(pl.multiple_of(i * 16, 16), 16)


def loop(n, body):
    def step(i, carry):
        body(i)
        return carry

    lax.fori_loop(0, n, step, 0)


def kernel(gg, gu, gd, wg, wu, wd, mg, mu, md, vg, vu, vd, WG, OD, gwide, gdown, *scratch):
    (G, GR, GD, L1, F1, B1, L2, F2, ZS, ZF, ZL, LZ, FD, BD, LDX, DS, YS, YF, YL, NS, NL, WD, WZ, YW, PF, PB, OW, OWD) = scratch[:-4]
    ssem, rsem, lsem, wsem = scratch[-4:]
    d = lax.axis_index("dp")
    x, y, z = d // 32, (d // 8) % 4, d % 8
    place = {"x": (x, 4), "y": (y, 4), "z": (z, 8)}

    def at(axis, k):
        p, n = place[axis]
        return lax.rem(p + (k + n) % n, n)

    def device(axis, k):
        p = at(axis, k)
        return {"dp": {"x": p * 32 + y * 8 + z, "y": x * 32 + p * 8 + z, "z": x * 32 + y * 8 + p}[axis]}

    used = [0]
    pending = []

    def send(src, dst, axis, k):
        i = used[0]
        used[0] += 1
        copy = pltpu.make_async_remote_copy(
            src_ref=src, dst_ref=dst, send_sem=ssem.at[i], recv_sem=rsem.at[i],
            device_id=device(axis, k), device_id_type=pl.DeviceIdType.MESH,
        )
        copy.start()
        pending.append(copy)
        return copy

    loads = {}

    def load(key, src, dst):
        copy = pltpu.make_async_copy(src, dst, lsem.at[len(loads)])
        copy.start()
        loads[key] = copy

    class Scatter:
        def __init__(self, axis, own, landing, add, need=None):
            self.axis, self.own, self.landing, self.add, self.need = axis, own, landing, add, need
            self.n = place[axis][1]
            self.length = {(h, s): length for h, s, length in chains(self.n)}
            self.slot = slots(self.n)
            self.copies = {}

        def at(self, h, s, t):
            return self.landing.at[self.slot[h, s, t]]

        def first(self, h, s):
            k = s * self.length[h, s]
            if self.need:
                self.need(h, k)
            self.copies[h, s, 1] = send(self.own(h, k), self.at(h, s, 1), self.axis, s)

        def start(self):
            for h, s, _ in chains(self.n):
                self.first(h, s)

        def arrive(self, h, s, t):
            self.copies[h, s, t].wait_recv()
            if t < self.length[h, s]:
                k = s * (self.length[h, s] - t)
                if self.need:
                    self.need(h, k)
                self.add(self.at(h, s, t), h, k)
                self.copies[h, s, t + 1] = send(self.at(h, s, t), self.at(h, s, t + 1), self.axis, s)

        def last(self, h):
            for s in WAYS:
                self.arrive(h, s, self.length[h, s])
            return [self.at(h, s, self.length[h, s]) for s in WAYS]

    class Gather:
        def __init__(self, axis, part):
            self.axis, self.part = axis, part
            self.n = place[axis][1]
            self.length = {(h, s): length for h, s, length in chains(self.n)}
            self.copies = {}

        def push(self, h, s, t):
            ref = self.part(h, -s * (t - 1))
            self.copies[h, s, t] = send(ref, ref, self.axis, s)

        def start(self):
            for h, s, _ in chains(self.n):
                self.push(h, s, 1)

        def arrive(self, h, s, t):
            self.copies[h, s, t].wait_recv()
            if t < self.length[h, s]:
                self.push(h, s, t + 1)
            return -s * t

    def load_wide(f, h, k):
        if f == 0:
            load((f, h, k), (gg, gu)[h].at[0, at("x", k)], G.at[h, 0, at("x", k)])
        else:
            load((f, h, k), (gg, gu)[h].at[1, :, at("y", k)], G.at[h, 1, :, at("y", k)])

    for h in BOTH:
        for f in BOTH:
            load_wide(f, h, 2)
    for i in BOTH:
        load(("down", i), gd.at[i], GR.at[i])
    for h, k in ((1, 1), (0, 3), (0, 1), (1, 3), (0, 0), (1, 0)):
        for f in BOTH:
            load_wide(f, h, k)
    mine = pl.multiple_of(8 * (d // 2), 8)
    low = pl.multiple_of(8 * ((11 * d) // 8) - 8 * (d // 127), 8)
    own_w = [pltpu.make_async_copy(w.at[:, pl.ds(mine, 8), :], OW.at[i], wsem.at[i]) for i, w in enumerate((wg, wu))]
    own_w.append(pltpu.make_async_copy(wd.at[:, pl.ds(low, 24), :], OWD, wsem.at[2]))
    for copy in own_w:
        copy.start()
    ready = set()

    def need(f, n):
        def wait(h, k):
            key = (f, h, k % n)
            if key not in ready:
                ready.add(key)
                loads[key].wait()

        return wait

    partners = [(a, k) for a, n in (("x", 4), ("y", 4), ("z", 8)) for k in range(1, n)]
    barrier = pltpu.get_barrier_semaphore()
    for a, k in partners:
        pl.semaphore_signal(barrier, inc=1, device_id=device(a, k), device_id_type=pl.DeviceIdType.MESH)

    row = lax.broadcasted_iota(jnp.int32, (ROWS, 128), 0)
    lane = lax.broadcasted_iota(jnp.int32, (ROWS, 128), 1)

    def split(i, n):
        q = (i * (2**18 // n + 1)) >> 18
        return q, i - q * n

    zz, rest = split(row, 88)
    yy, rest = split(rest, 22)
    layer, r = split(rest, 11)
    forth = layer * 352 + yy * 88 + zz * 11 + r
    layer, rest = split(row, 352)
    yy, rest = split(rest, 88)
    zz, r = split(rest, 11)
    back = zz * 88 + yy * 22 + layer * 11 + r
    for ref, there in ((PF, forth), (PB, back)):
        for c in range(0, ROWS, 128):
            n = min(128, ROWS - c)
            ref[:, c : c + n] = jnp.where(there == lane + c, 1.0, 0.0).astype(bf16)[:, :n]
    pl.semaphore_wait(barrier, len(partners))

    def wide(f):
        def own(h, k):
            return G.at[h, 0, at("x", k)] if f == 0 else G.at[h, 1, :, at("y", k)]

        return own

    def add_wide(f):
        def add(got, h, k):
            own = wide(f)(h, k)

            def body(i):
                rows = (i // 2, sixteen(i % 2))
                got[rows] = (got[rows].astype(f32) + own[rows].astype(f32)).astype(bf16)

            loop(8, body)

        return add

    def add_down(got, h, k):
        own = GD.at[h, at("z", k)]

        def body(i):
            got[i] = (got[i].astype(f32) + own[i].astype(f32)).astype(bf16)

        loop(4, body)

    first = [Scatter("xy"[f], wide(f), L1.at[f], add_wide(f), need(f, 4)) for f in BOTH]
    down = Scatter("z", lambda h, k: GD.at[h, at("z", k)], LZ, add_down)

    def end_wide(f, h):
        a, b = first[f].last(h)
        need(f, 4)(h, 0)
        own = wide(f)(h, 0)

        def body(i):
            rows = (i // 2, sixteen(i % 2))
            total = own[rows].astype(f32) + a[rows].astype(f32) + b[rows].astype(f32)
            F1[(f, h, *rows)] = total
            B1[(f, h, *rows)] = total.astype(bf16)

        loop(8, body)

    def end_down(h):
        a, b = down.last(h)
        own = GD.at[h, at("z", 0)]

        def body(i):
            total = own[i].astype(f32) + a[i].astype(f32) + b[i].astype(f32)
            FD[h, i] = total
            BD[h, i] = total.astype(bf16)

        loop(4, body)

    def add_second(f):
        axis = "yx"[f]

        def add(got, h, k):
            own = F1.at[f, h, at(axis, k)]

            def body(i):
                rows = (sixteen(i),)
                got[rows] = (got[rows].astype(f32) + own[rows]).astype(bf16)

            loop(2, body)

        return add

    def second_own(f):
        axis = "yx"[f]
        return lambda h, k: B1.at[f, h, at(axis, k)]

    def add_down_second(got, h, k):
        got[...] = (got[...].astype(f32) + FD[h, at("x", k)]).astype(bf16)

    second = [Scatter("yx"[f], second_own(f), L2.at[f], add_second(f)) for f in BOTH]
    down_second = Scatter("x", lambda h, k: BD.at[h, at("x", k)], LDX, add_down_second)

    def end_second(f, h):
        a, b = second[f].last(h)
        own = F1.at[f, h, at("yx"[f], 0)]

        def body(i):
            rows = (sixteen(i),)
            F2[(f, h, *rows)] = own[rows] + a[rows].astype(f32) + b[rows].astype(f32)

        loop(2, body)

    def arrive_pair(ring, t, short=False):
        for h, s in SHORT if short else LONG:
            ring.arrive(h, s, t)

    for f in BOTH:
        for h, s in LONG:
            first[f].first(h, s)
    for f in BOTH:
        for h, s in SHORT:
            first[f].first(h, s)
    for i in BOTH:
        loads["down", i].wait()

    def permute(i):
        rows = GR[:, pl.ds(pl.multiple_of(i * 352, 32), 352), :].reshape(ROWS, 512)
        out = jnp.dot(PF[...], rows, preferred_element_type=f32)
        for zz in range(Z):
            for h in BOTH:
                GD[h, zz, i] = out[88 * zz : 88 * zz + 88, 256 * h : 256 * h + 256].astype(bf16)

    loop(4, permute)
    down.start()
    arrive_pair(down, 1)
    arrive_pair(down, 1, True)
    arrive_pair(first[0], 1)
    arrive_pair(first[1], 1)
    arrive_pair(down, 2)
    arrive_pair(down, 2, True)
    arrive_pair(down, 3)
    for f in BOTH:
        for h in BOTH:
            end_wide(f, h)
        second[f].start()
    for h in BOTH:
        end_down(h)
    down_second.start()
    for f in BOTH:
        arrive_pair(second[f], 1)
    arrive_pair(down_second, 1)
    for f in BOTH:
        for h in BOTH:
            end_second(f, h)

    for h in BOTH:
        for j in range(4):
            t0, t1 = (F2[f, h, 8 * j : 8 * j + 8, :] for f in BOTH)
            for i, block in enumerate((jnp.concatenate([t0[:4], t1[:4]], 0), jnp.concatenate([t0[4:], t1[4:]], 0))):
                ZF[2 * j + i, h] = block
                ZS[2 * j + i, h] = block.astype(bf16)
    far = (4, 3, 5, 2, 6, 1, 7)
    third = {k: send(ZS.at[at("z", k)], ZL.at[k], "z", k) for k in far}

    for h in BOTH:
        a, b = down_second.last(h)
        DS[h, :88] = FD[h, at("x", 0)] + a[...].astype(f32) + b[...].astype(f32)
        DS[h, 88:] = jnp.zeros((8, 256), f32)
        for j in range(4):
            block = DS[h, 22 * j : 22 * j + 24, :]
            YF[j, h] = block
            YS[j, h] = block.astype(bf16)
    third_down = {k: send(YS.at[at("y", k)], YL.at[k], "y", k) for k in (2, 1, 3)}

    for k in (1, 3, 2):
        third_down[k].wait_recv()
    real = lax.broadcasted_iota(jnp.int32, (24, 256), 0) < 22
    squares = jnp.zeros((), f32)
    g_down = []
    for h in BOTH:
        total = YF[y, h]
        for k in (1, 2, 3):
            total = total + YL[k, h].astype(f32)
        total = jnp.where(real, total, 0.0).astype(bf16).astype(f32)
        g_down.append(total)
        squares += jnp.sum(total * total)
    for k in reversed(far):
        third[k].wait_recv()
    g_wide = []
    for h in BOTH:
        total = ZF[z, h]
        for k in range(1, 8):
            total = total + ZL[k, h].astype(f32)
        total = total.astype(bf16).astype(f32)
        g_wide.append(total)
        squares += jnp.sum(total * total)

    total = jnp.full((8, 128), squares, f32)
    for i, (a, n) in enumerate((("x", 4), ("y", 4), ("z", 8))):
        NS[i] = total
        copies = [send(NS.at[i], NL.at[i, k], a, k) for k in range(1, n)]
        for copy in copies:
            copy.wait_recv()
        for k in range(1, n):
            total = total + NL[i, k]
    factor = jnp.minimum(1.0, 0.5 * lax.rsqrt(total / COUNT + 1e-30))[0:1, 0:1]

    def adamw(w, m, v, g):
        m = 0.9 * m + 0.1 * g
        v = 0.95 * v + 0.05 * g * g
        return (w - 0.02 * (m * lax.rsqrt(v + 1e-8) + 0.1 * w)).astype(bf16)

    for copy in own_w:
        copy.wait()
    odd = d % 2 == 1
    for h, (m_, v_) in enumerate(((mg, vg), (mu, vu))):
        w = [OW[h, i].astype(f32) for i in BOTH]
        w = jnp.concatenate([jnp.where(odd, one[4:], one[:4]) for one in w], 0)
        m, v = (jnp.concatenate([r[0], r[1]], 0) for r in (m_, v_))
        g = g_wide[h] * factor
        gwide[h] = g
        WZ[z, h] = adamw(w, m, v, g)
    g = jnp.concatenate(g_down, 1) * factor
    gdown[...] = g
    for h in BOTH:
        DS[h, :24] = jnp.zeros((24, 256), f32)
    pick = lax.broadcasted_iota(jnp.int32, (24, 24), 1) == lax.broadcasted_iota(jnp.int32, (24, 24), 0) + (11 * d - low)
    pick = jnp.where(pick, 1.0, 0.0).astype(bf16)
    for layer in BOTH:
        w = jnp.dot(pick, OWD[layer], preferred_element_type=f32)[:11]
        w = adamw(w, md[:, layer, :], vd[:, layer, :], g[11 * layer : 11 * layer + 11])
        for h in BOTH:
            DS[h, 11 * layer : 11 * layer + 11, :] = w[:, 256 * h : 256 * h + 256].astype(f32)
    for h in BOTH:
        YW[y, h] = DS[h, :24].astype(bf16)

    wide_z = {k: send(WZ.at[z], WZ.at[z], "z", k) for k in far}
    down_y = {k: send(YW.at[y], YW.at[y], "y", k) for k in (2, 1, 3)}
    for k in (1, 3, 2):
        down_y[k].wait_recv()
    for h in BOTH:
        for j in range(4):
            DS[h, 22 * j : 22 * j + 24, :] = YW[j, h].astype(f32)
        WD[h, z, x] = DS[h, :88].astype(bf16)
    down_x = Gather("x", lambda h, k: WD.at[h, z, at("x", k)])
    down_x.start()
    for k in reversed(far):
        wide_z[k].wait_recv()
    for h in BOTH:
        for layer in BOTH:
            rows = slice(4 * layer, 4 * layer + 4)
            for j in range(2):
                parts = [WZ[4 * j + i, h].astype(f32)[rows] for i in range(4)]
                WG[h, layer, x, y, 16 * j : 16 * j + 16, :] = jnp.concatenate(parts, 0).astype(bf16)
    near = [Gather("y", lambda h, k: WG.at[h, 0, x, at("y", k)]), Gather("x", lambda h, k: WG.at[h, 1, at("x", k), y])]
    for ring in near:
        ring.start()
    arrive_pair(down_x, 1)
    arrive_pair(down_x, 1, True)
    arrive_pair(down_x, 2)
    down_z = Gather("z", lambda h, k: WD.at[h, at("z", k)])
    down_z.start()

    for ring in near:
        arrive_pair(ring, 1)
    for ring in near:
        arrive_pair(ring, 1, True)
    far_rings = [Gather("x", lambda h, k: WG.at[h, 0, at("x", k)]), Gather("y", lambda h, k: WG.at[h, 1, :, at("y", k)])]
    for f in BOTH:
        arrive_pair(near[f], 2)
        far_rings[f].start()
    arrive_pair(down_z, 1)
    arrive_pair(down_z, 1, True)
    arrive_pair(down_z, 2)
    for f in BOTH:
        arrive_pair(far_rings[f], 1)
    arrive_pair(down_z, 2, True)
    arrive_pair(down_z, 3)
    for f in BOTH:
        arrive_pair(far_rings[f], 1, True)
    arrive_pair(down_z, 3, True)
    arrive_pair(down_z, 4)

    def restore(i):
        for h in BOTH:
            rows = WD[h, :, i].astype(f32).reshape(ROWS, 256).astype(bf16)
            out = jnp.dot(PB[...], rows, preferred_element_type=f32).astype(bf16)
            for layer in BOTH:
                OD[layer, pl.ds(pl.multiple_of(i * 352, 32), 352), 256 * h : 256 * h + 256] = out[352 * layer : 352 * layer + 352]

    loop(4, restore)
    for f in BOTH:
        arrive_pair(far_rings[f], 2)
    for copy in pending:
        copy.wait_send()


def finish(W, OD, gwide, gdown, mg, mu, md, vg, vu, vd, og, ou, od, omg, omu, omd, ovg, ovu, ovd, sem):
    copies = [pltpu.make_async_copy(src, dst, sem.at[i]) for i, (src, dst) in enumerate(((W.at[0], og), (W.at[1], ou), (OD, od)))]
    for copy in copies:
        copy.start()

    def moments(m, v, g):
        return 0.9 * m + 0.1 * g, 0.95 * v + 0.05 * g * g

    for layer in BOTH:
        for h, (m, v, om, ov) in enumerate(((mg, vg, omg, ovg), (mu, vu, omu, ovu))):
            om[layer], ov[layer] = moments(m[layer], v[layer], gwide[h, 4 * layer : 4 * layer + 4, :])
        m, v = moments(md[:, layer, :], vd[:, layer, :], gdown[11 * layer : 11 * layer + 11, :])
        omd[:, layer, :] = m
        ovd[:, layer, :] = v
    for copy in copies:
        copy.wait()


def step_kernel(*args):
    hbm, vmem = pl.BlockSpec(memory_space=pl.ANY), pl.BlockSpec(memory_space=pltpu.VMEM)
    wide, deep = (2, 4, F), (11, 2, 512)
    unit, half = (4, 32, F), (4, 88, 256)
    pair, square, whole_down = (2, 2), (4, *unit), (2, 8, *half)
    blocks, small, tile = (8, 2, 8, F), (4, 2, 24, 256), (8, 128)
    shape = jax.ShapeDtypeStruct
    out = pl.pallas_call(
        kernel,
        out_shape=(pltpu.VMEM((*pair, *square), bf16), pltpu.VMEM((2, F, 512), bf16), pltpu.VMEM(blocks[1:], f32), pltpu.VMEM((24, 512), f32)),
        in_specs=[hbm] * 6 + [vmem] * 6,
        out_specs=(vmem,) * 4,
        scratch_shapes=[
            pltpu.VMEM((*pair, *square), bf16),
            pltpu.VMEM((2, F, 512), bf16),
            pltpu.VMEM(whole_down, bf16),
            pltpu.VMEM((2, 6, *unit), bf16),
            pltpu.VMEM((*pair, *unit), f32),
            pltpu.VMEM((*pair, *unit), bf16),
            pltpu.VMEM((2, 6, *unit[1:]), bf16),
            pltpu.VMEM((*pair, *unit[1:]), f32),
            pltpu.VMEM(blocks, bf16),
            pltpu.VMEM(blocks, f32),
            pltpu.VMEM(blocks, bf16),
            pltpu.VMEM((14, *half), bf16),
            pltpu.VMEM((2, *half), f32),
            pltpu.VMEM((2, *half), bf16),
            pltpu.VMEM((6, *half[1:]), bf16),
            pltpu.VMEM((2, 96, 256), f32),
            pltpu.VMEM(small, bf16),
            pltpu.VMEM(small, f32),
            pltpu.VMEM(small, bf16),
            pltpu.VMEM((3, *tile), f32),
            pltpu.VMEM((3, 8, *tile), f32),
            pltpu.VMEM(whole_down, bf16),
            pltpu.VMEM(blocks, bf16),
            pltpu.VMEM(small, bf16),
            pltpu.VMEM((ROWS, ROWS), bf16),
            pltpu.VMEM((ROWS, ROWS), bf16),
            pltpu.VMEM((*pair, 8, F), bf16),
            pltpu.VMEM((2, 24, 512), bf16),
            pltpu.SemaphoreType.DMA((SEMS,)),
            pltpu.SemaphoreType.DMA((SEMS,)),
            pltpu.SemaphoreType.DMA((LOADS,)),
            pltpu.SemaphoreType.DMA((3,)),
        ],
        compiler_params=pltpu.CompilerParams(collective_id=0, has_side_effects=True, vmem_limit_bytes=40 * 2**20),
        name="clipped_step",
    )(*args)
    out = [pltpu.with_memory_space_constraint(one, pltpu.VMEM) for one in out]
    return pl.pallas_call(
        finish,
        out_shape=(shape((2, *square), bf16),) * 2 + (shape((2, F, 512), bf16),) + (shape(wide, f32), shape(wide, f32), shape(deep, f32)) * 2,
        in_specs=[vmem] * 10,
        out_specs=(hbm,) * 3 + (vmem,) * 6,
        scratch_shapes=[pltpu.SemaphoreType.DMA((3,))],
        compiler_params=pltpu.CompilerParams(vmem_limit_bytes=40 * 2**20),
        name="finish",
    )(*out, *args[6:])


def solution(mesh):
    def step(gg, gu, gd, wg, wu, wd, mg, mu, md, vg, vu, vd):
        gg, gu = (g.reshape(2, 4, 4, 32, F) for g in (gg, gu))
        md, vd = (a.transpose(1, 0, 2) for a in (md, vd))
        og, ou, od, omg, omu, omd, ovg, ovu, ovd = step_kernel(gg, gu, gd[0], wg, wu, wd, mg, mu, md, vg, vu, vd)
        og, ou = (o.reshape(2, 512, F) for o in (og, ou))
        omd, ovd = (a.transpose(1, 0, 2) for a in (omd, ovd))
        return og, ou, od, omg, omu, omd, ovg, ovu, ovd

    all_of, cut = P(None, None, None), P(None, "dp", None)
    return jax.shard_map(
        step,
        mesh=mesh,
        in_specs=(P(("rep", "dp"), None, None, None),) * 3 + (all_of,) * 3 + (cut,) * 6,
        out_specs=(P("rep", None, None),) * 3 + (P("rep", "dp", None),) * 6,
        check_vma=False,
    )
```

```python
import functools

import jax
import jax.numpy as jnp
from jax import lax
from jax.experimental import pallas as pl
from jax.experimental.pallas import tpu as pltpu
from jax.sharding import PartitionSpec as P

X, Y, Z = 4, 4, 8
F = 1408
COUNT = 3 * 2 * 512 * F
SEMS = 256
LOADS = 32
ROWS = 704
f32, bf16 = jnp.float32, jnp.bfloat16
BOTH = (0, 1)
WAYS = (1, -1)
LONG = ((0, 1), (1, -1))
SHORT = ((1, 1), (0, -1))


def chains(n):
    return [(*one, n // 2) for one in LONG] + [(*one, n // 2 - 1) for one in SHORT]


def slots(n):
    return {key: i for i, key in enumerate((h, s, t) for h, s, length in chains(n) for t in range(1, length + 1))}


def sixteen(i):
    return pl.ds(pl.multiple_of(i * 16, 16), 16)


def loop(n, body):
    def step(i, carry):
        body(i)
        return carry

    lax.fori_loop(0, n, step, 0)


def kernel(gg, gu, gd, wg, wu, wd, mg, mu, md, vg, vu, vd, WG, OD, MW, MD, *scratch):
    (G, GR, GD, L1, F1, B1, L2, F2, ZS, ZF, ZL, LZ, FD, BD, LDX, DS, YS, YF, YL, NS, NL, WD, WZ, YW, PF, PB, OW, OWD, IW, ID) = scratch[:-4]
    ssem, rsem, lsem, wsem = scratch[-4:]
    d = lax.axis_index("dp")
    x, y, z = d // 32, (d // 8) % 4, d % 8
    place = {"x": (x, 4), "y": (y, 4), "z": (z, 8)}

    def at(axis, k):
        p, n = place[axis]
        return lax.rem(p + (k + n) % n, n)

    def device(axis, k):
        p = at(axis, k)
        return {"dp": {"x": p * 32 + y * 8 + z, "y": x * 32 + p * 8 + z, "z": x * 32 + y * 8 + p}[axis]}

    used = [0]
    pending = []

    def send(src, dst, axis, k):
        i = used[0]
        used[0] += 1
        copy = pltpu.make_async_remote_copy(
            src_ref=src, dst_ref=dst, send_sem=ssem.at[i], recv_sem=rsem.at[i],
            device_id=device(axis, k), device_id_type=pl.DeviceIdType.MESH,
        )
        copy.start()
        pending.append(copy)
        return copy

    loads = {}

    def load(key, src, dst):
        copy = pltpu.make_async_copy(src, dst, lsem.at[len(loads)])
        copy.start()
        loads[key] = copy

    class Scatter:
        def __init__(self, axis, own, landing, add, need=None):
            self.axis, self.own, self.landing, self.add, self.need = axis, own, landing, add, need
            self.n = place[axis][1]
            self.length = {(h, s): length for h, s, length in chains(self.n)}
            self.slot = slots(self.n)
            self.copies = {}

        def at(self, h, s, t):
            return self.landing.at[self.slot[h, s, t]]

        def first(self, h, s):
            k = s * self.length[h, s]
            if self.need:
                self.need(h, k)
            self.copies[h, s, 1] = send(self.own(h, k), self.at(h, s, 1), self.axis, s)

        def start(self):
            for h, s, _ in chains(self.n):
                self.first(h, s)

        def arrive(self, h, s, t):
            self.copies[h, s, t].wait_recv()
            if t < self.length[h, s]:
                k = s * (self.length[h, s] - t)
                if self.need:
                    self.need(h, k)
                self.add(self.at(h, s, t), h, k)
                self.copies[h, s, t + 1] = send(self.at(h, s, t), self.at(h, s, t + 1), self.axis, s)

        def last(self, h):
            for s in WAYS:
                self.arrive(h, s, self.length[h, s])
            return [self.at(h, s, self.length[h, s]) for s in WAYS]

    class Gather:
        def __init__(self, axis, part):
            self.axis, self.part = axis, part
            self.n = place[axis][1]
            self.length = {(h, s): length for h, s, length in chains(self.n)}
            self.copies = {}

        def push(self, h, s, t):
            ref = self.part(h, -s * (t - 1))
            self.copies[h, s, t] = send(ref, ref, self.axis, s)

        def start(self):
            for h, s, _ in chains(self.n):
                self.push(h, s, 1)

        def arrive(self, h, s, t):
            self.copies[h, s, t].wait_recv()
            if t < self.length[h, s]:
                self.push(h, s, t + 1)
            return -s * t

    def load_wide(f, h, k):
        if f == 0:
            load((f, h, k), (gg, gu)[h].at[0, at("x", k)], G.at[h, 0, at("x", k)])
        else:
            load((f, h, k), (gg, gu)[h].at[1, :, at("y", k)], G.at[h, 1, :, at("y", k)])

    for h in BOTH:
        for f in BOTH:
            load_wide(f, h, 2)
    for i in BOTH:
        load(("down", i), gd.at[i], GR.at[i])
    for h, k in ((1, 1), (0, 3), (0, 1), (1, 3), (0, 0), (1, 0)):
        for f in BOTH:
            load_wide(f, h, k)
    mine = pl.multiple_of(8 * (d // 2), 8)
    low = pl.multiple_of(8 * ((11 * d) // 8) - 8 * (d // 127), 8)
    own_w = [pltpu.make_async_copy(w.at[:, pl.ds(mine, 8), :], OW.at[i], wsem.at[i]) for i, w in enumerate((wg, wu))]
    own_w.append(pltpu.make_async_copy(wd.at[:, pl.ds(low, 24), :], OWD, wsem.at[2]))
    for i, (wide_, deep_) in enumerate((((mg, mu), md), ((vg, vu), vd))):
        for h in BOTH:
            own_w.append(pltpu.make_async_copy(wide_[h], IW.at[i, h], wsem.at[len(own_w)]))
        own_w.append(pltpu.make_async_copy(deep_, ID.at[i], wsem.at[len(own_w)]))
    for copy in own_w:
        copy.start()
    ready = set()

    def need(f, n):
        def wait(h, k):
            key = (f, h, k % n)
            if key not in ready:
                ready.add(key)
                loads[key].wait()

        return wait

    partners = [(a, k) for a, n in (("x", 4), ("y", 4), ("z", 8)) for k in range(1, n)]
    barrier = pltpu.get_barrier_semaphore()
    for a, k in partners:
        pl.semaphore_signal(barrier, inc=1, device_id=device(a, k), device_id_type=pl.DeviceIdType.MESH)

    row = lax.broadcasted_iota(jnp.int32, (ROWS, 128), 0)
    lane = lax.broadcasted_iota(jnp.int32, (ROWS, 128), 1)

    def split(i, n):
        q = (i * (2**18 // n + 1)) >> 18
        return q, i - q * n

    zz, rest = split(row, 88)
    yy, rest = split(rest, 22)
    layer, r = split(rest, 11)
    forth = layer * 352 + yy * 88 + zz * 11 + r
    layer, rest = split(row, 352)
    yy, rest = split(rest, 88)
    zz, r = split(rest, 11)
    back = zz * 88 + yy * 22 + layer * 11 + r
    for ref, there in ((PF, forth), (PB, back)):
        for c in range(0, ROWS, 128):
            n = min(128, ROWS - c)
            ref[:, c : c + n] = jnp.where(there == lane + c, 1.0, 0.0).astype(bf16)[:, :n]
    pl.semaphore_wait(barrier, len(partners))

    def wide(f):
        def own(h, k):
            return G.at[h, 0, at("x", k)] if f == 0 else G.at[h, 1, :, at("y", k)]

        return own

    def add_wide(f):
        def add(got, h, k):
            own = wide(f)(h, k)

            def body(i):
                rows = (i // 2, sixteen(i % 2))
                got[rows] = (got[rows].astype(f32) + own[rows].astype(f32)).astype(bf16)

            loop(8, body)

        return add

    def add_down(got, h, k):
        own = GD.at[h, at("z", k)]

        def body(i):
            got[i] = (got[i].astype(f32) + own[i].astype(f32)).astype(bf16)

        loop(4, body)

    first = [Scatter("xy"[f], wide(f), L1.at[f], add_wide(f), need(f, 4)) for f in BOTH]
    down = Scatter("z", lambda h, k: GD.at[h, at("z", k)], LZ, add_down)

    def end_wide(f, h):
        a, b = first[f].last(h)
        need(f, 4)(h, 0)
        own = wide(f)(h, 0)

        def body(i):
            rows = (i // 2, sixteen(i % 2))
            total = own[rows].astype(f32) + a[rows].astype(f32) + b[rows].astype(f32)
            F1[(f, h, *rows)] = total
            B1[(f, h, *rows)] = total.astype(bf16)

        loop(8, body)

    def end_down(h):
        a, b = down.last(h)
        own = GD.at[h, at("z", 0)]

        def body(i):
            total = own[i].astype(f32) + a[i].astype(f32) + b[i].astype(f32)
            FD[h, i] = total
            BD[h, i] = total.astype(bf16)

        loop(4, body)

    def add_second(f):
        axis = "yx"[f]

        def add(got, h, k):
            own = F1.at[f, h, at(axis, k)]

            def body(i):
                rows = (sixteen(i),)
                got[rows] = (got[rows].astype(f32) + own[rows]).astype(bf16)

            loop(2, body)

        return add

    def second_own(f):
        axis = "yx"[f]
        return lambda h, k: B1.at[f, h, at(axis, k)]

    def add_down_second(got, h, k):
        got[...] = (got[...].astype(f32) + FD[h, at("x", k)]).astype(bf16)

    second = [Scatter("yx"[f], second_own(f), L2.at[f], add_second(f)) for f in BOTH]
    down_second = Scatter("x", lambda h, k: BD.at[h, at("x", k)], LDX, add_down_second)

    def end_second(f, h):
        a, b = second[f].last(h)
        own = F1.at[f, h, at("yx"[f], 0)]

        def body(i):
            rows = (sixteen(i),)
            F2[(f, h, *rows)] = own[rows] + a[rows].astype(f32) + b[rows].astype(f32)

        loop(2, body)

    def arrive_pair(ring, t, short=False):
        for h, s in SHORT if short else LONG:
            ring.arrive(h, s, t)

    for f in BOTH:
        for h, s in LONG:
            first[f].first(h, s)
    for f in BOTH:
        for h, s in SHORT:
            first[f].first(h, s)
    for i in BOTH:
        loads["down", i].wait()

    def permute(i):
        rows = GR[:, pl.ds(pl.multiple_of(i * 352, 32), 352), :].reshape(ROWS, 512)
        out = jnp.dot(PF[...], rows, preferred_element_type=f32)
        for zz in range(Z):
            for h in BOTH:
                GD[h, zz, i] = out[88 * zz : 88 * zz + 88, 256 * h : 256 * h + 256].astype(bf16)

    loop(4, permute)
    down.start()
    arrive_pair(down, 1)
    arrive_pair(down, 1, True)
    arrive_pair(first[0], 1)
    arrive_pair(first[1], 1)
    arrive_pair(down, 2)
    arrive_pair(down, 2, True)
    arrive_pair(down, 3)
    for f in BOTH:
        for h in BOTH:
            end_wide(f, h)
        second[f].start()
    for h in BOTH:
        end_down(h)
    down_second.start()
    for f in BOTH:
        arrive_pair(second[f], 1)
    arrive_pair(down_second, 1)
    for f in BOTH:
        for h in BOTH:
            end_second(f, h)

    for h in BOTH:
        for j in range(4):
            t0, t1 = (F2[f, h, 8 * j : 8 * j + 8, :] for f in BOTH)
            for i, block in enumerate((jnp.concatenate([t0[:4], t1[:4]], 0), jnp.concatenate([t0[4:], t1[4:]], 0))):
                ZF[2 * j + i, h] = block
                ZS[2 * j + i, h] = block.astype(bf16)
    far = (4, 3, 5, 2, 6, 1, 7)
    third = {k: send(ZS.at[at("z", k)], ZL.at[k], "z", k) for k in far}

    for h in BOTH:
        a, b = down_second.last(h)
        DS[h, :88] = FD[h, at("x", 0)] + a[...].astype(f32) + b[...].astype(f32)
        DS[h, 88:] = jnp.zeros((8, 256), f32)
        for j in range(4):
            block = DS[h, 22 * j : 22 * j + 24, :]
            YF[j, h] = block
            YS[j, h] = block.astype(bf16)
    third_down = {k: send(YS.at[at("y", k)], YL.at[k], "y", k) for k in (2, 1, 3)}

    for k in (1, 3, 2):
        third_down[k].wait_recv()
    real = lax.broadcasted_iota(jnp.int32, (24, 256), 0) < 22
    squares = jnp.zeros((), f32)
    g_down = []
    for h in BOTH:
        total = YF[y, h]
        for k in (1, 2, 3):
            total = total + YL[k, h].astype(f32)
        total = jnp.where(real, total, 0.0).astype(bf16).astype(f32)
        g_down.append(total)
        squares += jnp.sum(total * total)
    for k in reversed(far):
        third[k].wait_recv()
    g_wide = []
    for h in BOTH:
        total = ZF[z, h]
        for k in range(1, 8):
            total = total + ZL[k, h].astype(f32)
        total = total.astype(bf16).astype(f32)
        g_wide.append(total)
        squares += jnp.sum(total * total)

    total = jnp.full((8, 128), squares, f32)
    for i, (a, n) in enumerate((("x", 4), ("y", 4), ("z", 8))):
        NS[i] = total
        copies = [send(NS.at[i], NL.at[i, k], a, k) for k in range(1, n)]
        for copy in copies:
            copy.wait_recv()
        for k in range(1, n):
            total = total + NL[i, k]
    factor = jnp.minimum(1.0, 0.5 * lax.rsqrt(total / COUNT + 1e-30))[0:1, 0:1]

    def adamw(w, m, v, g):
        m = 0.9 * m + 0.1 * g
        v = 0.95 * v + 0.05 * g * g
        return (w - 0.02 * (m * lax.rsqrt(v + 1e-8) + 0.1 * w)).astype(bf16), m, v

    for copy in own_w:
        copy.wait()
    odd = d % 2 == 1
    for h in BOTH:
        w = [OW[h, i].astype(f32) for i in BOTH]
        w = jnp.concatenate([jnp.where(odd, one[4:], one[:4]) for one in w], 0)
        m, v = (jnp.concatenate([IW[i, h, 0], IW[i, h, 1]], 0) for i in BOTH)
        WZ[z, h], *new = adamw(w, m, v, g_wide[h] * factor)
        for i, one in enumerate(new):
            for layer in BOTH:
                MW[i, h, layer] = one[4 * layer : 4 * layer + 4]
    g = jnp.concatenate(g_down, 1) * factor
    for h in BOTH:
        DS[h, :24] = jnp.zeros((24, 256), f32)
    pick = lax.broadcasted_iota(jnp.int32, (24, 24), 1) == lax.broadcasted_iota(jnp.int32, (24, 24), 0) + (11 * d - low)
    pick = jnp.where(pick, 1.0, 0.0).astype(bf16)
    for layer in BOTH:
        w = jnp.dot(pick, OWD[layer], preferred_element_type=f32)[:11]
        w, *new = adamw(w, ID[0, :, layer, :], ID[1, :, layer, :], g[11 * layer : 11 * layer + 11])
        for i, one in enumerate(new):
            MD[i, :, layer, :] = one
        for h in BOTH:
            DS[h, 11 * layer : 11 * layer + 11, :] = w[:, 256 * h : 256 * h + 256].astype(f32)
    for h in BOTH:
        YW[y, h] = DS[h, :24].astype(bf16)

    wide_z = {k: send(WZ.at[z], WZ.at[z], "z", k) for k in far}
    down_y = {k: send(YW.at[y], YW.at[y], "y", k) for k in (2, 1, 3)}
    for k in (1, 3, 2):
        down_y[k].wait_recv()
    for h in BOTH:
        for j in range(4):
            DS[h, 22 * j : 22 * j + 24, :] = YW[j, h].astype(f32)
        WD[h, z, x] = DS[h, :88].astype(bf16)
    down_x = Gather("x", lambda h, k: WD.at[h, z, at("x", k)])
    down_x.start()
    for k in reversed(far):
        wide_z[k].wait_recv()
    for h in BOTH:
        for layer in BOTH:
            rows = slice(4 * layer, 4 * layer + 4)
            for j in range(2):
                parts = [WZ[4 * j + i, h].astype(f32)[rows] for i in range(4)]
                WG[h, layer, x, y, 16 * j : 16 * j + 16, :] = jnp.concatenate(parts, 0).astype(bf16)
    near = [Gather("y", lambda h, k: WG.at[h, 0, x, at("y", k)]), Gather("x", lambda h, k: WG.at[h, 1, at("x", k), y])]
    for ring in near:
        ring.start()
    arrive_pair(down_x, 1)
    arrive_pair(down_x, 1, True)
    arrive_pair(down_x, 2)
    down_z = Gather("z", lambda h, k: WD.at[h, at("z", k)])
    down_z.start()

    for ring in near:
        arrive_pair(ring, 1)
    for ring in near:
        arrive_pair(ring, 1, True)
    far_rings = [Gather("x", lambda h, k: WG.at[h, 0, at("x", k)]), Gather("y", lambda h, k: WG.at[h, 1, :, at("y", k)])]
    for f in BOTH:
        arrive_pair(near[f], 2)
        far_rings[f].start()
    arrive_pair(down_z, 1)
    arrive_pair(down_z, 1, True)
    arrive_pair(down_z, 2)
    for f in BOTH:
        arrive_pair(far_rings[f], 1)
    arrive_pair(down_z, 2, True)
    arrive_pair(down_z, 3)
    for f in BOTH:
        arrive_pair(far_rings[f], 1, True)
    arrive_pair(down_z, 3, True)
    arrive_pair(down_z, 4)

    def restore(i):
        for h in BOTH:
            rows = WD[h, :, i].astype(f32).reshape(ROWS, 256).astype(bf16)
            out = jnp.dot(PB[...], rows, preferred_element_type=f32).astype(bf16)
            for layer in BOTH:
                OD[layer, pl.ds(pl.multiple_of(i * 352, 32), 352), 256 * h : 256 * h + 256] = out[352 * layer : 352 * layer + 352]

    loop(4, restore)
    for f in BOTH:
        arrive_pair(far_rings[f], 2)
    for copy in pending:
        copy.wait_send()


def finish(W, OD, MW, MD, *rest):
    sem = rest[-1]
    sources = [W.at[0], W.at[1], OD] + [r for i in BOTH for r in (MW.at[i, 0], MW.at[i, 1], MD.at[i])]
    copies = [pltpu.make_async_copy(src, dst, sem.at[i]) for i, (src, dst) in enumerate(zip(sources, rest))]
    for copy in copies:
        copy.start()
    for copy in copies:
        copy.wait()


def step_kernel(*args):
    hbm, vmem = pl.BlockSpec(memory_space=pl.ANY), pl.BlockSpec(memory_space=pltpu.VMEM)
    wide, deep = (2, 4, F), (11, 2, 512)
    unit, half = (4, 32, F), (4, 88, 256)
    pair, square, whole_down = (2, 2), (4, *unit), (2, 8, *half)
    blocks, small, tile = (8, 2, 8, F), (4, 2, 24, 256), (8, 128)
    shape = jax.ShapeDtypeStruct
    out = pl.pallas_call(
        kernel,
        out_shape=(pltpu.VMEM((*pair, *square), bf16), pltpu.VMEM((2, F, 512), bf16), pltpu.VMEM((*pair, *wide), f32), pltpu.VMEM((2, *deep), f32)),
        in_specs=[hbm] * 12,
        out_specs=(vmem,) * 4,
        scratch_shapes=[
            pltpu.VMEM((*pair, *square), bf16),
            pltpu.VMEM((2, F, 512), bf16),
            pltpu.VMEM(whole_down, bf16),
            pltpu.VMEM((2, 6, *unit), bf16),
            pltpu.VMEM((*pair, *unit), f32),
            pltpu.VMEM((*pair, *unit), bf16),
            pltpu.VMEM((2, 6, *unit[1:]), bf16),
            pltpu.VMEM((*pair, *unit[1:]), f32),
            pltpu.VMEM(blocks, bf16),
            pltpu.VMEM(blocks, f32),
            pltpu.VMEM(blocks, bf16),
            pltpu.VMEM((14, *half), bf16),
            pltpu.VMEM((2, *half), f32),
            pltpu.VMEM((2, *half), bf16),
            pltpu.VMEM((6, *half[1:]), bf16),
            pltpu.VMEM((2, 96, 256), f32),
            pltpu.VMEM(small, bf16),
            pltpu.VMEM(small, f32),
            pltpu.VMEM(small, bf16),
            pltpu.VMEM((3, *tile), f32),
            pltpu.VMEM((3, 8, *tile), f32),
            pltpu.VMEM(whole_down, bf16),
            pltpu.VMEM(blocks, bf16),
            pltpu.VMEM(small, bf16),
            pltpu.VMEM((ROWS, ROWS), bf16),
            pltpu.VMEM((ROWS, ROWS), bf16),
            pltpu.VMEM((*pair, 8, F), bf16),
            pltpu.VMEM((2, 24, 512), bf16),
            pltpu.VMEM((*pair, *wide), f32),
            pltpu.VMEM((2, *deep), f32),
            pltpu.SemaphoreType.DMA((SEMS,)),
            pltpu.SemaphoreType.DMA((SEMS,)),
            pltpu.SemaphoreType.DMA((LOADS,)),
            pltpu.SemaphoreType.DMA((9,)),
        ],
        compiler_params=pltpu.CompilerParams(collective_id=0, has_side_effects=True, vmem_limit_bytes=50 * 2**20),
        name="clipped_step",
    )(*args)
    out = [pltpu.with_memory_space_constraint(one, pltpu.VMEM) for one in out]
    return pl.pallas_call(
        finish,
        out_shape=(shape((2, *square), bf16),) * 2 + (shape((2, F, 512), bf16),) + (shape(wide, f32), shape(wide, f32), shape(deep, f32)) * 2,
        in_specs=[vmem] * 4,
        out_specs=(hbm,) * 9,
        scratch_shapes=[pltpu.SemaphoreType.DMA((9,))],
        compiler_params=pltpu.CompilerParams(vmem_limit_bytes=50 * 2**20),
        name="finish",
    )(*out)


def solution(mesh):
    def step(gg, gu, gd, wg, wu, wd, mg, mu, md, vg, vu, vd):
        gg, gu = (g.reshape(2, 4, 4, 32, F) for g in (gg, gu))
        md, vd = (a.transpose(1, 0, 2) for a in (md, vd))
        og, ou, od, omg, omu, omd, ovg, ovu, ovd = step_kernel(gg, gu, gd[0], wg, wu, wd, mg, mu, md, vg, vu, vd)
        og, ou = (o.reshape(2, 512, F) for o in (og, ou))
        omd, ovd = (a.transpose(1, 0, 2) for a in (omd, ovd))
        return og, ou, od, omg, omu, omd, ovg, ovu, ovd

    all_of, cut = P(None, None, None), P(None, "dp", None)
    return jax.shard_map(
        step,
        mesh=mesh,
        in_specs=(P(("rep", "dp"), None, None, None),) * 3 + (all_of,) * 3 + (cut,) * 6,
        out_specs=(P("rep", None, None),) * 3 + (P("rep", "dp", None),) * 6,
        check_vma=False,
    )
```

```python
import functools

import jax
import jax.numpy as jnp
from jax import lax
from jax.experimental import pallas as pl
from jax.experimental.pallas import tpu as pltpu
from jax.sharding import PartitionSpec as P

X, Y, Z = 4, 4, 8
F = 1408
COUNT = 3 * 2 * 512 * F
SEMS = 256
LOADS = 32
ROWS = 704
f32, bf16 = jnp.float32, jnp.bfloat16
BOTH = (0, 1)
WAYS = (1, -1)
LONG = ((0, 1), (1, -1))
SHORT = ((1, 1), (0, -1))


def chains(n):
    return [(*one, n // 2) for one in LONG] + [(*one, n // 2 - 1) for one in SHORT]


def slots(n):
    return {key: i for i, key in enumerate((h, s, t) for h, s, length in chains(n) for t in range(1, length + 1))}


def loop(n, body):
    def step(i, carry):
        body(i)
        return carry

    lax.fori_loop(0, n, step, 0)


def kernel(gg, gu, gd, wg, wu, wd, mg, mu, md, vg, vu, vd, WG, OD, MW, MD, *scratch):
    (G, GR, GD, L1, F1, B1, L2, F2, ZS, ZF, ZL, LZ, DS, YS, YF, YL, NS, NL, WD, WZ, YW, PF, PB, OW, OWD, IW, ID) = scratch[:-5]
    ssem, rsem, lsem, wsem, nsem = scratch[-5:]
    d = lax.axis_index("dp")
    x, y, z = d // 32, (d // 8) % 4, d % 8
    place = {"x": (x, 4), "y": (y, 4), "z": (z, 8)}

    def at(axis, k):
        p, n = place[axis]
        return lax.rem(p + (k + n) % n, n)

    def device(axis, k):
        p = at(axis, k)
        return {"x": p * 32 + y * 8 + z, "y": x * 32 + p * 8 + z, "z": x * 32 + y * 8 + p}[axis]

    used = [0]
    pending = []

    def send_to(target, src, dst):
        i = used[0]
        used[0] += 1
        copy = pltpu.make_async_remote_copy(
            src_ref=src, dst_ref=dst, send_sem=ssem.at[i], recv_sem=rsem.at[i],
            device_id={"dp": target}, device_id_type=pl.DeviceIdType.MESH,
        )
        copy.start()
        pending.append(copy)
        return copy

    def send(src, dst, axis, k):
        return send_to(device(axis, k), src, dst)

    plane = sorted(((i, j) for i in range(X) for j in range(Y) if i or j), key=lambda o: -sum(min(k, X - k) for k in o))

    def send_plane(source, target):
        return [send_to(at("x", i) * 32 + at("y", j) * 8 + z, source(i, j), target(i, j)) for i, j in plane]

    loads = {}

    def load(key, src, dst):
        copy = pltpu.make_async_copy(src, dst, lsem.at[len(loads)])
        copy.start()
        loads[key] = copy

    class Scatter:
        def __init__(self, axis, own, landing, add, need=None):
            self.axis, self.own, self.landing, self.add, self.need = axis, own, landing, add, need
            self.n = place[axis][1]
            self.length = {(h, s): length for h, s, length in chains(self.n)}
            self.slot = slots(self.n)
            self.copies = {}

        def at(self, h, s, t):
            return self.landing.at[self.slot[h, s, t]]

        def first(self, h, s):
            k = s * self.length[h, s]
            if self.need:
                self.need(h, k)
            self.copies[h, s, 1] = send(self.own(h, k), self.at(h, s, 1), self.axis, s)

        def start(self):
            for h, s, _ in chains(self.n):
                self.first(h, s)

        def arrive(self, h, s, t):
            self.copies[h, s, t].wait_recv()
            if t < self.length[h, s]:
                k = s * (self.length[h, s] - t)
                if self.need:
                    self.need(h, k)
                self.add(self.at(h, s, t), h, k)
                self.copies[h, s, t + 1] = send(self.at(h, s, t), self.at(h, s, t + 1), self.axis, s)

        def last(self, h):
            for s in WAYS:
                self.arrive(h, s, self.length[h, s])
            return [self.at(h, s, self.length[h, s]) for s in WAYS]

    class Gather:
        def __init__(self, axis, part):
            self.axis, self.part = axis, part
            self.n = place[axis][1]
            self.length = {(h, s): length for h, s, length in chains(self.n)}
            self.copies = {}

        def push(self, h, s, t):
            ref = self.part(h, -s * (t - 1))
            self.copies[h, s, t] = send(ref, ref, self.axis, s)

        def start(self):
            for h, s, _ in chains(self.n):
                self.push(h, s, 1)

        def arrive(self, h, s, t):
            self.copies[h, s, t].wait_recv()
            if t < self.length[h, s]:
                self.push(h, s, t + 1)
            return -s * t

    def load_wide(f, h, k):
        if f == 0:
            load((f, h, k), (gg, gu)[h].at[0, at("x", k)], G.at[h, 0, at("x", k)])
        else:
            load((f, h, k), (gg, gu)[h].at[1, :, at("y", k)], G.at[h, 1, :, at("y", k)])

    for h in BOTH:
        for f in BOTH:
            load_wide(f, h, 2)
    for i in BOTH:
        load(("down", i), gd.at[i], GR.at[i])
    for h, k in ((1, 1), (0, 3), (0, 1), (1, 3), (0, 0), (1, 0)):
        for f in BOTH:
            load_wide(f, h, k)
    mine = pl.multiple_of(8 * (d // 2), 8)
    low = pl.multiple_of(8 * ((11 * d) // 8) - 8 * (d // 127), 8)
    own_w = [pltpu.make_async_copy(w.at[:, pl.ds(mine, 8), :], OW.at[i], wsem.at[i]) for i, w in enumerate((wg, wu))]
    own_w.append(pltpu.make_async_copy(wd.at[:, pl.ds(low, 24), :], OWD, wsem.at[2]))
    for i, (wide_, deep_) in enumerate((((mg, mu), md), ((vg, vu), vd))):
        for h in BOTH:
            own_w.append(pltpu.make_async_copy(wide_[h], IW.at[i, h], wsem.at[len(own_w)]))
        own_w.append(pltpu.make_async_copy(deep_, ID.at[i], wsem.at[len(own_w)]))
    for copy in own_w:
        copy.start()
    ready = set()

    def need(f, n):
        def wait(h, k):
            key = (f, h, k % n)
            if key not in ready:
                ready.add(key)
                loads[key].wait()

        return wait

    barrier = pltpu.get_barrier_semaphore()
    for axis in place:
        for way in WAYS:
            pl.semaphore_signal(barrier, inc=1, device_id={"dp": device(axis, way)}, device_id_type=pl.DeviceIdType.MESH)

    row = lax.broadcasted_iota(jnp.int32, (ROWS, 128), 0)
    lane = lax.broadcasted_iota(jnp.int32, (ROWS, 128), 1)

    def split(i, n):
        q = (i * (2**18 // n + 1)) >> 18
        return q, i - q * n

    def one_hot(ref, there):
        for c in range(0, ROWS, 128):
            n = min(128, ROWS - c)
            ref[:, c : c + n] = jnp.where(there == lane + c, 1.0, 0.0).astype(bf16)[:, :n]

    zz, rest = split(row, 88)
    yy, rest = split(rest, 22)
    layer, r = split(rest, 11)
    one_hot(PF, layer * 352 + yy * 88 + zz * 11 + r)
    pl.semaphore_wait(barrier, 2 * len(place))

    def unit(ref, f, h, k, j):
        return ref.at[h, 0, at("x", k), at("y", j)] if f == 0 else ref.at[h, 1, at("x", j), at("y", k)]

    def by_rows(body):
        loop(2, lambda i: body(pl.ds(pl.multiple_of(i * 16, 16), 16)))

    def first_stage(f, j):
        def add(got, h, k):
            own = unit(G, f, h, k, j)

            def body(rows):
                got[rows] = (got[rows].astype(f32) + own[rows].astype(f32)).astype(bf16)

            by_rows(body)

        return Scatter("xy"[f], lambda h, k: unit(G, f, h, k, j), L1.at[f, j], add, need(f, 4))

    first = [[first_stage(f, j) for j in range(4)] for f in BOTH]

    def end_first(f, j):
        for h in BOTH:
            a, b = first[f][j].last(h)
            need(f, 4)(h, 0)
            own = unit(G, f, h, 0, j)
            place_j = at("yx"[f], j)
            travels = j == 2 or j == (3, 1)[h]

            def body(rows):
                total = own[rows].astype(f32) + a[rows].astype(f32) + b[rows].astype(f32)
                if travels:
                    B1[f, h, place_j, rows] = total.astype(bf16)
                else:
                    F1[f, h, place_j, rows] = total

            by_rows(body)

    def add_down(got, h, k):
        own = GD.at[h, at("z", k)]

        def body(i):
            got[i] = (got[i].astype(f32) + own[i].astype(f32)).astype(bf16)

        loop(4, body)

    down = Scatter("z", lambda h, k: GD.at[h, at("z", k)], LZ, add_down)

    def end_down(h):
        a, b = down.last(h)
        own = GD.at[h, at("z", 0)]

        def body(i):
            DS[h, :88] = own[i].astype(f32) + a[i].astype(f32) + b[i].astype(f32)
            for j in range(4):
                block = DS[h, 22 * j : 22 * j + 24, :]
                YF[i * 4 + j, h] = block
                YS[i * 4 + j, h] = block.astype(bf16)

        loop(4, body)

    def second_stage(f):
        axis = "yx"[f]

        def add(got, h, k):
            own = F1.at[f, h, at(axis, k)]

            def body(rows):
                got[rows] = (got[rows].astype(f32) + own[rows]).astype(bf16)

            by_rows(body)

        return Scatter(axis, lambda h, k: B1.at[f, h, at(axis, k)], L2.at[f], add)

    second = [second_stage(f) for f in BOTH]

    def end_second(f, h):
        a, b = second[f].last(h)
        own = F1.at[f, h, at("yx"[f], 0)]

        def body(rows):
            F2[f, h, rows] = own[rows] + a[rows].astype(f32) + b[rows].astype(f32)

        by_rows(body)

    def arrive_pair(ring, t, short=False):
        for h, s in SHORT if short else LONG:
            ring.arrive(h, s, t)

    def begin(j, pair):
        for f in BOTH:
            for h, s in pair:
                first[f][j].first(h, s)

    def arrive_first(j):
        for f in BOTH:
            arrive_pair(first[f][j], 1)

    order = (2, 1, 3, 0)
    for j in order:
        begin(j, LONG)
    for j in order[:2]:
        begin(j, SHORT)
    for i in BOTH:
        loads["down", i].wait()

    def permute(i):
        rows = GR[:, pl.ds(pl.multiple_of(i * 352, 32), 352), :].reshape(ROWS, 512)
        out = jnp.dot(PF[...], rows, preferred_element_type=f32)
        for zz in range(Z):
            for h in BOTH:
                GD[h, zz, i] = out[88 * zz : 88 * zz + 88, 256 * h : 256 * h + 256].astype(bf16)

    loop(4, permute)
    down.start()
    for j, later in zip(order, order[2:]):
        arrive_first(j)
        begin(later, SHORT)
    arrive_first(3)
    arrive_pair(down, 1)
    layer, rest = split(row, 352)
    yy, rest = split(rest, 88)
    zz, r = split(rest, 11)
    one_hot(PB, zz * 88 + yy * 22 + layer * 11 + r)
    for h in BOTH:
        DS[h, 88:] = jnp.zeros((8, 256), f32)
    arrive_pair(down, 1, True)
    for f in BOTH:
        end_first(f, 2)
        for h, s in LONG:
            second[f].first(h, s)
    arrive_first(0)
    arrive_pair(down, 2)
    for f in BOTH:
        end_first(f, 1)
    arrive_pair(down, 2, True)
    for f in BOTH:
        end_first(f, 3)
        for h, s in SHORT:
            second[f].first(h, s)
    arrive_pair(down, 3)
    for f in BOTH:
        arrive_pair(second[f], 1)
    for f in BOTH:
        end_first(f, 0)
    for f in BOTH:
        for h in BOTH:
            end_second(f, h)

    for h in BOTH:
        for j in range(4):
            t0, t1 = (F2[f, h, 8 * j : 8 * j + 8, :] for f in BOTH)
            for i, block in enumerate((jnp.concatenate([t0[:4], t1[:4]], 0), jnp.concatenate([t0[4:], t1[4:]], 0))):
                ZF[2 * j + i, h] = block
                ZS[2 * j + i, h] = block.astype(bf16)
    far = (4, 3, 5, 2, 6, 1, 7)
    third = {k: send(ZS.at[at("z", k)], ZL.at[k], "z", k) for k in far}
    for h in BOTH:
        end_down(h)
    third_down = send_plane(lambda i, j: YS.at[at("x", i) * 4 + at("y", j)], lambda i, j: YL.at[i * 4 + j])
    for copy in reversed(third_down):
        copy.wait_recv()
    real = lax.broadcasted_iota(jnp.int32, (24, 256), 0) < 22
    squares = jnp.zeros((), f32)
    g_down = []
    for h in BOTH:
        total = YF[x * 4 + y, h]
        for k in range(1, 16):
            total = total + YL[k, h].astype(f32)
        total = jnp.where(real, total, 0.0).astype(bf16).astype(f32)
        g_down.append(total)
        squares += jnp.sum(total * total)
    for k in reversed(far):
        third[k].wait_recv()
    g_wide = []
    for h in BOTH:
        total = ZF[z, h]
        for k in range(1, 8):
            total = total + ZL[k, h].astype(f32)
        total = total.astype(bf16).astype(f32)
        g_wide.append(total)
        squares += jnp.sum(total * total)

    NS[...] = jnp.full((1, 128), squares, f32)
    NL[0] = NS[...]

    def norm_copy(src, dst, target):
        return pltpu.make_async_remote_copy(
            src_ref=src, dst_ref=dst, send_sem=nsem.at[0], recv_sem=nsem.at[1],
            device_id={"dp": target}, device_id_type=pl.DeviceIdType.MESH,
        )

    def tell(i):
        k = lax.rem(i + 63, 127) + 1
        norm_copy(NS, NL.at[k], lax.rem(d + k, 128)).start()

    loop(127, tell)
    others = NL.at[pl.ds(1, 127)]
    told = norm_copy(others, others, device("x", 1))
    told.wait_recv()
    total = jnp.sum(NL[...], axis=0)
    factor = jnp.minimum(1.0, 0.5 * lax.rsqrt(total / COUNT + 1e-30))[0:1, 0:1]

    def adamw(w, m, v, g):
        m = 0.9 * m + 0.1 * g
        v = 0.95 * v + 0.05 * g * g
        return (w - 0.02 * (m * lax.rsqrt(v + 1e-8) + 0.1 * w)).astype(bf16), m, v

    for copy in own_w:
        copy.wait()
    odd = d % 2 == 1
    for h in BOTH:
        w = [OW[h, i].astype(f32) for i in BOTH]
        w = jnp.concatenate([jnp.where(odd, one[4:], one[:4]) for one in w], 0)
        m, v = (jnp.concatenate([IW[i, h, 0], IW[i, h, 1]], 0) for i in BOTH)
        WZ[z, h], *new = adamw(w, m, v, g_wide[h] * factor)
        for i, one in enumerate(new):
            for layer in BOTH:
                MW[i, h, layer] = one[4 * layer : 4 * layer + 4]
    g = jnp.concatenate(g_down, 1) * factor
    for h in BOTH:
        DS[h, :24] = jnp.zeros((24, 256), f32)
    pick = lax.broadcasted_iota(jnp.int32, (24, 24), 1) == lax.broadcasted_iota(jnp.int32, (24, 24), 0) + (11 * d - low)
    pick = jnp.where(pick, 1.0, 0.0).astype(bf16)
    for layer in BOTH:
        w = jnp.dot(pick, OWD[layer], preferred_element_type=f32)[:11]
        w, *new = adamw(w, ID[0, :, layer, :], ID[1, :, layer, :], g[11 * layer : 11 * layer + 11])
        for i, one in enumerate(new):
            MD[i, :, layer, :] = one
        for h in BOTH:
            DS[h, 11 * layer : 11 * layer + 11, :] = w[:, 256 * h : 256 * h + 256].astype(f32)
    for h in BOTH:
        YW[x * 4 + y, h] = DS[h, :24].astype(bf16)

    wide_z = {k: send(WZ.at[z], WZ.at[z], "z", k) for k in far}
    mine = YW.at[x * 4 + y]
    down_plane = send_plane(lambda i, j: mine, lambda i, j: mine)
    for copy in reversed(down_plane):
        copy.wait_recv()
    for i in range(X):
        for h in BOTH:
            for j in range(Y):
                DS[h, 22 * j : 22 * j + 24, :] = YW[i * 4 + j, h].astype(f32)
            WD[h, z, i] = DS[h, :88].astype(bf16)
    down_z = Gather("z", lambda h, k: WD.at[h, at("z", k)])
    down_z.start()
    for k in reversed(far):
        wide_z[k].wait_recv()
    for h in BOTH:
        for layer in BOTH:
            rows = slice(4 * layer, 4 * layer + 4)
            for j in range(2):
                parts = [WZ[4 * j + i, h].astype(f32)[rows] for i in range(4)]
                WG[h, layer, x, y, 16 * j : 16 * j + 16, :] = jnp.concatenate(parts, 0).astype(bf16)
    near = [Gather("yx"[f], functools.partial(lambda f, h, k: unit(WG, f, h, 0, k), f)) for f in BOTH]
    wide = [[Gather("xy"[f], functools.partial(lambda f, j, h, k: unit(WG, f, h, k, j), f, j)) for j in range(4)] for f in BOTH]

    def spread(f, h, j):
        for s in WAYS[:: 1 - 2 * h]:
            wide[f][j % 4].push(h, s, 1)

    def arrive_near(t, pair):
        for f in BOTH:
            for h, s in pair:
                spread(f, h, near[f].arrive(h, s, t))

    def arrive_wide(j, t, pair):
        for f in BOTH:
            for h, s in pair:
                wide[f][j].arrive(h, s, t)

    for ring in near:
        ring.start()
    for f in BOTH:
        for h in BOTH:
            spread(f, h, 0)
    arrive_near(1, LONG)
    arrive_near(1, SHORT)
    arrive_pair(down_z, 1)
    arrive_wide(0, 1, LONG)
    arrive_near(2, LONG)
    arrive_pair(down_z, 1, True)
    for j in (1, 3):
        arrive_wide(j, 1, LONG)
    arrive_pair(down_z, 2)
    arrive_pair(down_z, 2, True)
    arrive_wide(2, 1, LONG)
    arrive_pair(down_z, 3)
    arrive_pair(down_z, 3, True)
    arrive_pair(down_z, 4)

    def restore(i):
        for h in BOTH:
            rows = WD[h, :, i].astype(f32).reshape(ROWS, 256).astype(bf16)
            out = jnp.dot(PB[...], rows, preferred_element_type=f32).astype(bf16)
            for layer in BOTH:
                OD[layer, pl.ds(pl.multiple_of(i * 352, 32), 352), 256 * h : 256 * h + 256] = out[352 * layer : 352 * layer + 352]

    loop(4, restore)
    for j in range(4):
        arrive_wide(j, 1, SHORT)
        arrive_wide(j, 2, LONG)
    for copy in pending:
        copy.wait_send()
    told.wait_send()


def finish(W, OD, MW, MD, *rest):
    sem = rest[-1]
    sources = [W.at[0], W.at[1], OD] + [r for i in BOTH for r in (MW.at[i, 0], MW.at[i, 1], MD.at[i])]
    copies = [pltpu.make_async_copy(src, dst, sem.at[i]) for i, (src, dst) in enumerate(zip(sources, rest))]
    for copy in copies:
        copy.start()
    for copy in copies:
        copy.wait()


def step_kernel(*args):
    hbm, vmem = pl.BlockSpec(memory_space=pl.ANY), pl.BlockSpec(memory_space=pltpu.VMEM)
    wide, deep = (2, 4, F), (11, 2, 512)
    unit, half = (4, 32, F), (4, 88, 256)
    pair, square, whole_down = (2, 2), (4, *unit), (2, 8, *half)
    blocks, small = (8, 2, 8, F), (16, 2, 24, 256)
    shape = jax.ShapeDtypeStruct
    out = pl.pallas_call(
        kernel,
        out_shape=(pltpu.VMEM((*pair, *square), bf16), pltpu.VMEM((2, F, 512), bf16), pltpu.VMEM((*pair, *wide), f32), pltpu.VMEM((2, *deep), f32)),
        in_specs=[hbm] * 12,
        out_specs=(vmem,) * 4,
        scratch_shapes=[
            pltpu.VMEM((*pair, *square), bf16),
            pltpu.VMEM((2, F, 512), bf16),
            pltpu.VMEM(whole_down, bf16),
            pltpu.VMEM((2, 4, 6, *unit[1:]), bf16),
            pltpu.VMEM((*pair, *unit), f32),
            pltpu.VMEM((*pair, *unit), bf16),
            pltpu.VMEM((2, 6, *unit[1:]), bf16),
            pltpu.VMEM((*pair, *unit[1:]), f32),
            pltpu.VMEM(blocks, bf16),
            pltpu.VMEM(blocks, f32),
            pltpu.VMEM(blocks, bf16),
            pltpu.VMEM((14, *half), bf16),
            pltpu.VMEM((2, 96, 256), f32),
            pltpu.VMEM(small, bf16),
            pltpu.VMEM(small, f32),
            pltpu.VMEM(small, bf16),
            pltpu.VMEM((1, 128), f32),
            pltpu.VMEM((128, 1, 128), f32),
            pltpu.VMEM(whole_down, bf16),
            pltpu.VMEM(blocks, bf16),
            pltpu.VMEM(small, bf16),
            pltpu.VMEM((ROWS, ROWS), bf16),
            pltpu.VMEM((ROWS, ROWS), bf16),
            pltpu.VMEM((*pair, 8, F), bf16),
            pltpu.VMEM((2, 24, 512), bf16),
            pltpu.VMEM((*pair, *wide), f32),
            pltpu.VMEM((2, *deep), f32),
            pltpu.SemaphoreType.DMA((SEMS,)),
            pltpu.SemaphoreType.DMA((SEMS,)),
            pltpu.SemaphoreType.DMA((LOADS,)),
            pltpu.SemaphoreType.DMA((9,)),
            pltpu.SemaphoreType.DMA((2,)),
        ],
        compiler_params=pltpu.CompilerParams(collective_id=0, has_side_effects=True, vmem_limit_bytes=50 * 2**20),
        name="clipped_step",
    )(*args)
    out = [pltpu.with_memory_space_constraint(one, pltpu.VMEM) for one in out]
    return pl.pallas_call(
        finish,
        out_shape=(shape((2, *square), bf16),) * 2 + (shape((2, F, 512), bf16),) + (shape(wide, f32), shape(wide, f32), shape(deep, f32)) * 2,
        in_specs=[vmem] * 4,
        out_specs=(hbm,) * 9,
        scratch_shapes=[pltpu.SemaphoreType.DMA((9,))],
        compiler_params=pltpu.CompilerParams(vmem_limit_bytes=50 * 2**20),
        name="finish",
    )(*out)


def solution(mesh):
    def step(gg, gu, gd, wg, wu, wd, mg, mu, md, vg, vu, vd):
        gg, gu = (g.reshape(2, 4, 4, 32, F) for g in (gg, gu))
        md, vd = (a.transpose(1, 0, 2) for a in (md, vd))
        og, ou, od, omg, omu, omd, ovg, ovu, ovd = step_kernel(gg, gu, gd[0], wg, wu, wd, mg, mu, md, vg, vu, vd)
        og, ou = (o.reshape(2, 512, F) for o in (og, ou))
        omd, ovd = (a.transpose(1, 0, 2) for a in (omd, ovd))
        return og, ou, od, omg, omu, omd, ovg, ovu, ovd

    all_of, cut = P(None, None, None), P(None, "dp", None)
    return jax.shard_map(
        step,
        mesh=mesh,
        in_specs=(P(("rep", "dp"), None, None, None),) * 3 + (all_of,) * 3 + (cut,) * 6,
        out_specs=(P("rep", None, None),) * 3 + (P("rep", "dp", None),) * 6,
        check_vma=False,
    )
```

```python
import functools

import jax
import jax.numpy as jnp
import numpy as np
from jax import lax
from jax.experimental import pallas as pl
from jax.experimental.pallas import tpu as pltpu
from jax.sharding import PartitionSpec as P

X, Y, Z = 4, 4, 8
F = 1408
COUNT = 3 * 2 * 512 * F
SEMS = 320
LOADS = 32
ROWS = 704
f32, bf16 = jnp.float32, jnp.bfloat16
BOTH = (0, 1)
WAYS = (1, -1)
LONG = ((0, 1), (1, -1))
SHORT = ((1, 1), (0, -1))


def chains(n):
    return [(*one, n // 2) for one in LONG] + [(*one, n // 2 - 1) for one in SHORT]


def slots(n):
    return {key: i for i, key in enumerate((h, s, t) for h, s, length in chains(n) for t in range(1, length + 1))}


def one_hots():
    rows = np.arange(ROWS).reshape(2, 4, 8, 11).transpose(2, 1, 0, 3).reshape(-1)
    forth = rows[:, None] == np.arange(ROWS)
    return [jnp.asarray(p, bf16) for p in (forth, forth.T)]


def loop(n, body):
    def step(i, carry):
        body(i)
        return carry

    lax.fori_loop(0, n, step, 0)


def kernel(pf, pb, gg, gu, gd, wg, wu, wd, mg, mu, md, vg, vu, vd, WG, OD, MW, MD, *scratch):
    (G, GR, GD, L1, F1, B1, L2, F2, ZS, ZF, ZL, LZ, DS, YS, YF, YL, NS, NL, WD, WZ, YW, PF, PB, OW, OWD, IW, ID) = scratch[:-4]
    ssem, rsem, lsem, wsem = scratch[-4:]
    d = lax.axis_index("dp")
    x, y, z = d // 32, (d // 8) % 4, d % 8
    place = {"x": (x, 4), "y": (y, 4), "z": (z, 8)}

    def at(axis, k):
        p, n = place[axis]
        return lax.rem(p + (k + n) % n, n)

    def device(axis, k):
        p = at(axis, k)
        return {"x": p * 32 + y * 8 + z, "y": x * 32 + p * 8 + z, "z": x * 32 + y * 8 + p}[axis]

    barrier = pltpu.get_barrier_semaphore()
    for axis in place:
        for way in WAYS:
            pl.semaphore_signal(barrier, inc=1, device_id={"dp": device(axis, way)}, device_id_type=pl.DeviceIdType.MESH)

    used = [0]
    pending = []

    def send_to(target, src, dst):
        i = used[0]
        used[0] += 1
        copy = pltpu.make_async_remote_copy(
            src_ref=src, dst_ref=dst, send_sem=ssem.at[i], recv_sem=rsem.at[i],
            device_id={"dp": target}, device_id_type=pl.DeviceIdType.MESH,
        )
        copy.start()
        pending.append(copy)
        return copy

    def send(src, dst, axis, k):
        return send_to(device(axis, k), src, dst)

    def send_plane(i, source, target):
        ks = [k for k in (2, 1, 3, 0) if i or k]
        return {(i, k): send_to(at("x", i) * 32 + at("y", k) * 8 + z, source(k), target(k)) for k in ks}

    loads = {}

    def load(key, src, dst):
        copy = pltpu.make_async_copy(src, dst, lsem.at[len(loads)])
        copy.start()
        loads[key] = copy

    class Scatter:
        def __init__(self, axis, own, landing, add, need=None):
            self.axis, self.own, self.landing, self.add, self.need = axis, own, landing, add, need
            self.n = place[axis][1]
            self.length = {(h, s): length for h, s, length in chains(self.n)}
            self.slot = slots(self.n)
            self.copies = {}

        def at(self, h, s, t):
            return self.landing.at[self.slot[h, s, t]]

        def first(self, h, s):
            k = s * self.length[h, s]
            if self.need:
                self.need(h, k)
            self.copies[h, s, 1] = send(self.own(h, k), self.at(h, s, 1), self.axis, s)

        def start(self):
            for h, s, _ in chains(self.n):
                self.first(h, s)

        def arrive(self, h, s, t):
            self.copies[h, s, t].wait_recv()
            if t < self.length[h, s]:
                k = s * (self.length[h, s] - t)
                if self.need:
                    self.need(h, k)
                self.add(self.at(h, s, t), h, k)
                self.copies[h, s, t + 1] = send(self.at(h, s, t), self.at(h, s, t + 1), self.axis, s)

        def last(self, h):
            for s in WAYS:
                self.arrive(h, s, self.length[h, s])
            return [self.at(h, s, self.length[h, s]) for s in WAYS]

    class Gather:
        def __init__(self, axis, part):
            self.axis, self.part = axis, part
            self.n = place[axis][1]
            self.length = {(h, s): length for h, s, length in chains(self.n)}
            self.copies = {}

        def push(self, h, s, t):
            ref = self.part(h, -s * (t - 1))
            self.copies[h, s, t] = send(ref, ref, self.axis, s)

        def start(self):
            for h, s, _ in chains(self.n):
                self.push(h, s, 1)

        def arrive(self, h, s, t):
            self.copies[h, s, t].wait_recv()
            if t < self.length[h, s]:
                self.push(h, s, t + 1)
            return -s * t

    def load_wide(f, h, k):
        if f == 0:
            load((f, h, k), (gg, gu)[h].at[0, at("x", k)], G.at[h, 0, at("x", k)])
        else:
            load((f, h, k), (gg, gu)[h].at[1, :, at("y", k)], G.at[h, 1, :, at("y", k)])

    for h in BOTH:
        for f in BOTH:
            load_wide(f, h, 2)
    load(("down", 2), pf, PF)
    for i in BOTH:
        load(("down", i), gd.at[i], GR.at[i])
    for h, k in ((1, 1), (0, 3), (0, 1), (1, 3), (0, 0), (1, 0)):
        for f in BOTH:
            load_wide(f, h, k)
    load(("back", 0), pb, PB)
    mine = pl.multiple_of(8 * (d // 2), 8)
    low = pl.multiple_of(8 * ((11 * d) // 8) - 8 * (d // 127), 8)
    own_w = [pltpu.make_async_copy(w.at[:, pl.ds(mine, 8), :], OW.at[i], wsem.at[i]) for i, w in enumerate((wg, wu))]
    own_w.append(pltpu.make_async_copy(wd.at[:, pl.ds(low, 24), :], OWD, wsem.at[2]))
    for i, (wide_, deep_) in enumerate((((mg, mu), md), ((vg, vu), vd))):
        for h in BOTH:
            own_w.append(pltpu.make_async_copy(wide_[h], IW.at[i, h], wsem.at[len(own_w)]))
        own_w.append(pltpu.make_async_copy(deep_, ID.at[i], wsem.at[len(own_w)]))
    for copy in own_w:
        copy.start()
    ready = set()

    def need(f, n):
        def wait(h, k):
            key = (f, h, k % n)
            if key not in ready:
                ready.add(key)
                loads[key].wait()

        return wait

    pl.semaphore_wait(barrier, 2 * len(place))

    def unit(ref, f, h, k, j):
        return ref.at[h, 0, at("x", k), at("y", j)] if f == 0 else ref.at[h, 1, at("x", j), at("y", k)]

    def by_rows(body):
        loop(2, lambda i: body(pl.ds(pl.multiple_of(i * 16, 16), 16)))

    def first_stage(f, j):
        def add(got, h, k):
            own = unit(G, f, h, k, j)

            def body(rows):
                got[rows] = (got[rows].astype(f32) + own[rows].astype(f32)).astype(bf16)

            by_rows(body)

        return Scatter("xy"[f], lambda h, k: unit(G, f, h, k, j), L1.at[f, j], add, need(f, 4))

    first = [[first_stage(f, j) for j in range(4)] for f in BOTH]

    def end_first(f, j):
        for h in BOTH:
            a, b = first[f][j].last(h)
            need(f, 4)(h, 0)
            own = unit(G, f, h, 0, j)
            place_j = at("yx"[f], j)
            travels = j == 2 or j == (3, 1)[h]

            def body(rows):
                total = own[rows].astype(f32) + a[rows].astype(f32) + b[rows].astype(f32)
                if travels:
                    B1[f, h, place_j, rows] = total.astype(bf16)
                else:
                    F1[f, h, place_j, rows] = total

            by_rows(body)

    def down_stage(j):
        def own(h, k):
            return GD.at[h, at("z", k), at("x", j)]

        def add(got, h, k):
            got[...] = (got[...].astype(f32) + own(h, k)[...].astype(f32)).astype(bf16)

        return Scatter("z", own, LZ.at[j], add)

    down = [down_stage(j) for j in range(X)]

    def end_down(j):
        i = at("x", j)
        for h in BOTH:
            a, b = down[j].last(h)
            DS[h, :88] = GD[h, z, i].astype(f32) + a[...].astype(f32) + b[...].astype(f32)
            for yy in range(Y):
                block = DS[h, 22 * yy : 22 * yy + 24, :]
                YS[i * 4 + yy, h] = block.astype(bf16)
                if j == 0:
                    YF[yy, h] = block
        return send_plane(j, lambda k: YS.at[i * 4 + at("y", k)], lambda k: YL.at[j * 4 + k])

    def second_stage(f):
        axis = "yx"[f]

        def add(got, h, k):
            own = F1.at[f, h, at(axis, k)]

            def body(rows):
                got[rows] = (got[rows].astype(f32) + own[rows]).astype(bf16)

            by_rows(body)

        return Scatter(axis, lambda h, k: B1.at[f, h, at(axis, k)], L2.at[f], add)

    second = [second_stage(f) for f in BOTH]

    def end_second(f, h):
        a, b = second[f].last(h)
        own = F1.at[f, h, at("yx"[f], 0)]

        def body(rows):
            F2[f, h, rows] = own[rows] + a[rows].astype(f32) + b[rows].astype(f32)

        by_rows(body)

    def arrive_pair(ring, t, short=False):
        for h, s in SHORT if short else LONG:
            ring.arrive(h, s, t)

    def begin(j, pair):
        for f in BOTH:
            for h, s in pair:
                first[f][j].first(h, s)

    def arrive_first(j):
        for f in BOTH:
            arrive_pair(first[f][j], 1)

    def arrive_down(t, short=False):
        for j in order:
            arrive_pair(down[j], t, short)

    order = (2, 1, 3, 0)
    for j in order:
        begin(j, LONG)
    for j in order[:2]:
        begin(j, SHORT)
    for i in range(3):
        loads["down", i].wait()

    def permute(j):
        i = at("x", j)
        rows = GR[:, pl.ds(pl.multiple_of(i * 352, 32), 352), :].reshape(ROWS, 512)
        out = jnp.dot(PF[...], rows, preferred_element_type=f32)
        for zz in range(Z):
            for h in BOTH:
                GD[h, zz, i] = out[88 * zz : 88 * zz + 88, 256 * h : 256 * h + 256].astype(bf16)

    for j in order:
        permute(j)
        down[j].start()
    for j, later in zip(order, order[2:]):
        arrive_first(j)
        begin(later, SHORT)
    arrive_first(3)
    arrive_down(1)
    for h in BOTH:
        DS[h, 88:] = jnp.zeros((8, 256), f32)
    arrive_down(1, True)
    for f in BOTH:
        end_first(f, 2)
        for h, s in LONG:
            second[f].first(h, s)
    arrive_first(0)
    arrive_down(2)
    for f in BOTH:
        end_first(f, 1)
    arrive_down(2, True)
    for f in BOTH:
        end_first(f, 3)
        for h, s in SHORT:
            second[f].first(h, s)
    arrive_down(3)
    for f in BOTH:
        arrive_pair(second[f], 1)
    for f in BOTH:
        end_first(f, 0)
    far = (4, 3, 5, 2, 6, 1, 7)
    third = []
    for h in BOTH:
        for f in BOTH:
            end_second(f, h)
        for j in range(4):
            t0, t1 = (F2[f, h, 8 * j : 8 * j + 8, :] for f in BOTH)
            for i, block in enumerate((jnp.concatenate([t0[:4], t1[:4]], 0), jnp.concatenate([t0[4:], t1[4:]], 0))):
                ZF[2 * j + i, h] = block
                ZS[2 * j + i, h] = block.astype(bf16)
        third.append({k: send(ZS.at[at("z", k), h], ZL.at[k, h], "z", k) for k in far})
    third_down = {}
    for j in order:
        third_down.update(end_down(j))
    for copy in third_down.values():
        copy.wait_recv()
    real = lax.broadcasted_iota(jnp.int32, (24, 256), 0) < 22
    squares = jnp.zeros((), f32)
    g_down = []
    for h in BOTH:
        total = YF[y, h]
        for k in range(1, 16):
            total = total + YL[k, h].astype(f32)
        total = jnp.where(real, total, 0.0).astype(bf16).astype(f32)
        g_down.append(total)
        squares += jnp.sum(total * total)
    g_wide = []
    for h in BOTH:
        for k in reversed(far):
            third[h][k].wait_recv()
        total = ZF[z, h]
        for k in range(1, 8):
            total = total + ZL[k, h].astype(f32)
        total = total.astype(bf16).astype(f32)
        g_wide.append(total)
        squares += jnp.sum(total * total)

    total = jnp.full((1, 128), squares, f32)
    NS[0] = total
    told = {}
    for i in order:
        told.update(send_plane(i, lambda k: NS.at[0], lambda k: NL.at[i * 4 + k]))
    for copy in told.values():
        copy.wait_recv()
    for k in range(1, 16):
        total = total + NL[k]
    NS[1] = total
    told = {k: send(NS.at[1], NL.at[16 + k], "z", k) for k in far}
    for k in reversed(far):
        told[k].wait_recv()
    for k in range(1, 8):
        total = total + NL[16 + k]
    factor = jnp.minimum(1.0, 0.5 * lax.rsqrt(total / COUNT + 1e-30))[0:1, 0:1]

    def adamw(w, m, v, g):
        m = 0.9 * m + 0.1 * g
        v = 0.95 * v + 0.05 * g * g
        return (w - 0.02 * (m * lax.rsqrt(v + 1e-8) + 0.1 * w)).astype(bf16), m, v

    for copy in own_w:
        copy.wait()
    odd = d % 2 == 1
    for h in BOTH:
        w = [OW[h, i].astype(f32) for i in BOTH]
        w = jnp.concatenate([jnp.where(odd, one[4:], one[:4]) for one in w], 0)
        m, v = (jnp.concatenate([IW[i, h, 0], IW[i, h, 1]], 0) for i in BOTH)
        WZ[z, h], *new = adamw(w, m, v, g_wide[h] * factor)
        for i, one in enumerate(new):
            for layer in BOTH:
                MW[i, h, layer] = one[4 * layer : 4 * layer + 4]
    g = jnp.concatenate(g_down, 1) * factor
    for h in BOTH:
        DS[h, :24] = jnp.zeros((24, 256), f32)
    pick = lax.broadcasted_iota(jnp.int32, (24, 24), 1) == lax.broadcasted_iota(jnp.int32, (24, 24), 0) + (11 * d - low)
    pick = jnp.where(pick, 1.0, 0.0).astype(bf16)
    for layer in BOTH:
        w = jnp.dot(pick, OWD[layer], preferred_element_type=f32)[:11]
        w, *new = adamw(w, ID[0, :, layer, :], ID[1, :, layer, :], g[11 * layer : 11 * layer + 11])
        for i, one in enumerate(new):
            MD[i, :, layer, :] = one
        for h in BOTH:
            DS[h, 11 * layer : 11 * layer + 11, :] = w[:, 256 * h : 256 * h + 256].astype(f32)
    for h in BOTH:
        YW[x * 4 + y, h] = DS[h, :24].astype(bf16)

    wide_z = [{k: send(WZ.at[z, h], WZ.at[z, h], "z", k) for k in far} for h in BOTH]
    mine = YW.at[x * 4 + y]
    plane = {}
    for i in (0, 2, 1, 3):
        plane.update(send_plane(i, lambda k: mine, lambda k: mine))
    down = [Gather("z", functools.partial(lambda j, h, k: WD.at[h, at("z", k), at("x", j)], j)) for j in range(X)]

    def begin_down(j):
        for k in range(Y):
            if (j, k) != (0, 0):
                plane[-j % 4, k].wait_recv()
        i = at("x", j)
        for h in BOTH:
            for yy in range(Y):
                DS[h, 22 * yy : 22 * yy + 24, :] = YW[i * 4 + yy, h].astype(f32)
            WD[h, z, i] = DS[h, :88].astype(bf16)
        down[j].start()

    def begin_wide(h):
        for k in reversed(far):
            wide_z[h][k].wait_recv()
        for layer in BOTH:
            rows = slice(4 * layer, 4 * layer + 4)
            for j in range(2):
                parts = [WZ[4 * j + i, h].astype(f32)[rows] for i in range(4)]
                WG[h, layer, x, y, 16 * j : 16 * j + 16, :] = jnp.concatenate(parts, 0).astype(bf16)

    near = [Gather("yx"[f], functools.partial(lambda f, h, k: unit(WG, f, h, 0, k), f)) for f in BOTH]
    wide = [[Gather("xy"[f], functools.partial(lambda f, j, h, k: unit(WG, f, h, k, j), f, j)) for j in range(4)] for f in BOTH]

    def spread(f, h, j):
        for s in WAYS[:: 1 - 2 * h]:
            wide[f][j % 4].push(h, s, 1)

    def arrive_near(t, pair):
        for f in BOTH:
            for h, s in pair:
                spread(f, h, near[f].arrive(h, s, t))

    def arrive_wide(j, t, pair):
        for f in BOTH:
            for h, s in pair:
                wide[f][j].arrive(h, s, t)

    begin_down(0)
    for h in BOTH:
        begin_wide(h)
        for f in BOTH:
            for s in WAYS[:: 1 - 2 * h]:
                near[f].push(h, s, 1)
        for f in BOTH:
            spread(f, h, 0)
        if h == 0:
            for j in order[:3]:
                begin_down(j)
    arrive_near(1, LONG)
    arrive_near(1, SHORT)
    arrive_down(1)
    arrive_wide(0, 1, LONG)
    arrive_near(2, LONG)
    arrive_down(1, True)
    for j in (1, 3):
        arrive_wide(j, 1, LONG)
    arrive_down(2)
    arrive_down(2, True)
    arrive_wide(2, 1, LONG)
    arrive_down(3)
    loads["back", 0].wait()
    for j in (0, 2, 1, 3):
        arrive_pair(down[j], 3, True)
        arrive_pair(down[j], 4)
        i = at("x", j)
        for h in BOTH:
            rows = WD[h, :, i].astype(f32).reshape(ROWS, 256).astype(bf16)
            out = jnp.dot(PB[...], rows, preferred_element_type=f32).astype(bf16)
            for layer in BOTH:
                OD[layer, pl.ds(pl.multiple_of(i * 352, 32), 352), 256 * h : 256 * h + 256] = out[352 * layer : 352 * layer + 352]
        arrive_wide(j, 1, SHORT)
        arrive_wide(j, 2, LONG)
    for copy in pending:
        copy.wait_send()


def finish(W, OD, MW, MD, *rest):
    sem = rest[-1]
    sources = [W.at[0], W.at[1], OD] + [r for i in BOTH for r in (MW.at[i, 0], MW.at[i, 1], MD.at[i])]
    copies = [pltpu.make_async_copy(src, dst, sem.at[i]) for i, (src, dst) in enumerate(zip(sources, rest))]
    for copy in copies:
        copy.start()
    for copy in copies:
        copy.wait()


def step_kernel(*args):
    hbm, vmem = pl.BlockSpec(memory_space=pl.ANY), pl.BlockSpec(memory_space=pltpu.VMEM)
    wide, deep = (2, 4, F), (11, 2, 512)
    unit, half = (4, 32, F), (4, 88, 256)
    pair, square, whole_down = (2, 2), (4, *unit), (2, 8, *half)
    blocks, small = (8, 2, 8, F), (16, 2, 24, 256)
    shape = jax.ShapeDtypeStruct
    out = pl.pallas_call(
        kernel,
        out_shape=(pltpu.VMEM((*pair, *square), bf16), pltpu.VMEM((2, F, 512), bf16), pltpu.VMEM((*pair, *wide), f32), pltpu.VMEM((2, *deep), f32)),
        in_specs=[hbm] * 14,
        out_specs=(vmem,) * 4,
        scratch_shapes=[
            pltpu.VMEM((*pair, *square), bf16),
            pltpu.VMEM((2, F, 512), bf16),
            pltpu.VMEM(whole_down, bf16),
            pltpu.VMEM((2, 4, 6, *unit[1:]), bf16),
            pltpu.VMEM((*pair, *unit), f32),
            pltpu.VMEM((*pair, *unit), bf16),
            pltpu.VMEM((2, 6, *unit[1:]), bf16),
            pltpu.VMEM((*pair, *unit[1:]), f32),
            pltpu.VMEM(blocks, bf16),
            pltpu.VMEM(blocks, f32),
            pltpu.VMEM(blocks, bf16),
            pltpu.VMEM((4, 14, *half[1:]), bf16),
            pltpu.VMEM((2, 96, 256), f32),
            pltpu.VMEM(small, bf16),
            pltpu.VMEM((4, *small[1:]), f32),
            pltpu.VMEM(small, bf16),
            pltpu.VMEM((2, 1, 128), f32),
            pltpu.VMEM((24, 1, 128), f32),
            pltpu.VMEM(whole_down, bf16),
            pltpu.VMEM(blocks, bf16),
            pltpu.VMEM(small, bf16),
            pltpu.VMEM((ROWS, ROWS), bf16),
            pltpu.VMEM((ROWS, ROWS), bf16),
            pltpu.VMEM((*pair, 8, F), bf16),
            pltpu.VMEM((2, 24, 512), bf16),
            pltpu.VMEM((*pair, *wide), f32),
            pltpu.VMEM((2, *deep), f32),
            pltpu.SemaphoreType.DMA((SEMS,)),
            pltpu.SemaphoreType.DMA((SEMS,)),
            pltpu.SemaphoreType.DMA((LOADS,)),
            pltpu.SemaphoreType.DMA((9,)),
        ],
        compiler_params=pltpu.CompilerParams(collective_id=0, has_side_effects=True, vmem_limit_bytes=50 * 2**20),
        name="clipped_step",
    )(*one_hots(), *args)
    out = [pltpu.with_memory_space_constraint(one, pltpu.VMEM) for one in out]
    return pl.pallas_call(
        finish,
        out_shape=(shape((2, *square), bf16),) * 2 + (shape((2, F, 512), bf16),) + (shape(wide, f32), shape(wide, f32), shape(deep, f32)) * 2,
        in_specs=[vmem] * 4,
        out_specs=(hbm,) * 9,
        scratch_shapes=[pltpu.SemaphoreType.DMA((9,))],
        compiler_params=pltpu.CompilerParams(vmem_limit_bytes=50 * 2**20),
        name="finish",
    )(*out)


def solution(mesh):
    def step(gg, gu, gd, wg, wu, wd, mg, mu, md, vg, vu, vd):
        gg, gu = (g.reshape(2, 4, 4, 32, F) for g in (gg, gu))
        md, vd = (a.transpose(1, 0, 2) for a in (md, vd))
        og, ou, od, omg, omu, omd, ovg, ovu, ovd = step_kernel(gg, gu, gd[0], wg, wu, wd, mg, mu, md, vg, vu, vd)
        og, ou = (o.reshape(2, 512, F) for o in (og, ou))
        omd, ovd = (a.transpose(1, 0, 2) for a in (omd, ovd))
        return og, ou, od, omg, omu, omd, ovg, ovu, ovd

    all_of, cut = P(None, None, None), P(None, "dp", None)
    return jax.shard_map(
        step,
        mesh=mesh,
        in_specs=(P(("rep", "dp"), None, None, None),) * 3 + (all_of,) * 3 + (cut,) * 6,
        out_specs=(P("rep", None, None),) * 3 + (P("rep", "dp", None),) * 6,
        check_vma=False,
    )
```

```python
import functools

import jax
import jax.numpy as jnp
import numpy as np
from jax import lax
from jax.experimental import pallas as pl
from jax.experimental.pallas import tpu as pltpu
from jax.sharding import PartitionSpec as P

X, Y, Z = 4, 4, 8
F = 1408
COUNT = 3 * 2 * 512 * F
SEMS = 320
LOADS = 32
ROWS = 704
f32, bf16 = jnp.float32, jnp.bfloat16
BOTH = (0, 1)
WAYS = (1, -1)
LONG = ((0, 1), (1, -1))
SHORT = ((1, 1), (0, -1))


def chains(n):
    return [(*one, n // 2) for one in LONG] + [(*one, n // 2 - 1) for one in SHORT]


def slots(n):
    return {key: i for i, key in enumerate((h, s, t) for h, s, length in chains(n) for t in range(1, length + 1))}


def one_hots():
    rows = np.arange(ROWS).reshape(2, 4, 8, 11).transpose(2, 1, 0, 3).reshape(-1)
    forth = rows[:, None] == np.arange(ROWS)
    return [jnp.asarray(p, bf16) for p in (forth, forth.T)]


def loop(n, body):
    def step(i, carry):
        body(i)
        return carry

    lax.fori_loop(0, n, step, 0)


def kernel(pf, pb, gg, gu, gd, wg, wu, wd, mg, mu, md, vg, vu, vd, WG, OD, MW, MD, *scratch):
    (G, GR, GD, L1, F1, B1, L2, F2, ZS, ZF, ZL, LZ, DS, YS, YF, YL, NS, NL, WD, WZ, YW, PF, PB, OW, OWD, IW, ID) = scratch[:-4]
    ssem, rsem, lsem, wsem = scratch[-4:]
    d = lax.axis_index("dp")
    x, y, z = d // 32, (d // 8) % 4, d % 8
    place = {"x": (x, 4), "y": (y, 4), "z": (z, 8)}

    def at(axis, k):
        p, n = place[axis]
        return lax.rem(p + (k + n) % n, n)

    def device(axis, k):
        p = at(axis, k)
        return {"x": p * 32 + y * 8 + z, "y": x * 32 + p * 8 + z, "z": x * 32 + y * 8 + p}[axis]

    barrier = pltpu.get_barrier_semaphore()
    for axis in place:
        for way in WAYS:
            pl.semaphore_signal(barrier, inc=1, device_id={"dp": device(axis, way)}, device_id_type=pl.DeviceIdType.MESH)

    used = [0]
    pending = []

    def send_to(target, src, dst):
        i = used[0]
        used[0] += 1
        copy = pltpu.make_async_remote_copy(
            src_ref=src, dst_ref=dst, send_sem=ssem.at[i], recv_sem=rsem.at[i],
            device_id={"dp": target}, device_id_type=pl.DeviceIdType.MESH,
        )
        copy.start()
        pending.append(copy)
        return copy

    def send(src, dst, axis, k):
        return send_to(device(axis, k), src, dst)

    def send_plane(i, source, target):
        ks = [k for k in (2, 1, 3, 0) if i or k]
        return {(i, k): send_to(at("x", i) * 32 + at("y", k) * 8 + z, source(k), target(k)) for k in ks}

    loads = {}

    def load(key, src, dst):
        copy = pltpu.make_async_copy(src, dst, lsem.at[len(loads)])
        copy.start()
        loads[key] = copy

    class Scatter:
        def __init__(self, axis, own, landing, add, need=None):
            self.axis, self.own, self.landing, self.add, self.need = axis, own, landing, add, need
            self.n = place[axis][1]
            self.length = {(h, s): length for h, s, length in chains(self.n)}
            self.slot = slots(self.n)
            self.copies = {}

        def at(self, h, s, t):
            return self.landing.at[self.slot[h, s, t]]

        def first(self, h, s):
            k = s * self.length[h, s]
            if self.need:
                self.need(h, k)
            self.copies[h, s, 1] = send(self.own(h, k), self.at(h, s, 1), self.axis, s)

        def start(self):
            for h, s, _ in chains(self.n):
                self.first(h, s)

        def arrive(self, h, s, t):
            self.copies[h, s, t].wait_recv()
            if t < self.length[h, s]:
                k = s * (self.length[h, s] - t)
                if self.need:
                    self.need(h, k)
                self.add(self.at(h, s, t), h, k)
                self.copies[h, s, t + 1] = send(self.at(h, s, t), self.at(h, s, t + 1), self.axis, s)

        def last(self, h):
            for s in WAYS:
                self.arrive(h, s, self.length[h, s])
            return [self.at(h, s, self.length[h, s]) for s in WAYS]

    class Gather:
        def __init__(self, axis, part):
            self.axis, self.part = axis, part
            self.n = place[axis][1]
            self.length = {(h, s): length for h, s, length in chains(self.n)}
            self.copies = {}

        def push(self, h, s, t):
            ref = self.part(h, -s * (t - 1))
            self.copies[h, s, t] = send(ref, ref, self.axis, s)

        def start(self):
            for h, s, _ in chains(self.n):
                self.push(h, s, 1)

        def arrive(self, h, s, t):
            self.copies[h, s, t].wait_recv()
            if t < self.length[h, s]:
                self.push(h, s, t + 1)
            return -s * t

    def load_wide(f, h, k):
        if f == 0:
            load((f, h, k), (gg, gu)[h].at[0, at("x", k)], G.at[h, 0, at("x", k)])
        else:
            load((f, h, k), (gg, gu)[h].at[1, :, at("y", k)], G.at[h, 1, :, at("y", k)])

    for h, k in ((0, 2), (1, 2), (1, 1), (0, 3)):
        for f in BOTH:
            load_wide(f, h, k)
    load(("down", 2), pf, PF)
    for i in BOTH:
        load(("down", i), gd.at[i], GR.at[i])
    low = pl.multiple_of(8 * ((11 * d) // 8) - 8 * (d // 127), 8)
    own_w = []

    def load_rest():
        for h, k in ((0, 1), (1, 3), (0, 0), (1, 0)):
            for f in BOTH:
                load_wide(f, h, k)
        load(("back", 0), pb, PB)
        mine = pl.multiple_of(8 * (d // 2), 8)
        pairs = [(w.at[:, pl.ds(mine, 8), :], OW.at[i]) for i, w in enumerate((wg, wu))]
        pairs.append((wd.at[:, pl.ds(low, 24), :], OWD))
        for i, (wide_, deep_) in enumerate((((mg, mu), md), ((vg, vu), vd))):
            pairs += [(wide_[h], IW.at[i, h]) for h in BOTH]
            pairs.append((deep_, ID.at[i]))
        for src, dst in pairs:
            own_w.append(pltpu.make_async_copy(src, dst, wsem.at[len(own_w)]))
            own_w[-1].start()

    ready = set()

    def need(f, n):
        def wait(h, k):
            key = (f, h, k % n)
            if key not in ready:
                ready.add(key)
                loads[key].wait()

        return wait

    pl.semaphore_wait(barrier, 2 * len(place))

    def unit(ref, f, h, k, j):
        return ref.at[h, 0, at("x", k), at("y", j)] if f == 0 else ref.at[h, 1, at("x", j), at("y", k)]

    def by_rows(body):
        loop(2, lambda i: body(pl.ds(pl.multiple_of(i * 16, 16), 16)))

    def first_stage(f, j):
        def add(got, h, k):
            own = unit(G, f, h, k, j)

            def body(rows):
                got[rows] = (got[rows].astype(f32) + own[rows].astype(f32)).astype(bf16)

            by_rows(body)

        return Scatter("xy"[f], lambda h, k: unit(G, f, h, k, j), L1.at[f, j], add, need(f, 4))

    first = [[first_stage(f, j) for j in range(4)] for f in BOTH]

    def end_first(f, j):
        for h in BOTH:
            a, b = first[f][j].last(h)
            need(f, 4)(h, 0)
            own = unit(G, f, h, 0, j)
            place_j = at("yx"[f], j)
            travels = j == 2 or j == (3, 1)[h]

            def body(rows):
                total = own[rows].astype(f32) + a[rows].astype(f32) + b[rows].astype(f32)
                if travels:
                    B1[f, h, place_j, rows] = total.astype(bf16)
                else:
                    F1[f, h, place_j, rows] = total

            by_rows(body)

    def down_stage(j):
        def own(h, k):
            return GD.at[h, at("z", k), at("x", j)]

        def add(got, h, k):
            got[...] = (got[...].astype(f32) + own(h, k)[...].astype(f32)).astype(bf16)

        return Scatter("z", own, LZ.at[j], add)

    down = [down_stage(j) for j in range(X)]

    def end_down(j):
        i = at("x", j)
        for h in BOTH:
            a, b = down[j].last(h)
            DS[h, :88] = GD[h, z, i].astype(f32) + a[...].astype(f32) + b[...].astype(f32)
            for yy in range(Y):
                block = DS[h, 22 * yy : 22 * yy + 24, :]
                YS[i * 4 + yy, h] = block.astype(bf16)
                if j == 0:
                    YF[yy, h] = block
        return send_plane(j, lambda k: YS.at[i * 4 + at("y", k)], lambda k: YL.at[j * 4 + k])

    def second_stage(f):
        axis = "yx"[f]

        def add(got, h, k):
            own = F1.at[f, h, at(axis, k)]

            def body(rows):
                got[rows] = (got[rows].astype(f32) + own[rows]).astype(bf16)

            by_rows(body)

        return Scatter(axis, lambda h, k: B1.at[f, h, at(axis, k)], L2.at[f], add)

    second = [second_stage(f) for f in BOTH]

    def end_second(f, h):
        a, b = second[f].last(h)
        own = F1.at[f, h, at("yx"[f], 0)]

        def body(rows):
            F2[f, h, rows] = own[rows] + a[rows].astype(f32) + b[rows].astype(f32)

        by_rows(body)

    def arrive_pair(ring, t, short=False):
        for h, s in SHORT if short else LONG:
            ring.arrive(h, s, t)

    def begin(j, pair):
        for f in BOTH:
            for h, s in pair:
                first[f][j].first(h, s)

    def arrive_first(j):
        for f in BOTH:
            arrive_pair(first[f][j], 1)

    def arrive_down(t, short=False):
        for j in order:
            arrive_pair(down[j], t, short)

    order = (2, 1, 3, 0)
    for j in order:
        begin(j, LONG)
    for j in order[:2]:
        begin(j, SHORT)
    load_rest()
    for i in range(3):
        loads["down", i].wait()

    def permute(j):
        i = at("x", j)
        rows = GR[:, pl.ds(pl.multiple_of(i * 352, 32), 352), :].reshape(ROWS, 512)
        out = jnp.dot(PF[...], rows, preferred_element_type=f32)
        for zz in range(Z):
            for h in BOTH:
                GD[h, zz, i] = out[88 * zz : 88 * zz + 88, 256 * h : 256 * h + 256].astype(bf16)

    for j in order:
        permute(j)
        down[j].start()
    for j, later in zip(order, order[2:]):
        arrive_first(j)
        begin(later, SHORT)
    arrive_first(3)
    arrive_down(1)
    for h in BOTH:
        DS[h, 88:] = jnp.zeros((8, 256), f32)
    arrive_down(1, True)
    for f in BOTH:
        end_first(f, 2)
        for h, s in LONG:
            second[f].first(h, s)
    arrive_first(0)
    arrive_down(2)
    for f in BOTH:
        end_first(f, 1)
    arrive_down(2, True)
    for f in BOTH:
        end_first(f, 3)
        for h, s in SHORT:
            second[f].first(h, s)
    arrive_down(3)
    for f in BOTH:
        arrive_pair(second[f], 1)
    for f in BOTH:
        end_first(f, 0)
    far = (4, 3, 5, 2, 6, 1, 7)
    third = []
    for h in BOTH:
        for f in BOTH:
            end_second(f, h)
        for j in range(4):
            t0, t1 = (F2[f, h, 8 * j : 8 * j + 8, :] for f in BOTH)
            for i, block in enumerate((jnp.concatenate([t0[:4], t1[:4]], 0), jnp.concatenate([t0[4:], t1[4:]], 0))):
                ZF[2 * j + i, h] = block
                ZS[2 * j + i, h] = block.astype(bf16)
        third.append({k: send(ZS.at[at("z", k), h], ZL.at[k, h], "z", k) for k in far})
    third_down = {}
    for j in order:
        third_down.update(end_down(j))
    for copy in third_down.values():
        copy.wait_recv()
    real = lax.broadcasted_iota(jnp.int32, (24, 256), 0) < 22
    squares = jnp.zeros((), f32)
    g_down = []
    for h in BOTH:
        total = YF[y, h]
        for k in range(1, 16):
            total = total + YL[k, h].astype(f32)
        total = jnp.where(real, total, 0.0).astype(bf16).astype(f32)
        g_down.append(total)
        squares += jnp.sum(total * total)
    g_wide = []
    for h in BOTH:
        for k in reversed(far):
            third[h][k].wait_recv()
        total = ZF[z, h]
        for k in range(1, 8):
            total = total + ZL[k, h].astype(f32)
        total = total.astype(bf16).astype(f32)
        g_wide.append(total)
        squares += jnp.sum(total * total)

    total = jnp.full((1, 128), squares, f32)
    NS[0] = total
    told = {}
    for i in order:
        told.update(send_plane(i, lambda k: NS.at[0], lambda k: NL.at[i * 4 + k]))
    for copy in told.values():
        copy.wait_recv()
    for k in range(1, 16):
        total = total + NL[k]
    NS[1] = total
    told = {k: send(NS.at[1], NL.at[16 + k], "z", k) for k in far}
    for k in reversed(far):
        told[k].wait_recv()
    for k in range(1, 8):
        total = total + NL[16 + k]
    factor = jnp.minimum(1.0, 0.5 * lax.rsqrt(total / COUNT + 1e-30))[0:1, 0:1]

    def adamw(w, m, v, g):
        m = 0.9 * m + 0.1 * g
        v = 0.95 * v + 0.05 * g * g
        return (w - 0.02 * (m * lax.rsqrt(v + 1e-8) + 0.1 * w)).astype(bf16), m, v

    for copy in own_w:
        copy.wait()
    odd = d % 2 == 1
    wide_z = []
    for h in BOTH:
        w = [OW[h, i].astype(f32) for i in BOTH]
        w = jnp.concatenate([jnp.where(odd, one[4:], one[:4]) for one in w], 0)
        m, v = (jnp.concatenate([IW[i, h, 0], IW[i, h, 1]], 0) for i in BOTH)
        WZ[z, h], *new = adamw(w, m, v, g_wide[h] * factor)
        wide_z.append({k: send(WZ.at[z, h], WZ.at[z, h], "z", k) for k in far})
        for i, one in enumerate(new):
            for layer in BOTH:
                MW[i, h, layer] = one[4 * layer : 4 * layer + 4]
    g = jnp.concatenate(g_down, 1) * factor
    for h in BOTH:
        DS[h, :24] = jnp.zeros((24, 256), f32)
    pick = lax.broadcasted_iota(jnp.int32, (24, 24), 1) == lax.broadcasted_iota(jnp.int32, (24, 24), 0) + (11 * d - low)
    pick = jnp.where(pick, 1.0, 0.0).astype(bf16)
    for layer in BOTH:
        w = jnp.dot(pick, OWD[layer], preferred_element_type=f32)[:11]
        w, *new = adamw(w, ID[0, :, layer, :], ID[1, :, layer, :], g[11 * layer : 11 * layer + 11])
        for i, one in enumerate(new):
            MD[i, :, layer, :] = one
        for h in BOTH:
            DS[h, 11 * layer : 11 * layer + 11, :] = w[:, 256 * h : 256 * h + 256].astype(f32)
    for h in BOTH:
        YW[x * 4 + y, h] = DS[h, :24].astype(bf16)

    mine = YW.at[x * 4 + y]
    plane = {}
    for i in (0, 2, 1, 3):
        plane.update(send_plane(i, lambda k: mine, lambda k: mine))
    down = [Gather("z", functools.partial(lambda j, h, k: WD.at[h, at("z", k), at("x", j)], j)) for j in range(X)]

    def begin_down(j):
        for k in range(Y):
            if (j, k) != (0, 0):
                plane[-j % 4, k].wait_recv()
        i = at("x", j)
        for h in BOTH:
            for yy in range(Y):
                DS[h, 22 * yy : 22 * yy + 24, :] = YW[i * 4 + yy, h].astype(f32)
            WD[h, z, i] = DS[h, :88].astype(bf16)
        down[j].start()

    def begin_wide(h):
        for k in reversed(far):
            wide_z[h][k].wait_recv()
        for layer in BOTH:
            rows = slice(4 * layer, 4 * layer + 4)
            for j in range(2):
                parts = [WZ[4 * j + i, h].astype(f32)[rows] for i in range(4)]
                WG[h, layer, x, y, 16 * j : 16 * j + 16, :] = jnp.concatenate(parts, 0).astype(bf16)

    near = [Gather("yx"[f], functools.partial(lambda f, h, k: unit(WG, f, h, 0, k), f)) for f in BOTH]
    wide = [[Gather("xy"[f], functools.partial(lambda f, j, h, k: unit(WG, f, h, k, j), f, j)) for j in range(4)] for f in BOTH]

    def spread(f, h, j):
        for s in WAYS[:: 1 - 2 * h]:
            wide[f][j % 4].push(h, s, 1)

    def arrive_near(t, pair):
        for f in BOTH:
            for h, s in pair:
                spread(f, h, near[f].arrive(h, s, t))

    def arrive_wide(j, t, pair):
        for f in BOTH:
            for h, s in pair:
                wide[f][j].arrive(h, s, t)

    begin_down(0)
    for h in BOTH:
        begin_wide(h)
        for f in BOTH:
            for s in WAYS[:: 1 - 2 * h]:
                near[f].push(h, s, 1)
        for f in BOTH:
            spread(f, h, 0)
        if h == 0:
            for j in order[:3]:
                begin_down(j)
    arrive_near(1, LONG)
    arrive_near(1, SHORT)
    arrive_down(1)
    arrive_wide(0, 1, LONG)
    arrive_near(2, LONG)
    arrive_down(1, True)
    for j in (1, 3):
        arrive_wide(j, 1, LONG)
    arrive_down(2)
    arrive_down(2, True)
    arrive_wide(2, 1, LONG)
    arrive_down(3)
    loads["back", 0].wait()
    for j in (0, 2, 1, 3):
        arrive_pair(down[j], 3, True)
        arrive_pair(down[j], 4)
        i = at("x", j)
        for h in BOTH:
            rows = WD[h, :, i].astype(f32).reshape(ROWS, 256).astype(bf16)
            out = jnp.dot(PB[...], rows, preferred_element_type=f32).astype(bf16)
            for layer in BOTH:
                OD[layer, pl.ds(pl.multiple_of(i * 352, 32), 352), 256 * h : 256 * h + 256] = out[352 * layer : 352 * layer + 352]
        arrive_wide(j, 1, SHORT)
        arrive_wide(j, 2, LONG)
    for copy in pending:
        copy.wait_send()


def finish(W, OD, MW, MD, *rest):
    sem = rest[-1]
    sources = [W.at[0], W.at[1], OD] + [r for i in BOTH for r in (MW.at[i, 0], MW.at[i, 1], MD.at[i])]
    copies = [pltpu.make_async_copy(src, dst, sem.at[i]) for i, (src, dst) in enumerate(zip(sources, rest))]
    for copy in copies:
        copy.start()
    for copy in copies:
        copy.wait()


def step_kernel(*args):
    hbm, vmem = pl.BlockSpec(memory_space=pl.ANY), pl.BlockSpec(memory_space=pltpu.VMEM)
    wide, deep = (2, 4, F), (11, 2, 512)
    unit, half = (4, 32, F), (4, 88, 256)
    pair, square, whole_down = (2, 2), (4, *unit), (2, 8, *half)
    blocks, small = (8, 2, 8, F), (16, 2, 24, 256)
    shape = jax.ShapeDtypeStruct
    out = pl.pallas_call(
        kernel,
        out_shape=(pltpu.VMEM((*pair, *square), bf16), pltpu.VMEM((2, F, 512), bf16), pltpu.VMEM((*pair, *wide), f32), pltpu.VMEM((2, *deep), f32)),
        in_specs=[hbm] * 14,
        out_specs=(vmem,) * 4,
        scratch_shapes=[
            pltpu.VMEM((*pair, *square), bf16),
            pltpu.VMEM((2, F, 512), bf16),
            pltpu.VMEM(whole_down, bf16),
            pltpu.VMEM((2, 4, 6, *unit[1:]), bf16),
            pltpu.VMEM((*pair, *unit), f32),
            pltpu.VMEM((*pair, *unit), bf16),
            pltpu.VMEM((2, 6, *unit[1:]), bf16),
            pltpu.VMEM((*pair, *unit[1:]), f32),
            pltpu.VMEM(blocks, bf16),
            pltpu.VMEM(blocks, f32),
            pltpu.VMEM(blocks, bf16),
            pltpu.VMEM((4, 14, *half[1:]), bf16),
            pltpu.VMEM((2, 96, 256), f32),
            pltpu.VMEM(small, bf16),
            pltpu.VMEM((4, *small[1:]), f32),
            pltpu.VMEM(small, bf16),
            pltpu.VMEM((2, 1, 128), f32),
            pltpu.VMEM((24, 1, 128), f32),
            pltpu.VMEM(whole_down, bf16),
            pltpu.VMEM(blocks, bf16),
            pltpu.VMEM(small, bf16),
            pltpu.VMEM((ROWS, ROWS), bf16),
            pltpu.VMEM((ROWS, ROWS), bf16),
            pltpu.VMEM((*pair, 8, F), bf16),
            pltpu.VMEM((2, 24, 512), bf16),
            pltpu.VMEM((*pair, *wide), f32),
            pltpu.VMEM((2, *deep), f32),
            pltpu.SemaphoreType.DMA((SEMS,)),
            pltpu.SemaphoreType.DMA((SEMS,)),
            pltpu.SemaphoreType.DMA((LOADS,)),
            pltpu.SemaphoreType.DMA((9,)),
        ],
        compiler_params=pltpu.CompilerParams(collective_id=0, has_side_effects=True, vmem_limit_bytes=50 * 2**20),
        name="clipped_step",
    )(*one_hots(), *args)
    out = [pltpu.with_memory_space_constraint(one, pltpu.VMEM) for one in out]
    return pl.pallas_call(
        finish,
        out_shape=(shape((2, *square), bf16),) * 2 + (shape((2, F, 512), bf16),) + (shape(wide, f32), shape(wide, f32), shape(deep, f32)) * 2,
        in_specs=[vmem] * 4,
        out_specs=(hbm,) * 9,
        scratch_shapes=[pltpu.SemaphoreType.DMA((9,))],
        compiler_params=pltpu.CompilerParams(vmem_limit_bytes=50 * 2**20),
        name="finish",
    )(*out)


def solution(mesh):
    def step(gg, gu, gd, wg, wu, wd, mg, mu, md, vg, vu, vd):
        gg, gu = (g.reshape(2, 4, 4, 32, F) for g in (gg, gu))
        md, vd = (a.transpose(1, 0, 2) for a in (md, vd))
        og, ou, od, omg, omu, omd, ovg, ovu, ovd = step_kernel(gg, gu, gd[0], wg, wu, wd, mg, mu, md, vg, vu, vd)
        og, ou = (o.reshape(2, 512, F) for o in (og, ou))
        omd, ovd = (a.transpose(1, 0, 2) for a in (omd, ovd))
        return og, ou, od, omg, omu, omd, ovg, ovu, ovd

    all_of, cut = P(None, None, None), P(None, "dp", None)
    return jax.shard_map(
        step,
        mesh=mesh,
        in_specs=(P(("rep", "dp"), None, None, None),) * 3 + (all_of,) * 3 + (cut,) * 6,
        out_specs=(P("rep", None, None),) * 3 + (P("rep", "dp", None),) * 6,
        check_vma=False,
    )
```

```python
import functools

import jax
import jax.numpy as jnp
import numpy as np
from jax import lax
from jax.experimental import pallas as pl
from jax.experimental.pallas import tpu as pltpu
from jax.sharding import PartitionSpec as P

X, Y, Z = 4, 4, 8
F = 1408
COUNT = 3 * 2 * 512 * F
SEMS = 320
LOADS = 32
ROWS = 704
f32, bf16 = jnp.float32, jnp.bfloat16
BOTH = (0, 1)
WAYS = (1, -1)
LONG = ((0, 1), (1, -1))
SHORT = ((1, 1), (0, -1))


def chains(n):
    return [(*one, n // 2) for one in LONG] + [(*one, n // 2 - 1) for one in SHORT]


def slots(n):
    return {key: i for i, key in enumerate((h, s, t) for h, s, length in chains(n) for t in range(1, length + 1))}


def one_hots():
    rows = np.arange(ROWS).reshape(2, 4, 8, 11).transpose(2, 1, 0, 3).reshape(-1)
    forth = rows[:, None] == np.arange(ROWS)
    return [jnp.asarray(p, bf16) for p in (forth, forth.T)]


def loop(n, body):
    def step(i, carry):
        body(i)
        return carry

    lax.fori_loop(0, n, step, 0)


def kernel(pf, pb, gg, gu, gd, wg, wu, wd, mg, mu, md, vg, vu, vd, WG, OD, MW, MD, *scratch):
    (G, GR, GD, L1, F1, B1, L2, F2, ZS, ZF, ZL, LZ, DS, YS, YF, YL, NS, NL, WD, WZ, YW, PF, PB, OW, OWD, IW, ID) = scratch[:-4]
    ssem, rsem, lsem, wsem = scratch[-4:]
    d = lax.axis_index("dp")
    x, y, z = d // 32, (d // 8) % 4, d % 8
    place = {"x": (x, 4), "y": (y, 4), "z": (z, 8)}

    def at(axis, k):
        p, n = place[axis]
        return lax.rem(p + (k + n) % n, n)

    def device(axis, k):
        p = at(axis, k)
        return {"x": p * 32 + y * 8 + z, "y": x * 32 + p * 8 + z, "z": x * 32 + y * 8 + p}[axis]

    barrier = pltpu.get_barrier_semaphore()
    for axis in place:
        for way in WAYS:
            pl.semaphore_signal(barrier, inc=1, device_id={"dp": device(axis, way)}, device_id_type=pl.DeviceIdType.MESH)

    used = [0]
    pending = []

    def send_to(target, src, dst):
        i = used[0]
        used[0] += 1
        copy = pltpu.make_async_remote_copy(
            src_ref=src, dst_ref=dst, send_sem=ssem.at[i], recv_sem=rsem.at[i],
            device_id={"dp": target}, device_id_type=pl.DeviceIdType.MESH,
        )
        copy.start()
        pending.append(copy)
        return copy

    def send(src, dst, axis, k):
        return send_to(device(axis, k), src, dst)

    def send_plane(i, source, target):
        ks = [k for k in (2, 1, 3, 0) if i or k]
        return {(i, k): send_to(at("x", i) * 32 + at("y", k) * 8 + z, source(k), target(k)) for k in ks}

    loads = {}

    def load(key, src, dst):
        copy = pltpu.make_async_copy(src, dst, lsem.at[len(loads)])
        copy.start()
        loads[key] = copy

    class Scatter:
        def __init__(self, axis, own, landing, add, need=None):
            self.axis, self.own, self.landing, self.add, self.need = axis, own, landing, add, need
            self.n = place[axis][1]
            self.length = {(h, s): length for h, s, length in chains(self.n)}
            self.slot = slots(self.n)
            self.copies = {}

        def at(self, h, s, t):
            return self.landing.at[self.slot[h, s, t]]

        def first(self, h, s):
            k = s * self.length[h, s]
            if self.need:
                self.need(h, k)
            self.copies[h, s, 1] = send(self.own(h, k), self.at(h, s, 1), self.axis, s)

        def start(self):
            for h, s, _ in chains(self.n):
                self.first(h, s)

        def arrive(self, h, s, t):
            self.copies[h, s, t].wait_recv()
            if t < self.length[h, s]:
                k = s * (self.length[h, s] - t)
                if self.need:
                    self.need(h, k)
                self.add(self.at(h, s, t), h, k)
                self.copies[h, s, t + 1] = send(self.at(h, s, t), self.at(h, s, t + 1), self.axis, s)

        def last(self, h):
            for s in WAYS:
                self.arrive(h, s, self.length[h, s])
            return [self.at(h, s, self.length[h, s]) for s in WAYS]

    class Gather:
        def __init__(self, axis, part):
            self.axis, self.part = axis, part
            self.n = place[axis][1]
            self.length = {(h, s): length for h, s, length in chains(self.n)}
            self.copies = {}

        def push(self, h, s, t):
            ref = self.part(h, -s * (t - 1))
            self.copies[h, s, t] = send(ref, ref, self.axis, s)

        def start(self):
            for h, s, _ in chains(self.n):
                self.push(h, s, 1)

        def arrive(self, h, s, t):
            self.copies[h, s, t].wait_recv()
            if t < self.length[h, s]:
                self.push(h, s, t + 1)
            return -s * t

    def load_wide(f, h, k):
        if f == 0:
            load((f, h, k), (gg, gu)[h].at[0, at("x", k)], G.at[h, 0, at("x", k)])
        else:
            load((f, h, k), (gg, gu)[h].at[1, :, at("y", k)], G.at[h, 1, :, at("y", k)])

    for h, k in ((0, 2), (1, 2), (1, 1), (0, 3)):
        for f in BOTH:
            load_wide(f, h, k)
    load(("down", 2), pf, PF)
    for i in BOTH:
        load(("down", i), gd.at[i], GR.at[i])
    low = pl.multiple_of(8 * ((11 * d) // 8) - 8 * (d // 127), 8)
    own_w = []

    def load_rest():
        for h, k in ((0, 1), (1, 3), (0, 0), (1, 0)):
            for f in BOTH:
                load_wide(f, h, k)
        load(("back", 0), pb, PB)
        mine = pl.multiple_of(8 * (d // 2), 8)
        pairs = [(w.at[:, pl.ds(mine, 8), :], OW.at[i]) for i, w in enumerate((wg, wu))]
        pairs.append((wd.at[:, pl.ds(low, 24), :], OWD))
        for i, (wide_, deep_) in enumerate((((mg, mu), md), ((vg, vu), vd))):
            pairs += [(wide_[h], IW.at[i, h]) for h in BOTH]
            pairs.append((deep_, ID.at[i]))
        for src, dst in pairs:
            own_w.append(pltpu.make_async_copy(src, dst, wsem.at[len(own_w)]))
            own_w[-1].start()

    ready = set()

    def need(f, n):
        def wait(h, k):
            key = (f, h, k % n)
            if key not in ready:
                ready.add(key)
                loads[key].wait()

        return wait

    pl.semaphore_wait(barrier, 2 * len(place))

    def unit(ref, f, h, k, j):
        return ref.at[h, 0, at("x", k), at("y", j)] if f == 0 else ref.at[h, 1, at("x", j), at("y", k)]

    def by_rows(body):
        loop(2, lambda i: body(pl.ds(pl.multiple_of(i * 16, 16), 16)))

    def first_stage(f, j):
        def add(got, h, k):
            own = unit(G, f, h, k, j)

            def body(rows):
                got[rows] = (got[rows].astype(f32) + own[rows].astype(f32)).astype(bf16)

            by_rows(body)

        return Scatter("xy"[f], lambda h, k: unit(G, f, h, k, j), L1.at[f, j], add, need(f, 4))

    first = [[first_stage(f, j) for j in range(4)] for f in BOTH]

    def end_first(f, j):
        for h in BOTH:
            a, b = first[f][j].last(h)
            need(f, 4)(h, 0)
            own = unit(G, f, h, 0, j)
            place_j = at("yx"[f], j)
            travels = j == 2 or j == (3, 1)[h]

            def body(rows):
                total = own[rows].astype(f32) + a[rows].astype(f32) + b[rows].astype(f32)
                if travels:
                    B1[f, h, place_j, rows] = total.astype(bf16)
                else:
                    F1[f, h, place_j, rows] = total

            by_rows(body)

    def down_stage(j):
        def own(h, k):
            return GD.at[h, at("z", k), at("x", j)]

        def add(got, h, k):
            got[...] = (got[...].astype(f32) + own(h, k)[...].astype(f32)).astype(bf16)

        return Scatter("z", own, LZ.at[j], add)

    down = [down_stage(j) for j in range(X)]

    def end_down(j):
        i = at("x", j)
        for h in BOTH:
            a, b = down[j].last(h)
            DS[h, :88] = GD[h, z, i].astype(f32) + a[...].astype(f32) + b[...].astype(f32)
            for yy in range(Y):
                block = DS[h, 22 * yy : 22 * yy + 24, :]
                YS[i * 4 + yy, h] = block.astype(bf16)
                if j == 0:
                    YF[yy, h] = block
        return send_plane(j, lambda k: YS.at[i * 4 + at("y", k)], lambda k: YL.at[j * 4 + k])

    def second_stage(f):
        axis = "yx"[f]

        def add(got, h, k):
            own = F1.at[f, h, at(axis, k)]

            def body(rows):
                got[rows] = (got[rows].astype(f32) + own[rows]).astype(bf16)

            by_rows(body)

        return Scatter(axis, lambda h, k: B1.at[f, h, at(axis, k)], L2.at[f], add)

    second = [second_stage(f) for f in BOTH]

    def end_second(f, h):
        a, b = second[f].last(h)
        own = F1.at[f, h, at("yx"[f], 0)]

        def body(rows):
            F2[f, h, rows] = own[rows] + a[rows].astype(f32) + b[rows].astype(f32)

        by_rows(body)

    def arrive_pair(ring, t, short=False):
        for h, s in SHORT if short else LONG:
            ring.arrive(h, s, t)

    def begin(j, pair):
        for f in BOTH:
            for h, s in pair:
                first[f][j].first(h, s)

    def arrive_first(j):
        for f in BOTH:
            arrive_pair(first[f][j], 1)

    def arrive_down(t, short=False):
        for j in order:
            arrive_pair(down[j], t, short)

    order = (2, 1, 3, 0)
    for j in order:
        begin(j, LONG)
    for j in order[:2]:
        begin(j, SHORT)
    load_rest()
    for i in range(3):
        loads["down", i].wait()

    def permute(j):
        i = at("x", j)
        rows = GR[:, pl.ds(pl.multiple_of(i * 352, 32), 352), :].reshape(ROWS, 512)
        out = jnp.dot(PF[...], rows, preferred_element_type=f32)
        for zz in range(Z):
            for h in BOTH:
                GD[h, zz, i] = out[88 * zz : 88 * zz + 88, 256 * h : 256 * h + 256].astype(bf16)

    for j in order:
        permute(j)
        down[j].start()
    for j, later in zip(order, order[2:]):
        arrive_first(j)
        begin(later, SHORT)
    arrive_first(3)
    arrive_down(1)
    for h in BOTH:
        DS[h, 88:] = jnp.zeros((8, 256), f32)
    arrive_down(1, True)
    for f in BOTH:
        end_first(f, 2)
        for h, s in LONG:
            second[f].first(h, s)
    arrive_first(0)
    arrive_down(2)
    for f in BOTH:
        end_first(f, 1)
    arrive_down(2, True)
    for f in BOTH:
        end_first(f, 3)
        for h, s in SHORT:
            second[f].first(h, s)
    arrive_down(3)
    for f in BOTH:
        arrive_pair(second[f], 1)
    for f in BOTH:
        end_first(f, 0)
    far = (4, 3, 5, 2, 6, 1, 7)
    third, relay = [], []
    for h in BOTH:
        for f in BOTH:
            end_second(f, h)
        for j in range(4):
            t0, t1 = (F2[f, h, 8 * j : 8 * j + 8, :] for f in BOTH)
            for i, block in enumerate((jnp.concatenate([t0[:4], t1[:4]], 0), jnp.concatenate([t0[4:], t1[4:]], 0))):
                ZF[2 * j + i, h] = block
                ZS[2 * j + i, h] = block.astype(bf16)
        way = WAYS[h]
        relay.append(send(ZS.at[at("z", 4), h], ZL.at[4, h], "z", way))
        third.append({k: send(ZS.at[at("z", k), h], ZL.at[k, h], "z", k) for k in (-3 * way % Z, 2, 6)})
    for h in BOTH:
        k = 3 * WAYS[h] % Z
        relay[h].wait_recv()
        ZL[4, h] = (ZL[4, h].astype(f32) + ZF[at("z", k), h]).astype(bf16)
        third[h].update({k: send(src, ZL.at[k, h], "z", k) for k, src in ((k, ZL.at[4, h]), (1, ZS.at[at("z", 1), h]), (7, ZS.at[at("z", 7), h]))})
    third_down = {}
    for j in order:
        third_down.update(end_down(j))
    for copy in third_down.values():
        copy.wait_recv()
    real = lax.broadcasted_iota(jnp.int32, (24, 256), 0) < 22
    squares = jnp.zeros((), f32)
    g_down = []
    for h in BOTH:
        total = YF[y, h]
        for k in range(1, 16):
            total = total + YL[k, h].astype(f32)
        total = jnp.where(real, total, 0.0).astype(bf16).astype(f32)
        g_down.append(total)
        squares += jnp.sum(total * total)
    g_wide = []
    for h in BOTH:
        for copy in third[h].values():
            copy.wait_recv()
        total = ZF[z, h]
        for k in third[h]:
            total = total + ZL[k, h].astype(f32)
        total = total.astype(bf16).astype(f32)
        g_wide.append(total)
        squares += jnp.sum(total * total)

    total = jnp.full((1, 128), squares, f32)
    NS[0] = total
    told = {}
    for i in order:
        told.update(send_plane(i, lambda k: NS.at[0], lambda k: NL.at[i * 4 + k]))
    for copy in told.values():
        copy.wait_recv()
    for k in range(1, 16):
        total = total + NL[k]
    NS[1] = total
    told = {k: send(NS.at[1], NL.at[16 + k], "z", k) for k in far}
    for k in reversed(far):
        told[k].wait_recv()
    for k in range(1, 8):
        total = total + NL[16 + k]
    factor = jnp.minimum(1.0, 0.5 * lax.rsqrt(total / COUNT + 1e-30))[0:1, 0:1]

    def adamw(w, m, v, g):
        m = 0.9 * m + 0.1 * g
        v = 0.95 * v + 0.05 * g * g
        return (w - 0.02 * (m * lax.rsqrt(v + 1e-8) + 0.1 * w)).astype(bf16), m, v

    for copy in own_w:
        copy.wait()
    odd = d % 2 == 1
    wide_z = []
    for h in BOTH:
        w = [OW[h, i].astype(f32) for i in BOTH]
        w = jnp.concatenate([jnp.where(odd, one[4:], one[:4]) for one in w], 0)
        m, v = (jnp.concatenate([IW[i, h, 0], IW[i, h, 1]], 0) for i in BOTH)
        WZ[z, h], *new = adamw(w, m, v, g_wide[h] * factor)
        wide_z.append({k: send(WZ.at[z, h], WZ.at[z, h], "z", k) for k in (3, 5, 2, 6, 1, 7)})
        for i, one in enumerate(new):
            for layer in BOTH:
                MW[i, h, layer] = one[4 * layer : 4 * layer + 4]
    g = jnp.concatenate(g_down, 1) * factor
    for h in BOTH:
        DS[h, :24] = jnp.zeros((24, 256), f32)
    pick = lax.broadcasted_iota(jnp.int32, (24, 24), 1) == lax.broadcasted_iota(jnp.int32, (24, 24), 0) + (11 * d - low)
    pick = jnp.where(pick, 1.0, 0.0).astype(bf16)
    for layer in BOTH:
        w = jnp.dot(pick, OWD[layer], preferred_element_type=f32)[:11]
        w, *new = adamw(w, ID[0, :, layer, :], ID[1, :, layer, :], g[11 * layer : 11 * layer + 11])
        for i, one in enumerate(new):
            MD[i, :, layer, :] = one
        for h in BOTH:
            DS[h, 11 * layer : 11 * layer + 11, :] = w[:, 256 * h : 256 * h + 256].astype(f32)
    for h in BOTH:
        YW[x * 4 + y, h] = DS[h, :24].astype(bf16)

    mine = YW.at[x * 4 + y]
    plane = {}
    spread_order = (0, 2, 1, 3)
    for i in spread_order:
        plane.update(send_plane(i, lambda k: mine, lambda k: mine))
    down = [Gather("z", functools.partial(lambda j, h, k: WD.at[h, at("z", k), at("x", j)], j)) for j in range(X)]

    def begin_down(j):
        for k in range(Y):
            if (j, k) != (0, 0):
                plane[-j % 4, k].wait_recv()
        i = at("x", j)
        for h in BOTH:
            for yy in range(Y):
                DS[h, 22 * yy : 22 * yy + 24, :] = YW[i * 4 + yy, h].astype(f32)
            WD[h, z, i] = DS[h, :88].astype(bf16)
        down[j].start()

    def begin_wide(h):
        for copy in wide_z[h].values():
            copy.wait_recv()
        for layer in BOTH:
            rows = slice(4 * layer, 4 * layer + 4)
            for j in range(2):
                parts = [WZ[4 * j + i, h].astype(f32)[rows] for i in range(4)]
                WG[h, layer, x, y, 16 * j : 16 * j + 16, :] = jnp.concatenate(parts, 0).astype(bf16)

    near = [Gather("yx"[f], functools.partial(lambda f, h, k: unit(WG, f, h, 0, k), f)) for f in BOTH]
    wide = [[Gather("xy"[f], functools.partial(lambda f, j, h, k: unit(WG, f, h, k, j), f, j)) for j in range(4)] for f in BOTH]

    def spread(f, h, j):
        for s in WAYS[:: 1 - 2 * h]:
            wide[f][j % 4].push(h, s, 1)

    def arrive_near(h, t, ways=WAYS):
        for s in ways:
            for f in BOTH:
                spread(f, h, near[f].arrive(h, s, t))

    def arrive_wide(j, h, t=1):
        for f in BOTH:
            wide[f][j].arrive(h, WAYS[h], t)

    def both_down(t, *js):
        for j in js:
            arrive_pair(down[j], t)
            arrive_pair(down[j], t, True)

    for h, way in enumerate(WAYS):
        k = 3 * way % Z
        wide_z[h].pop(k).wait_recv()
        other = WZ.at[at("z", -k), h]
        wide_z[h][4] = send(other, other, "z", way)
    begin_down(0)
    for h in BOTH:
        begin_wide(h)
        for f in BOTH:
            for s in WAYS[:: 1 - 2 * h]:
                near[f].push(h, s, 1)
        for f in BOTH:
            spread(f, h, 0)
        if h == 0:
            for j in order[:3]:
                begin_down(j)
    arrive_near(0, 1)
    both_down(1, 0)
    arrive_wide(0, 0)
    both_down(1, 2)
    arrive_near(1, 1)
    both_down(1, 1)
    arrive_wide(0, 1)
    both_down(1, 3)
    arrive_near(0, 2, WAYS[:1])
    both_down(2, 0)
    arrive_wide(3, 0)
    both_down(2, 2)
    arrive_wide(1, 0)
    arrive_near(1, 2, WAYS[1:])
    both_down(2, 1)
    arrive_wide(1, 1)
    both_down(2, 3)
    arrive_wide(3, 1)
    for j in spread_order[:2]:
        arrive_pair(down[j], 3)
    for h in BOTH:
        arrive_wide(2, h)
    for j in spread_order[2:]:
        arrive_pair(down[j], 3)
    loads["back", 0].wait()
    for j in spread_order:
        arrive_pair(down[j], 3, True)
        arrive_pair(down[j], 4)
        i = at("x", j)
        for h in BOTH:
            rows = WD[h, :, i].astype(f32).reshape(ROWS, 256).astype(bf16)
            out = jnp.dot(PB[...], rows, preferred_element_type=f32).astype(bf16)
            for layer in BOTH:
                OD[layer, pl.ds(pl.multiple_of(i * 352, 32), 352), 256 * h : 256 * h + 256] = out[352 * layer : 352 * layer + 352]
    for j in spread_order:
        for f in BOTH:
            arrive_pair(wide[f][j], 1, True)
        for h in BOTH:
            arrive_wide(j, h, 2)
    for copy in pending:
        copy.wait_send()


def finish(W, OD, MW, MD, *rest):
    sem = rest[-1]
    sources = [W.at[0], W.at[1], OD] + [r for i in BOTH for r in (MW.at[i, 0], MW.at[i, 1], MD.at[i])]
    copies = [pltpu.make_async_copy(src, dst, sem.at[i]) for i, (src, dst) in enumerate(zip(sources, rest))]
    for copy in copies:
        copy.start()
    for copy in copies:
        copy.wait()


def step_kernel(*args):
    hbm, vmem = pl.BlockSpec(memory_space=pl.ANY), pl.BlockSpec(memory_space=pltpu.VMEM)
    wide, deep = (2, 4, F), (11, 2, 512)
    unit, half = (4, 32, F), (4, 88, 256)
    pair, square, whole_down = (2, 2), (4, *unit), (2, 8, *half)
    blocks, small = (8, 2, 8, F), (16, 2, 24, 256)
    shape = jax.ShapeDtypeStruct
    out = pl.pallas_call(
        kernel,
        out_shape=(pltpu.VMEM((*pair, *square), bf16), pltpu.VMEM((2, F, 512), bf16), pltpu.VMEM((*pair, *wide), f32), pltpu.VMEM((2, *deep), f32)),
        in_specs=[hbm] * 14,
        out_specs=(vmem,) * 4,
        scratch_shapes=[
            pltpu.VMEM((*pair, *square), bf16),
            pltpu.VMEM((2, F, 512), bf16),
            pltpu.VMEM(whole_down, bf16),
            pltpu.VMEM((2, 4, 6, *unit[1:]), bf16),
            pltpu.VMEM((*pair, *unit), f32),
            pltpu.VMEM((*pair, *unit), bf16),
            pltpu.VMEM((2, 6, *unit[1:]), bf16),
            pltpu.VMEM((*pair, *unit[1:]), f32),
            pltpu.VMEM(blocks, bf16),
            pltpu.VMEM(blocks, f32),
            pltpu.VMEM(blocks, bf16),
            pltpu.VMEM((4, 14, *half[1:]), bf16),
            pltpu.VMEM((2, 96, 256), f32),
            pltpu.VMEM(small, bf16),
            pltpu.VMEM((4, *small[1:]), f32),
            pltpu.VMEM(small, bf16),
            pltpu.VMEM((2, 1, 128), f32),
            pltpu.VMEM((24, 1, 128), f32),
            pltpu.VMEM(whole_down, bf16),
            pltpu.VMEM(blocks, bf16),
            pltpu.VMEM(small, bf16),
            pltpu.VMEM((ROWS, ROWS), bf16),
            pltpu.VMEM((ROWS, ROWS), bf16),
            pltpu.VMEM((*pair, 8, F), bf16),
            pltpu.VMEM((2, 24, 512), bf16),
            pltpu.VMEM((*pair, *wide), f32),
            pltpu.VMEM((2, *deep), f32),
            pltpu.SemaphoreType.DMA((SEMS,)),
            pltpu.SemaphoreType.DMA((SEMS,)),
            pltpu.SemaphoreType.DMA((LOADS,)),
            pltpu.SemaphoreType.DMA((9,)),
        ],
        compiler_params=pltpu.CompilerParams(collective_id=0, has_side_effects=True, vmem_limit_bytes=50 * 2**20),
        name="clipped_step",
    )(*one_hots(), *args)
    out = [pltpu.with_memory_space_constraint(one, pltpu.VMEM) for one in out]
    return pl.pallas_call(
        finish,
        out_shape=(shape((2, *square), bf16),) * 2 + (shape((2, F, 512), bf16),) + (shape(wide, f32), shape(wide, f32), shape(deep, f32)) * 2,
        in_specs=[vmem] * 4,
        out_specs=(hbm,) * 9,
        scratch_shapes=[pltpu.SemaphoreType.DMA((9,))],
        compiler_params=pltpu.CompilerParams(vmem_limit_bytes=50 * 2**20),
        name="finish",
    )(*out)


def solution(mesh):
    def step(gg, gu, gd, wg, wu, wd, mg, mu, md, vg, vu, vd):
        gg, gu = (g.reshape(2, 4, 4, 32, F) for g in (gg, gu))
        md, vd = (a.transpose(1, 0, 2) for a in (md, vd))
        og, ou, od, omg, omu, omd, ovg, ovu, ovd = step_kernel(gg, gu, gd[0], wg, wu, wd, mg, mu, md, vg, vu, vd)
        og, ou = (o.reshape(2, 512, F) for o in (og, ou))
        omd, ovd = (a.transpose(1, 0, 2) for a in (omd, ovd))
        return og, ou, od, omg, omu, omd, ovg, ovu, ovd

    all_of, cut = P(None, None, None), P(None, "dp", None)
    return jax.shard_map(
        step,
        mesh=mesh,
        in_specs=(P(("rep", "dp"), None, None, None),) * 3 + (all_of,) * 3 + (cut,) * 6,
        out_specs=(P("rep", None, None),) * 3 + (P("rep", "dp", None),) * 6,
        check_vma=False,
    )
```

```python
import functools

import jax
import jax.numpy as jnp
import numpy as np
from jax import lax
from jax.experimental import pallas as pl
from jax.experimental.pallas import tpu as pltpu
from jax.sharding import PartitionSpec as P

X, Y, Z = 4, 4, 8
F = 1408
COUNT = 3 * 2 * 512 * F
SEMS = 320
LOADS = 32
ROWS = 704
f32, bf16 = jnp.float32, jnp.bfloat16
BOTH = (0, 1)
WAYS = (1, -1)
LONG = ((0, 1), (1, -1))
SHORT = ((1, 1), (0, -1))


def chains(n):
    return [(*one, n // 2) for one in LONG] + [(*one, n // 2 - 1) for one in SHORT]


def slots(n):
    return {key: i for i, key in enumerate((h, s, t) for h, s, length in chains(n) for t in range(1, length + 1))}


def one_hots():
    rows = np.arange(ROWS).reshape(2, 4, 8, 11).transpose(2, 1, 0, 3).reshape(-1)
    forth = rows[:, None] == np.arange(ROWS)
    return [jnp.asarray(p, bf16) for p in (forth, forth.T)]


def loop(n, body):
    def step(i, carry):
        body(i)
        return carry

    lax.fori_loop(0, n, step, 0)


def kernel(pf, pb, gg, gu, gd, wg, wu, wd, mg, mu, md, vg, vu, vd, WG, OD, MW, MD, *scratch):
    (G, GR, GD, L1, F1, B1, L2, F2, ZS, ZF, ZL, LZ, DS, YS, YF, YL, NS, NL, WD, WZ, YW, PF, PB, OW, OWD, IW, ID) = scratch[:-4]
    ssem, rsem, lsem, wsem = scratch[-4:]
    d = lax.axis_index("dp")
    x, y, z = d // 32, (d // 8) % 4, d % 8
    place = {"x": (x, 4), "y": (y, 4), "z": (z, 8)}

    def at(axis, k):
        p, n = place[axis]
        return lax.rem(p + (k + n) % n, n)

    def device(axis, k):
        p = at(axis, k)
        return {"x": p * 32 + y * 8 + z, "y": x * 32 + p * 8 + z, "z": x * 32 + y * 8 + p}[axis]

    barrier = pltpu.get_barrier_semaphore()
    for axis in place:
        for way in WAYS:
            pl.semaphore_signal(barrier, inc=1, device_id={"dp": device(axis, way)}, device_id_type=pl.DeviceIdType.MESH)

    used = [0]
    pending = []

    def send_to(target, src, dst):
        i = used[0]
        used[0] += 1
        copy = pltpu.make_async_remote_copy(
            src_ref=src, dst_ref=dst, send_sem=ssem.at[i], recv_sem=rsem.at[i],
            device_id={"dp": target}, device_id_type=pl.DeviceIdType.MESH,
        )
        copy.start()
        pending.append(copy)
        return copy

    def send(src, dst, axis, k):
        return send_to(device(axis, k), src, dst)

    def send_plane(i, source, target):
        ks = [k for k in (2, 1, 3, 0) if i or k]
        return {(i, k): send_to(at("x", i) * 32 + at("y", k) * 8 + z, source(k), target(k)) for k in ks}

    loads = {}

    def load(key, src, dst):
        copy = pltpu.make_async_copy(src, dst, lsem.at[len(loads)])
        copy.start()
        loads[key] = copy

    class Scatter:
        def __init__(self, axis, own, landing, add, need=None):
            self.axis, self.own, self.landing, self.add, self.need = axis, own, landing, add, need
            self.n = place[axis][1]
            self.length = {(h, s): length for h, s, length in chains(self.n)}
            self.slot = slots(self.n)
            self.copies = {}

        def at(self, h, s, t):
            return self.landing.at[self.slot[h, s, t]]

        def first(self, h, s):
            k = s * self.length[h, s]
            if self.need:
                self.need(h, k)
            self.copies[h, s, 1] = send(self.own(h, k), self.at(h, s, 1), self.axis, s)

        def start(self):
            for h, s, _ in chains(self.n):
                self.first(h, s)

        def arrive(self, h, s, t):
            self.copies[h, s, t].wait_recv()
            if t < self.length[h, s]:
                k = s * (self.length[h, s] - t)
                if self.need:
                    self.need(h, k)
                self.add(self.at(h, s, t), h, k)
                self.copies[h, s, t + 1] = send(self.at(h, s, t), self.at(h, s, t + 1), self.axis, s)

        def last(self, h):
            for s in WAYS:
                self.arrive(h, s, self.length[h, s])
            return [self.at(h, s, self.length[h, s]) for s in WAYS]

    class Gather:
        def __init__(self, axis, part):
            self.axis, self.part = axis, part
            self.n = place[axis][1]
            self.length = {(h, s): length for h, s, length in chains(self.n)}
            self.copies = {}

        def push(self, h, s, t):
            ref = self.part(h, -s * (t - 1))
            self.copies[h, s, t] = send(ref, ref, self.axis, s)

        def start(self):
            for h, s, _ in chains(self.n):
                self.push(h, s, 1)

        def arrive(self, h, s, t):
            self.copies[h, s, t].wait_recv()
            if t < self.length[h, s]:
                self.push(h, s, t + 1)
            return -s * t

    def load_wide(f, h, k):
        if f == 0:
            load((f, h, k), (gg, gu)[h].at[0, at("x", k)], G.at[h, 0, at("x", k)])
        else:
            load((f, h, k), (gg, gu)[h].at[1, :, at("y", k)], G.at[h, 1, :, at("y", k)])

    for h, k in ((0, 2), (1, 2), (1, 1), (0, 3)):
        for f in BOTH:
            load_wide(f, h, k)
    load(("down", 2), pf, PF)
    for i in BOTH:
        load(("down", i), gd.at[i], GR.at[i])
    low = pl.multiple_of(8 * ((11 * d) // 8) - 8 * (d // 127), 8)
    own_w = []

    def load_rest():
        for h, k in ((0, 1), (1, 3), (0, 0), (1, 0)):
            for f in BOTH:
                load_wide(f, h, k)
        load(("back", 0), pb, PB)
        mine = pl.multiple_of(8 * (d // 2), 8)
        pairs = [(w.at[:, pl.ds(mine, 8), :], OW.at[i]) for i, w in enumerate((wg, wu))]
        pairs.append((wd.at[:, pl.ds(low, 24), :], OWD))
        for i, (wide_, deep_) in enumerate((((mg, mu), md), ((vg, vu), vd))):
            pairs += [(wide_[h], IW.at[i, h]) for h in BOTH]
            pairs.append((deep_, ID.at[i]))
        for src, dst in pairs:
            own_w.append(pltpu.make_async_copy(src, dst, wsem.at[len(own_w)]))
            own_w[-1].start()

    ready = set()

    def need(f, n):
        def wait(h, k):
            key = (f, h, k % n)
            if key not in ready:
                ready.add(key)
                loads[key].wait()

        return wait

    pl.semaphore_wait(barrier, 2 * len(place))

    def unit(ref, f, h, k, j):
        return ref.at[h, 0, at("x", k), at("y", j)] if f == 0 else ref.at[h, 1, at("x", j), at("y", k)]

    def by_rows(body):
        loop(2, lambda i: body(pl.ds(pl.multiple_of(i * 16, 16), 16)))

    def first_stage(f, j):
        def add(got, h, k):
            own = unit(G, f, h, k, j)

            def body(rows):
                got[rows] = (got[rows].astype(f32) + own[rows].astype(f32)).astype(bf16)

            by_rows(body)

        return Scatter("xy"[f], lambda h, k: unit(G, f, h, k, j), L1.at[f, j], add, need(f, 4))

    first = [[first_stage(f, j) for j in range(4)] for f in BOTH]

    def end_first(h, j):
        for f in BOTH:
            a, b = first[f][j].last(h)
            need(f, 4)(h, 0)
            own = unit(G, f, h, 0, j)
            place_j = at("yx"[f], j)
            travels = j == 2 or j == (3, 1)[h]

            def body(rows):
                total = own[rows].astype(f32) + a[rows].astype(f32) + b[rows].astype(f32)
                if travels:
                    B1[f, h, place_j, rows] = total.astype(bf16)
                else:
                    F1[f, h, place_j, rows] = total

            by_rows(body)

    def down_stage(j):
        def own(h, k):
            return GD.at[h, at("z", k), at("x", j)]

        def add(got, h, k):
            got[...] = (got[...].astype(f32) + own(h, k)[...].astype(f32)).astype(bf16)

        return Scatter("z", own, LZ.at[j], add)

    down = [down_stage(j) for j in range(X)]

    def end_down(j):
        i = at("x", j)
        for h in BOTH:
            a, b = down[j].last(h)
            DS[h, :88] = GD[h, z, i].astype(f32) + a[...].astype(f32) + b[...].astype(f32)
            for yy in range(Y):
                block = DS[h, 22 * yy : 22 * yy + 24, :]
                YS[i * 4 + yy, h] = block.astype(bf16)
                if j == 0:
                    YF[yy, h] = block
        return send_plane(j, lambda k: YS.at[i * 4 + at("y", k)], lambda k: YL.at[j * 4 + k])

    def second_stage(f):
        axis = "yx"[f]

        def add(got, h, k):
            own = F1.at[f, h, at(axis, k)]

            def body(rows):
                got[rows] = (got[rows].astype(f32) + own[rows]).astype(bf16)

            by_rows(body)

        return Scatter(axis, lambda h, k: B1.at[f, h, at(axis, k)], L2.at[f], add)

    second = [second_stage(f) for f in BOTH]

    def end_second(f, h):
        a, b = second[f].last(h)
        own = F1.at[f, h, at("yx"[f], 0)]

        def body(rows):
            F2[f, h, rows] = own[rows] + a[rows].astype(f32) + b[rows].astype(f32)

        by_rows(body)

    def arrive_pair(ring, t, short=False):
        for h, s in SHORT if short else LONG:
            ring.arrive(h, s, t)

    def begin(which, *js):
        for j in js:
            for f in BOTH:
                first[f][j].first(*which)

    def arrive_first(which, *js):
        for j in js:
            for f in BOTH:
                first[f][j].arrive(*which, 1)

    def begin_second(which):
        for f in BOTH:
            second[f].first(*which)

    def arrive_second(which):
        for f in BOTH:
            second[f].arrive(*which, 1)

    def arrive_down(t, short=False):
        for j in order:
            arrive_pair(down[j], t, short)

    gate_long, up_long = LONG
    up_short, gate_short = SHORT
    gate, up = BOTH
    order = (2, 1, 3, 0)
    u2, u1, u3, u0 = order
    begin(gate_long, *order)
    begin(gate_short, *order)
    begin(up_long, *order)
    load_rest()
    for i in range(3):
        loads["down", i].wait()

    def permute(j):
        i = at("x", j)
        rows = GR[:, pl.ds(pl.multiple_of(i * 352, 32), 352), :].reshape(ROWS, 512)
        out = jnp.dot(PF[...], rows, preferred_element_type=f32)
        for zz in range(Z):
            for h in BOTH:
                GD[h, zz, i] = out[88 * zz : 88 * zz + 88, 256 * h : 256 * h + 256].astype(bf16)

    for j in order:
        permute(j)
        down[j].start()
    arrive_first(gate_long, u2, u1, u3)
    arrive_down(1)
    arrive_first(gate_long, u0)
    for h in BOTH:
        DS[h, 88:] = jnp.zeros((8, 256), f32)
    end_first(gate, u2)
    begin_second(gate_long)
    arrive_down(1, True)
    begin(up_short, u2, u1)
    arrive_first(up_long, u2, u1)
    end_first(gate, u1)
    end_first(gate, u3)
    begin_second(gate_short)
    arrive_first(up_long, u3)
    arrive_down(2)
    end_first(gate, u0)
    arrive_second(gate_long)
    arrive_down(2, True)
    begin(up_short, u3, u0)
    end_first(up, u2)
    begin_second(up_long)
    arrive_first(up_long, u0)
    end_first(up, u1)
    begin_second(up_short)
    arrive_down(3)

    far = (4, 3, 5, 2, 6, 1, 7)
    third, relay, third_down = [], [], {}

    def begin_third(h):
        for f in BOTH:
            end_second(f, h)
        for j in range(4):
            t0, t1 = (F2[f, h, 8 * j : 8 * j + 8, :] for f in BOTH)
            for i, block in enumerate((jnp.concatenate([t0[:4], t1[:4]], 0), jnp.concatenate([t0[4:], t1[4:]], 0))):
                ZF[2 * j + i, h] = block
                ZS[2 * j + i, h] = block.astype(bf16)
        way = WAYS[h]
        relay.append(send(ZS.at[at("z", 4), h], ZL.at[4, h], "z", way))
        third.append({k: send(ZS.at[at("z", k), h], ZL.at[k, h], "z", k) for k in (-3 * way % Z, 2, 6)})

    def pass_on(h):
        k = 3 * WAYS[h] % Z
        relay[h].wait_recv()
        ZL[4, h] = (ZL[4, h].astype(f32) + ZF[at("z", k), h]).astype(bf16)
        third[h].update({k: send(src, ZL.at[k, h], "z", k) for k, src in ((k, ZL.at[4, h]), (1, ZS.at[at("z", 1), h]), (7, ZS.at[at("z", 7), h]))})

    begin_third(gate)
    end_first(up, u3)
    arrive_second(up_long)
    third_down.update(end_down(u2))
    end_first(up, u0)
    for j in (u1, u3):
        third_down.update(end_down(j))
    pass_on(gate)
    third_down.update(end_down(u0))
    begin_third(up)
    pass_on(up)
    for copy in third_down.values():
        copy.wait_recv()
    real = lax.broadcasted_iota(jnp.int32, (24, 256), 0) < 22
    squares = jnp.zeros((), f32)
    g_down = []
    for h in BOTH:
        total = YF[y, h]
        for k in range(1, 16):
            total = total + YL[k, h].astype(f32)
        total = jnp.where(real, total, 0.0).astype(bf16).astype(f32)
        g_down.append(total)
        squares += jnp.sum(total * total)
    g_wide = []
    for h in BOTH:
        for copy in third[h].values():
            copy.wait_recv()
        total = ZF[z, h]
        for k in third[h]:
            total = total + ZL[k, h].astype(f32)
        total = total.astype(bf16).astype(f32)
        g_wide.append(total)
        squares += jnp.sum(total * total)

    total = jnp.full((1, 128), squares, f32)
    NS[0] = total
    told = {}
    for i in order:
        told.update(send_plane(i, lambda k: NS.at[0], lambda k: NL.at[i * 4 + k]))
    for copy in told.values():
        copy.wait_recv()
    for k in range(1, 16):
        total = total + NL[k]
    NS[1] = total
    told = {k: send(NS.at[1], NL.at[16 + k], "z", k) for k in far}
    for k in reversed(far):
        told[k].wait_recv()
    for k in range(1, 8):
        total = total + NL[16 + k]
    factor = jnp.minimum(1.0, 0.5 * lax.rsqrt(total / COUNT + 1e-30))[0:1, 0:1]

    def adamw(w, m, v, g):
        m = 0.9 * m + 0.1 * g
        v = 0.95 * v + 0.05 * g * g
        return (w - 0.02 * (m * lax.rsqrt(v + 1e-8) + 0.1 * w)).astype(bf16), m, v

    for copy in own_w:
        copy.wait()
    odd = d % 2 == 1
    wide_z = []
    for h in BOTH:
        w = [OW[h, i].astype(f32) for i in BOTH]
        w = jnp.concatenate([jnp.where(odd, one[4:], one[:4]) for one in w], 0)
        m, v = (jnp.concatenate([IW[i, h, 0], IW[i, h, 1]], 0) for i in BOTH)
        WZ[z, h], *new = adamw(w, m, v, g_wide[h] * factor)
        wide_z.append({k: send(WZ.at[z, h], WZ.at[z, h], "z", k) for k in (3, 5, 2, 6, 1, 7)})
        for i, one in enumerate(new):
            for layer in BOTH:
                MW[i, h, layer] = one[4 * layer : 4 * layer + 4]
    g = jnp.concatenate(g_down, 1) * factor
    for h in BOTH:
        DS[h, :24] = jnp.zeros((24, 256), f32)
    pick = lax.broadcasted_iota(jnp.int32, (24, 24), 1) == lax.broadcasted_iota(jnp.int32, (24, 24), 0) + (11 * d - low)
    pick = jnp.where(pick, 1.0, 0.0).astype(bf16)
    for layer in BOTH:
        w = jnp.dot(pick, OWD[layer], preferred_element_type=f32)[:11]
        w, *new = adamw(w, ID[0, :, layer, :], ID[1, :, layer, :], g[11 * layer : 11 * layer + 11])
        for i, one in enumerate(new):
            MD[i, :, layer, :] = one
        for h in BOTH:
            DS[h, 11 * layer : 11 * layer + 11, :] = w[:, 256 * h : 256 * h + 256].astype(f32)
    for h in BOTH:
        YW[x * 4 + y, h] = DS[h, :24].astype(bf16)

    mine = YW.at[x * 4 + y]
    plane = {}
    spread_order = (0, 2, 1, 3)
    for i in spread_order:
        plane.update(send_plane(i, lambda k: mine, lambda k: mine))
    down = [Gather("z", functools.partial(lambda j, h, k: WD.at[h, at("z", k), at("x", j)], j)) for j in range(X)]

    def begin_down(j):
        for k in range(Y):
            if (j, k) != (0, 0):
                plane[-j % 4, k].wait_recv()
        i = at("x", j)
        for h in BOTH:
            for yy in range(Y):
                DS[h, 22 * yy : 22 * yy + 24, :] = YW[i * 4 + yy, h].astype(f32)
            WD[h, z, i] = DS[h, :88].astype(bf16)
        down[j].start()

    def begin_wide(h):
        for copy in wide_z[h].values():
            copy.wait_recv()
        for layer in BOTH:
            rows = slice(4 * layer, 4 * layer + 4)
            for j in range(2):
                parts = [WZ[4 * j + i, h].astype(f32)[rows] for i in range(4)]
                WG[h, layer, x, y, 16 * j : 16 * j + 16, :] = jnp.concatenate(parts, 0).astype(bf16)

    near = [Gather("yx"[f], functools.partial(lambda f, h, k: unit(WG, f, h, 0, k), f)) for f in BOTH]
    wide = [[Gather("xy"[f], functools.partial(lambda f, j, h, k: unit(WG, f, h, k, j), f, j)) for j in range(4)] for f in BOTH]

    def spread(f, h, j):
        for s in WAYS[:: 1 - 2 * h]:
            wide[f][j % 4].push(h, s, 1)

    def arrive_near(h, t, ways=WAYS):
        for s in ways:
            for f in BOTH:
                spread(f, h, near[f].arrive(h, s, t))

    def arrive_wide(j, h, t=1):
        for f in BOTH:
            wide[f][j].arrive(h, WAYS[h], t)

    def both_down(t, *js):
        for j in js:
            arrive_pair(down[j], t)
            arrive_pair(down[j], t, True)

    for h, way in enumerate(WAYS):
        k = 3 * way % Z
        wide_z[h].pop(k).wait_recv()
        other = WZ.at[at("z", -k), h]
        wide_z[h][4] = send(other, other, "z", way)
    begin_down(0)
    for h in BOTH:
        begin_wide(h)
        for f in BOTH:
            for s in WAYS[:: 1 - 2 * h]:
                near[f].push(h, s, 1)
        for f in BOTH:
            spread(f, h, 0)
        if h == 0:
            for j in order[:3]:
                begin_down(j)
    arrive_near(0, 1)
    both_down(1, 0)
    arrive_wide(0, 0)
    both_down(1, 2)
    arrive_near(1, 1)
    both_down(1, 1)
    arrive_wide(0, 1)
    both_down(1, 3)
    arrive_near(0, 2, WAYS[:1])
    both_down(2, 0)
    arrive_wide(3, 0)
    both_down(2, 2)
    arrive_wide(1, 0)
    arrive_near(1, 2, WAYS[1:])
    both_down(2, 1)
    arrive_wide(1, 1)
    both_down(2, 3)
    arrive_wide(3, 1)
    for j in spread_order[:2]:
        arrive_pair(down[j], 3)
    for h in BOTH:
        arrive_wide(2, h)
    for j in spread_order[2:]:
        arrive_pair(down[j], 3)
    loads["back", 0].wait()
    for j in spread_order:
        arrive_pair(down[j], 3, True)
        arrive_pair(down[j], 4)
        i = at("x", j)
        for h in BOTH:
            rows = WD[h, :, i].astype(f32).reshape(ROWS, 256).astype(bf16)
            out = jnp.dot(PB[...], rows, preferred_element_type=f32).astype(bf16)
            for layer in BOTH:
                OD[layer, pl.ds(pl.multiple_of(i * 352, 32), 352), 256 * h : 256 * h + 256] = out[352 * layer : 352 * layer + 352]
    for j in spread_order:
        for f in BOTH:
            arrive_pair(wide[f][j], 1, True)
        for h in BOTH:
            arrive_wide(j, h, 2)
    for copy in pending:
        copy.wait_send()


def finish(W, OD, MW, MD, *rest):
    sem = rest[-1]
    sources = [W.at[0], W.at[1], OD] + [r for i in BOTH for r in (MW.at[i, 0], MW.at[i, 1], MD.at[i])]
    copies = [pltpu.make_async_copy(src, dst, sem.at[i]) for i, (src, dst) in enumerate(zip(sources, rest))]
    for copy in copies:
        copy.start()
    for copy in copies:
        copy.wait()


def step_kernel(*args):
    hbm, vmem = pl.BlockSpec(memory_space=pl.ANY), pl.BlockSpec(memory_space=pltpu.VMEM)
    wide, deep = (2, 4, F), (11, 2, 512)
    unit, half = (4, 32, F), (4, 88, 256)
    pair, square, whole_down = (2, 2), (4, *unit), (2, 8, *half)
    blocks, small = (8, 2, 8, F), (16, 2, 24, 256)
    shape = jax.ShapeDtypeStruct
    out = pl.pallas_call(
        kernel,
        out_shape=(pltpu.VMEM((*pair, *square), bf16), pltpu.VMEM((2, F, 512), bf16), pltpu.VMEM((*pair, *wide), f32), pltpu.VMEM((2, *deep), f32)),
        in_specs=[hbm] * 14,
        out_specs=(vmem,) * 4,
        scratch_shapes=[
            pltpu.VMEM((*pair, *square), bf16),
            pltpu.VMEM((2, F, 512), bf16),
            pltpu.VMEM(whole_down, bf16),
            pltpu.VMEM((2, 4, 6, *unit[1:]), bf16),
            pltpu.VMEM((*pair, *unit), f32),
            pltpu.VMEM((*pair, *unit), bf16),
            pltpu.VMEM((2, 6, *unit[1:]), bf16),
            pltpu.VMEM((*pair, *unit[1:]), f32),
            pltpu.VMEM(blocks, bf16),
            pltpu.VMEM(blocks, f32),
            pltpu.VMEM(blocks, bf16),
            pltpu.VMEM((4, 14, *half[1:]), bf16),
            pltpu.VMEM((2, 96, 256), f32),
            pltpu.VMEM(small, bf16),
            pltpu.VMEM((4, *small[1:]), f32),
            pltpu.VMEM(small, bf16),
            pltpu.VMEM((2, 1, 128), f32),
            pltpu.VMEM((24, 1, 128), f32),
            pltpu.VMEM(whole_down, bf16),
            pltpu.VMEM(blocks, bf16),
            pltpu.VMEM(small, bf16),
            pltpu.VMEM((ROWS, ROWS), bf16),
            pltpu.VMEM((ROWS, ROWS), bf16),
            pltpu.VMEM((*pair, 8, F), bf16),
            pltpu.VMEM((2, 24, 512), bf16),
            pltpu.VMEM((*pair, *wide), f32),
            pltpu.VMEM((2, *deep), f32),
            pltpu.SemaphoreType.DMA((SEMS,)),
            pltpu.SemaphoreType.DMA((SEMS,)),
            pltpu.SemaphoreType.DMA((LOADS,)),
            pltpu.SemaphoreType.DMA((9,)),
        ],
        compiler_params=pltpu.CompilerParams(collective_id=0, has_side_effects=True, vmem_limit_bytes=50 * 2**20),
        name="clipped_step",
    )(*one_hots(), *args)
    out = [pltpu.with_memory_space_constraint(one, pltpu.VMEM) for one in out]
    return pl.pallas_call(
        finish,
        out_shape=(shape((2, *square), bf16),) * 2 + (shape((2, F, 512), bf16),) + (shape(wide, f32), shape(wide, f32), shape(deep, f32)) * 2,
        in_specs=[vmem] * 4,
        out_specs=(hbm,) * 9,
        scratch_shapes=[pltpu.SemaphoreType.DMA((9,))],
        compiler_params=pltpu.CompilerParams(vmem_limit_bytes=50 * 2**20),
        name="finish",
    )(*out)


def solution(mesh):
    def step(gg, gu, gd, wg, wu, wd, mg, mu, md, vg, vu, vd):
        gg, gu = (g.reshape(2, 4, 4, 32, F) for g in (gg, gu))
        md, vd = (a.transpose(1, 0, 2) for a in (md, vd))
        og, ou, od, omg, omu, omd, ovg, ovu, ovd = step_kernel(gg, gu, gd[0], wg, wu, wd, mg, mu, md, vg, vu, vd)
        og, ou = (o.reshape(2, 512, F) for o in (og, ou))
        omd, ovd = (a.transpose(1, 0, 2) for a in (omd, ovd))
        return og, ou, od, omg, omu, omd, ovg, ovu, ovd

    all_of, cut = P(None, None, None), P(None, "dp", None)
    return jax.shard_map(
        step,
        mesh=mesh,
        in_specs=(P(("rep", "dp"), None, None, None),) * 3 + (all_of,) * 3 + (cut,) * 6,
        out_specs=(P("rep", None, None),) * 3 + (P("rep", "dp", None),) * 6,
        check_vma=False,
    )
```

```python
import functools

import jax
import jax.numpy as jnp
import numpy as np
from jax import lax
from jax.experimental import pallas as pl
from jax.experimental.pallas import tpu as pltpu
from jax.sharding import PartitionSpec as P

X, Y, Z = 4, 4, 8
F = 1408
COUNT = 3 * 2 * 512 * F
SEMS = 320
LOADS = 32
ROWS = 704
f32, bf16 = jnp.float32, jnp.bfloat16
BOTH = (0, 1)
WAYS = (1, -1)
LONG = ((0, 1), (1, -1))
SHORT = ((1, 1), (0, -1))


def chains(n):
    return [(*one, n // 2) for one in LONG] + [(*one, n // 2 - 1) for one in SHORT]


def slots(n):
    return {key: i for i, key in enumerate((h, s, t) for h, s, length in chains(n) for t in range(1, length + 1))}


def one_hots():
    rows = np.arange(ROWS).reshape(2, 4, 8, 11).transpose(2, 1, 0, 3).reshape(-1)
    forth = rows[:, None] == np.arange(ROWS)
    return [jnp.asarray(p, bf16) for p in (forth, forth.T)]


def loop(n, body):
    def step(i, carry):
        body(i)
        return carry

    lax.fori_loop(0, n, step, 0)


def kernel(pf, pb, gg, gu, gd, wg, wu, wd, mg, mu, md, vg, vu, vd, WG, OD, MW, MD, *scratch):
    (G, GR, GD, L1, F1, B1, L2, F2, ZS, ZF, ZL, LZ, DS, YS, YF, YL, NS, NL, WD, WZ, YW, PF, PB, OW, OWD, IW, ID) = scratch[:-4]
    ssem, rsem, lsem, wsem = scratch[-4:]
    d = lax.axis_index("dp")
    x, y, z = d // 32, (d // 8) % 4, d % 8
    place = {"x": (x, 4), "y": (y, 4), "z": (z, 8)}

    def at(axis, k):
        p, n = place[axis]
        return lax.rem(p + (k + n) % n, n)

    def device(axis, k):
        p = at(axis, k)
        return {"x": p * 32 + y * 8 + z, "y": x * 32 + p * 8 + z, "z": x * 32 + y * 8 + p}[axis]

    barrier = pltpu.get_barrier_semaphore()
    for axis in place:
        for way in WAYS:
            pl.semaphore_signal(barrier, inc=1, device_id={"dp": device(axis, way)}, device_id_type=pl.DeviceIdType.MESH)

    used = [0]
    pending = []

    def send_to(target, src, dst):
        i = used[0]
        used[0] += 1
        copy = pltpu.make_async_remote_copy(
            src_ref=src, dst_ref=dst, send_sem=ssem.at[i], recv_sem=rsem.at[i],
            device_id={"dp": target}, device_id_type=pl.DeviceIdType.MESH,
        )
        copy.start()
        pending.append(copy)
        return copy

    def send(src, dst, axis, k):
        return send_to(device(axis, k), src, dst)

    def send_plane(i, source, target):
        ks = [k for k in (2, 1, 3, 0) if i or k]
        return {(i, k): send_to(at("x", i) * 32 + at("y", k) * 8 + z, source(k), target(k)) for k in ks}

    loads = {}

    def load(key, src, dst):
        copy = pltpu.make_async_copy(src, dst, lsem.at[len(loads)])
        copy.start()
        loads[key] = copy

    class Scatter:
        def __init__(self, axis, own, landing, add, need=None):
            self.axis, self.own, self.landing, self.add, self.need = axis, own, landing, add, need
            self.n = place[axis][1]
            self.length = {(h, s): length for h, s, length in chains(self.n)}
            self.slot = slots(self.n)
            self.copies = {}

        def at(self, h, s, t):
            return self.landing.at[self.slot[h, s, t]]

        def first(self, h, s):
            k = s * self.length[h, s]
            if self.need:
                self.need(h, k)
            self.copies[h, s, 1] = send(self.own(h, k), self.at(h, s, 1), self.axis, s)

        def start(self):
            for h, s, _ in chains(self.n):
                self.first(h, s)

        def arrive(self, h, s, t):
            self.copies[h, s, t].wait_recv()
            if t < self.length[h, s]:
                k = s * (self.length[h, s] - t)
                if self.need:
                    self.need(h, k)
                self.add(self.at(h, s, t), h, k)
                self.copies[h, s, t + 1] = send(self.at(h, s, t), self.at(h, s, t + 1), self.axis, s)

        def last(self, h):
            for s in WAYS:
                self.arrive(h, s, self.length[h, s])
            return [self.at(h, s, self.length[h, s]) for s in WAYS]

    class Gather:
        def __init__(self, axis, part):
            self.axis, self.part = axis, part
            self.n = place[axis][1]
            self.length = {(h, s): length for h, s, length in chains(self.n)}
            self.copies = {}

        def push(self, h, s, t):
            ref = self.part(h, -s * (t - 1))
            self.copies[h, s, t] = send(ref, ref, self.axis, s)

        def start(self):
            for h, s, _ in chains(self.n):
                self.push(h, s, 1)

        def arrive(self, h, s, t):
            self.copies[h, s, t].wait_recv()
            if t < self.length[h, s]:
                self.push(h, s, t + 1)
            return -s * t

    def load_wide(f, h, k):
        if f == 0:
            load((f, h, k), (gg, gu)[h].at[0, at("x", k)], G.at[h, 0, at("x", k)])
        else:
            load((f, h, k), (gg, gu)[h].at[1, :, at("y", k)], G.at[h, 1, :, at("y", k)])

    for h, k in ((0, 2), (1, 2), (1, 1), (0, 3)):
        for f in BOTH:
            load_wide(f, h, k)
    load(("down", 2), pf, PF)
    for i in BOTH:
        load(("down", i), gd.at[i], GR.at[i])
    low = pl.multiple_of(8 * ((11 * d) // 8) - 8 * (d // 127), 8)
    own_w = []

    def load_rest():
        for h, k in ((0, 1), (1, 3), (0, 0), (1, 0)):
            for f in BOTH:
                load_wide(f, h, k)
        load(("back", 0), pb, PB)
        mine = pl.multiple_of(8 * (d // 2), 8)
        pairs = [(w.at[:, pl.ds(mine, 8), :], OW.at[i]) for i, w in enumerate((wg, wu))]
        pairs.append((wd.at[:, pl.ds(low, 24), :], OWD))
        for i, (wide_, deep_) in enumerate((((mg, mu), md), ((vg, vu), vd))):
            pairs += [(wide_[h], IW.at[i, h]) for h in BOTH]
            pairs.append((deep_, ID.at[i]))
        for src, dst in pairs:
            own_w.append(pltpu.make_async_copy(src, dst, wsem.at[len(own_w)]))
            own_w[-1].start()

    ready = set()

    def need(f, n):
        def wait(h, k):
            key = (f, h, k % n)
            if key not in ready:
                ready.add(key)
                loads[key].wait()

        return wait

    pl.semaphore_wait(barrier, 2 * len(place))

    def unit(ref, f, h, k, j):
        return ref.at[h, 0, at("x", k), at("y", j)] if f == 0 else ref.at[h, 1, at("x", j), at("y", k)]

    def by_rows(body):
        loop(2, lambda i: body(pl.ds(pl.multiple_of(i * 16, 16), 16)))

    def first_stage(f, j):
        def add(got, h, k):
            own = unit(G, f, h, k, j)

            def body(rows):
                got[rows] = (got[rows].astype(f32) + own[rows].astype(f32)).astype(bf16)

            by_rows(body)

        return Scatter("xy"[f], lambda h, k: unit(G, f, h, k, j), L1.at[f, j], add, need(f, 4))

    first = [[first_stage(f, j) for j in range(4)] for f in BOTH]

    def end_first(h, j):
        for f in BOTH:
            a, b = first[f][j].last(h)
            need(f, 4)(h, 0)
            own = unit(G, f, h, 0, j)
            place_j = at("yx"[f], j)
            travels = j == 2 or j == (3, 1)[h]

            def body(rows):
                total = own[rows].astype(f32) + a[rows].astype(f32) + b[rows].astype(f32)
                if travels:
                    B1[f, h, place_j, rows] = total.astype(bf16)
                else:
                    F1[f, h, place_j, rows] = total

            by_rows(body)

    def down_stage(j):
        def own(h, k):
            return GD.at[h, at("z", k), at("x", j)]

        def add(got, h, k):
            got[...] = (got[...].astype(f32) + own(h, k)[...].astype(f32)).astype(bf16)

        return Scatter("z", own, LZ.at[j], add)

    down = [down_stage(j) for j in range(X)]

    def end_down(j):
        i = at("x", j)
        for h in BOTH:
            a, b = down[j].last(h)
            DS[h, :88] = GD[h, z, i].astype(f32) + a[...].astype(f32) + b[...].astype(f32)
            for yy in range(Y):
                block = DS[h, 22 * yy : 22 * yy + 24, :]
                YS[i * 4 + yy, h] = block.astype(bf16)
                if j == 0:
                    YF[yy, h] = block
        return send_plane(j, lambda k: YS.at[i * 4 + at("y", k)], lambda k: YL.at[j * 4 + k])

    def second_stage(f):
        axis = "yx"[f]

        def add(got, h, k):
            own = F1.at[f, h, at(axis, k)]

            def body(rows):
                got[rows] = (got[rows].astype(f32) + own[rows]).astype(bf16)

            by_rows(body)

        return Scatter(axis, lambda h, k: B1.at[f, h, at(axis, k)], L2.at[f], add)

    second = [second_stage(f) for f in BOTH]

    def end_second(f, h):
        a, b = second[f].last(h)
        own = F1.at[f, h, at("yx"[f], 0)]

        def body(rows):
            F2[f, h, rows] = own[rows] + a[rows].astype(f32) + b[rows].astype(f32)

        by_rows(body)

    def arrive_pair(ring, t, short=False):
        for h, s in SHORT if short else LONG:
            ring.arrive(h, s, t)

    def begin(which, *js):
        for j in js:
            for f in BOTH:
                first[f][j].first(*which)

    def arrive_first(which, *js):
        for j in js:
            for f in BOTH:
                first[f][j].arrive(*which, 1)

    def begin_second(which):
        for f in BOTH:
            second[f].first(*which)

    def arrive_second(which):
        for f in BOTH:
            second[f].arrive(*which, 1)

    def arrive_down(t, short=False):
        for j in order:
            arrive_pair(down[j], t, short)

    gate_long, up_long = LONG
    up_short, gate_short = SHORT
    gate, up = BOTH
    order = (2, 1, 3, 0)
    u2, u1, u3, u0 = order
    begin(gate_long, *order)
    begin(gate_short, *order)
    begin(up_long, *order)
    load_rest()
    for i in range(3):
        loads["down", i].wait()

    def permute(j):
        i = at("x", j)
        rows = GR[:, pl.ds(pl.multiple_of(i * 352, 32), 352), :].reshape(ROWS, 512)
        out = jnp.dot(PF[...], rows, preferred_element_type=f32)
        for zz in range(Z):
            for h in BOTH:
                GD[h, zz, i] = out[88 * zz : 88 * zz + 88, 256 * h : 256 * h + 256].astype(bf16)

    for j in order:
        permute(j)
        down[j].start()
    arrive_first(gate_long, u2, u1, u3)
    arrive_down(1)
    arrive_first(gate_long, u0)
    for h in BOTH:
        DS[h, 88:] = jnp.zeros((8, 256), f32)
    end_first(gate, u2)
    begin_second(gate_long)
    arrive_down(1, True)
    begin(up_short, u2, u1)
    arrive_first(up_long, u2, u1)
    end_first(gate, u1)
    end_first(gate, u3)
    begin_second(gate_short)
    arrive_first(up_long, u3)
    arrive_down(2)
    end_first(gate, u0)
    arrive_second(gate_long)
    arrive_down(2, True)
    begin(up_short, u3, u0)
    end_first(up, u2)
    begin_second(up_long)
    arrive_first(up_long, u0)
    end_first(up, u1)
    begin_second(up_short)
    arrive_down(3)

    far = (4, 3, 5, 2, 6, 1, 7)
    third, third_down = [], {}

    def begin_third(h):
        for f in BOTH:
            end_second(f, h)
        for j in range(4):
            t0, t1 = (F2[f, h, 8 * j : 8 * j + 8, :] for f in BOTH)
            for i, block in enumerate((jnp.concatenate([t0[:4], t1[:4]], 0), jnp.concatenate([t0[4:], t1[4:]], 0))):
                ZF[2 * j + i, h] = block
                ZS[2 * j + i, h] = block.astype(bf16)
        third.append({k: send(ZS.at[at("z", k), h], ZL.at[k, h], "z", k) for k in far})

    begin_third(gate)
    end_first(up, u3)
    arrive_second(up_long)
    third_down.update(end_down(u2))
    end_first(up, u0)
    for j in (u1, u3):
        third_down.update(end_down(j))
    third_down.update(end_down(u0))
    begin_third(up)
    for copy in third_down.values():
        copy.wait_recv()
    real = lax.broadcasted_iota(jnp.int32, (24, 256), 0) < 22
    squares = jnp.zeros((), f32)
    g_down = []
    for h in BOTH:
        total = YF[y, h]
        for k in range(1, 16):
            total = total + YL[k, h].astype(f32)
        total = jnp.where(real, total, 0.0).astype(bf16).astype(f32)
        g_down.append(total)
        squares += jnp.sum(total * total)
    g_wide = []
    for h in BOTH:
        for copy in third[h].values():
            copy.wait_recv()
        total = ZF[z, h]
        for k in third[h]:
            total = total + ZL[k, h].astype(f32)
        total = total.astype(bf16).astype(f32)
        g_wide.append(total)
        squares += jnp.sum(total * total)

    total = jnp.full((1, 128), squares, f32)
    NS[0] = total
    told = {}
    for i in order:
        told.update(send_plane(i, lambda k: NS.at[0], lambda k: NL.at[i * 4 + k]))
    for copy in told.values():
        copy.wait_recv()
    for k in range(1, 16):
        total = total + NL[k]
    NS[1] = total
    told = {k: send(NS.at[1], NL.at[16 + k], "z", k) for k in far}
    for k in reversed(far):
        told[k].wait_recv()
    for k in range(1, 8):
        total = total + NL[16 + k]
    factor = jnp.minimum(1.0, 0.5 * lax.rsqrt(total / COUNT + 1e-30))[0:1, 0:1]

    def adamw(w, m, v, g):
        m = 0.9 * m + 0.1 * g
        v = 0.95 * v + 0.05 * g * g
        return (w - 0.02 * (m * lax.rsqrt(v + 1e-8) + 0.1 * w)).astype(bf16), m, v

    for copy in own_w:
        copy.wait()
    odd = d % 2 == 1
    wide_z = []
    for h in BOTH:
        w = [OW[h, i].astype(f32) for i in BOTH]
        w = jnp.concatenate([jnp.where(odd, one[4:], one[:4]) for one in w], 0)
        m, v = (jnp.concatenate([IW[i, h, 0], IW[i, h, 1]], 0) for i in BOTH)
        WZ[z, h], *new = adamw(w, m, v, g_wide[h] * factor)
        wide_z.append({k: send(WZ.at[z, h], WZ.at[z, h], "z", k) for k in far})
        for i, one in enumerate(new):
            for layer in BOTH:
                MW[i, h, layer] = one[4 * layer : 4 * layer + 4]
    g = jnp.concatenate(g_down, 1) * factor
    for h in BOTH:
        DS[h, :24] = jnp.zeros((24, 256), f32)
    pick = lax.broadcasted_iota(jnp.int32, (24, 24), 1) == lax.broadcasted_iota(jnp.int32, (24, 24), 0) + (11 * d - low)
    pick = jnp.where(pick, 1.0, 0.0).astype(bf16)
    for layer in BOTH:
        w = jnp.dot(pick, OWD[layer], preferred_element_type=f32)[:11]
        w, *new = adamw(w, ID[0, :, layer, :], ID[1, :, layer, :], g[11 * layer : 11 * layer + 11])
        for i, one in enumerate(new):
            MD[i, :, layer, :] = one
        for h in BOTH:
            DS[h, 11 * layer : 11 * layer + 11, :] = w[:, 256 * h : 256 * h + 256].astype(f32)
    for h in BOTH:
        YW[x * 4 + y, h] = DS[h, :24].astype(bf16)

    mine = YW.at[x * 4 + y]
    plane = {}
    spread_order = (0, 2, 1, 3)
    for i in spread_order:
        plane.update(send_plane(i, lambda k: mine, lambda k: mine))
    down = [Gather("z", functools.partial(lambda j, h, k: WD.at[h, at("z", k), at("x", j)], j)) for j in range(X)]

    def begin_down(j):
        for k in range(Y):
            if (j, k) != (0, 0):
                plane[-j % 4, k].wait_recv()
        i = at("x", j)
        for h in BOTH:
            for yy in range(Y):
                DS[h, 22 * yy : 22 * yy + 24, :] = YW[i * 4 + yy, h].astype(f32)
            WD[h, z, i] = DS[h, :88].astype(bf16)
        down[j].start()

    def begin_wide(h):
        for copy in wide_z[h].values():
            copy.wait_recv()
        for layer in BOTH:
            rows = slice(4 * layer, 4 * layer + 4)
            for j in range(2):
                parts = [WZ[4 * j + i, h].astype(f32)[rows] for i in range(4)]
                WG[h, layer, x, y, 16 * j : 16 * j + 16, :] = jnp.concatenate(parts, 0).astype(bf16)

    near = [Gather("yx"[f], functools.partial(lambda f, h, k: unit(WG, f, h, 0, k), f)) for f in BOTH]
    wide = [[Gather("xy"[f], functools.partial(lambda f, j, h, k: unit(WG, f, h, k, j), f, j)) for j in range(4)] for f in BOTH]

    def spread(f, h, j):
        for s in WAYS[:: 1 - 2 * h]:
            wide[f][j % 4].push(h, s, 1)

    def arrive_near(h, t, ways=WAYS):
        for s in ways:
            for f in BOTH:
                spread(f, h, near[f].arrive(h, s, t))

    def arrive_wide(j, h, t=1):
        for f in BOTH:
            wide[f][j].arrive(h, WAYS[h], t)

    def both_down(t, *js):
        for j in js:
            arrive_pair(down[j], t)
            arrive_pair(down[j], t, True)

    begin_down(0)
    for h in BOTH:
        begin_wide(h)
        for f in BOTH:
            for s in WAYS[:: 1 - 2 * h]:
                near[f].push(h, s, 1)
        for f in BOTH:
            spread(f, h, 0)
        if h == 0:
            for j in order[:3]:
                begin_down(j)
    arrive_near(0, 1)
    both_down(1, 0)
    arrive_wide(0, 0)
    both_down(1, 2)
    arrive_near(1, 1)
    both_down(1, 1)
    arrive_wide(0, 1)
    both_down(1, 3)
    arrive_near(0, 2, WAYS[:1])
    both_down(2, 0)
    arrive_wide(3, 0)
    both_down(2, 2)
    arrive_wide(1, 0)
    arrive_near(1, 2, WAYS[1:])
    both_down(2, 1)
    arrive_wide(1, 1)
    both_down(2, 3)
    arrive_wide(3, 1)
    for j in spread_order[:2]:
        arrive_pair(down[j], 3)
    for h in BOTH:
        arrive_wide(2, h)
    for j in spread_order[2:]:
        arrive_pair(down[j], 3)
    loads["back", 0].wait()
    for j in spread_order:
        arrive_pair(down[j], 3, True)
        arrive_pair(down[j], 4)
        i = at("x", j)
        for h in BOTH:
            rows = WD[h, :, i].astype(f32).reshape(ROWS, 256).astype(bf16)
            out = jnp.dot(PB[...], rows, preferred_element_type=f32).astype(bf16)
            for layer in BOTH:
                OD[layer, pl.ds(pl.multiple_of(i * 352, 32), 352), 256 * h : 256 * h + 256] = out[352 * layer : 352 * layer + 352]
    for j in spread_order:
        for f in BOTH:
            arrive_pair(wide[f][j], 1, True)
        for h in BOTH:
            arrive_wide(j, h, 2)
    for copy in pending:
        copy.wait_send()


def finish(W, OD, MW, MD, *rest):
    sem = rest[-1]
    sources = [W.at[0], W.at[1], OD] + [r for i in BOTH for r in (MW.at[i, 0], MW.at[i, 1], MD.at[i])]
    copies = [pltpu.make_async_copy(src, dst, sem.at[i]) for i, (src, dst) in enumerate(zip(sources, rest))]
    for copy in copies:
        copy.start()
    for copy in copies:
        copy.wait()


def step_kernel(*args):
    hbm, vmem = pl.BlockSpec(memory_space=pl.ANY), pl.BlockSpec(memory_space=pltpu.VMEM)
    wide, deep = (2, 4, F), (11, 2, 512)
    unit, half = (4, 32, F), (4, 88, 256)
    pair, square, whole_down = (2, 2), (4, *unit), (2, 8, *half)
    blocks, small = (8, 2, 8, F), (16, 2, 24, 256)
    shape = jax.ShapeDtypeStruct
    out = pl.pallas_call(
        kernel,
        out_shape=(pltpu.VMEM((*pair, *square), bf16), pltpu.VMEM((2, F, 512), bf16), pltpu.VMEM((*pair, *wide), f32), pltpu.VMEM((2, *deep), f32)),
        in_specs=[hbm] * 14,
        out_specs=(vmem,) * 4,
        scratch_shapes=[
            pltpu.VMEM((*pair, *square), bf16),
            pltpu.VMEM((2, F, 512), bf16),
            pltpu.VMEM(whole_down, bf16),
            pltpu.VMEM((2, 4, 6, *unit[1:]), bf16),
            pltpu.VMEM((*pair, *unit), f32),
            pltpu.VMEM((*pair, *unit), bf16),
            pltpu.VMEM((2, 6, *unit[1:]), bf16),
            pltpu.VMEM((*pair, *unit[1:]), f32),
            pltpu.VMEM(blocks, bf16),
            pltpu.VMEM(blocks, f32),
            pltpu.VMEM(blocks, bf16),
            pltpu.VMEM((4, 14, *half[1:]), bf16),
            pltpu.VMEM((2, 96, 256), f32),
            pltpu.VMEM(small, bf16),
            pltpu.VMEM((4, *small[1:]), f32),
            pltpu.VMEM(small, bf16),
            pltpu.VMEM((2, 1, 128), f32),
            pltpu.VMEM((24, 1, 128), f32),
            pltpu.VMEM(whole_down, bf16),
            pltpu.VMEM(blocks, bf16),
            pltpu.VMEM(small, bf16),
            pltpu.VMEM((ROWS, ROWS), bf16),
            pltpu.VMEM((ROWS, ROWS), bf16),
            pltpu.VMEM((*pair, 8, F), bf16),
            pltpu.VMEM((2, 24, 512), bf16),
            pltpu.VMEM((*pair, *wide), f32),
            pltpu.VMEM((2, *deep), f32),
            pltpu.SemaphoreType.DMA((SEMS,)),
            pltpu.SemaphoreType.DMA((SEMS,)),
            pltpu.SemaphoreType.DMA((LOADS,)),
            pltpu.SemaphoreType.DMA((9,)),
        ],
        compiler_params=pltpu.CompilerParams(collective_id=0, has_side_effects=True, vmem_limit_bytes=50 * 2**20),
        name="clipped_step",
    )(*one_hots(), *args)
    out = [pltpu.with_memory_space_constraint(one, pltpu.VMEM) for one in out]
    return pl.pallas_call(
        finish,
        out_shape=(shape((2, *square), bf16),) * 2 + (shape((2, F, 512), bf16),) + (shape(wide, f32), shape(wide, f32), shape(deep, f32)) * 2,
        in_specs=[vmem] * 4,
        out_specs=(hbm,) * 9,
        scratch_shapes=[pltpu.SemaphoreType.DMA((9,))],
        compiler_params=pltpu.CompilerParams(vmem_limit_bytes=50 * 2**20),
        name="finish",
    )(*out)


def solution(mesh):
    def step(gg, gu, gd, wg, wu, wd, mg, mu, md, vg, vu, vd):
        gg, gu = (g.reshape(2, 4, 4, 32, F) for g in (gg, gu))
        md, vd = (a.transpose(1, 0, 2) for a in (md, vd))
        og, ou, od, omg, omu, omd, ovg, ovu, ovd = step_kernel(gg, gu, gd[0], wg, wu, wd, mg, mu, md, vg, vu, vd)
        og, ou = (o.reshape(2, 512, F) for o in (og, ou))
        omd, ovd = (a.transpose(1, 0, 2) for a in (omd, ovd))
        return og, ou, od, omg, omu, omd, ovg, ovu, ovd

    all_of, cut = P(None, None, None), P(None, "dp", None)
    return jax.shard_map(
        step,
        mesh=mesh,
        in_specs=(P(("rep", "dp"), None, None, None),) * 3 + (all_of,) * 3 + (cut,) * 6,
        out_specs=(P("rep", None, None),) * 3 + (P("rep", "dp", None),) * 6,
        check_vma=False,
    )
```

```python
import functools

import jax
import jax.numpy as jnp
import numpy as np
from jax import lax
from jax.experimental import pallas as pl
from jax.experimental.pallas import tpu as pltpu
from jax.sharding import PartitionSpec as P

X, Y, Z = 4, 4, 8
F = 1408
COUNT = 3 * 2 * 512 * F
SEMS = 320
LOADS = 32
ROWS = 704
f32, bf16 = jnp.float32, jnp.bfloat16
BOTH = (0, 1)
WAYS = (1, -1)
LONG = ((0, 1), (1, -1))
SHORT = ((1, 1), (0, -1))


def chains(n):
    return [(*one, n // 2) for one in LONG] + [(*one, n // 2 - 1) for one in SHORT]


def slots(n):
    return {key: i for i, key in enumerate((h, s, t) for h, s, length in chains(n) for t in range(1, length + 1))}


def one_hots():
    rows = np.arange(ROWS).reshape(2, 4, 8, 11).transpose(2, 1, 0, 3).reshape(-1)
    forth = rows[:, None] == np.arange(ROWS)
    return [jnp.asarray(p, bf16) for p in (forth, forth.T)]


def loop(n, body):
    def step(i, carry):
        body(i)
        return carry

    lax.fori_loop(0, n, step, 0)


def kernel(pf, pb, gg, gu, gd, wg, wu, wd, mg, mu, md, vg, vu, vd, WG, OD, MW, MD, *scratch):
    (G, GR, GD, L1, F1, B1, L2, F2, ZS, ZF, ZL, LZ, DS, YS, YF, YL, NS, NL, WD, WZ, YW, PF, PB, OW, OWD, IW, ID) = scratch[:-4]
    ssem, rsem, lsem, wsem = scratch[-4:]
    d = lax.axis_index("dp")
    x, y, z = d // 32, (d // 8) % 4, d % 8
    place = {"x": (x, 4), "y": (y, 4), "z": (z, 8)}

    def at(axis, k):
        p, n = place[axis]
        return lax.rem(p + (k + n) % n, n)

    def device(axis, k):
        p = at(axis, k)
        return {"x": p * 32 + y * 8 + z, "y": x * 32 + p * 8 + z, "z": x * 32 + y * 8 + p}[axis]

    barrier = pltpu.get_barrier_semaphore()
    for axis in place:
        for way in WAYS:
            pl.semaphore_signal(barrier, inc=1, device_id={"dp": device(axis, way)}, device_id_type=pl.DeviceIdType.MESH)

    used = [0]
    pending = []

    def send_to(target, src, dst):
        i = used[0]
        used[0] += 1
        copy = pltpu.make_async_remote_copy(
            src_ref=src, dst_ref=dst, send_sem=ssem.at[i], recv_sem=rsem.at[i],
            device_id={"dp": target}, device_id_type=pl.DeviceIdType.MESH,
        )
        copy.start()
        pending.append(copy)
        return copy

    def send(src, dst, axis, k):
        return send_to(device(axis, k), src, dst)

    def send_plane(i, source, target):
        ks = [k for k in (2, 1, 3, 0) if i or k]
        return {(i, k): send_to(at("x", i) * 32 + at("y", k) * 8 + z, source(k), target(k)) for k in ks}

    def drain(count):
        for copy in pending[:count]:
            copy.wait_send()
        del pending[:count]

    loads = {}

    def load(key, src, dst):
        copy = pltpu.make_async_copy(src, dst, lsem.at[len(loads)])
        copy.start()
        loads[key] = copy

    class Scatter:
        def __init__(self, axis, own, landing, add, need=None):
            self.axis, self.own, self.landing, self.add, self.need = axis, own, landing, add, need
            self.n = place[axis][1]
            self.length = {(h, s): length for h, s, length in chains(self.n)}
            self.slot = slots(self.n)
            self.copies = {}

        def at(self, h, s, t):
            return self.landing.at[self.slot[h, s, t]]

        def first(self, h, s):
            k = s * self.length[h, s]
            if self.need:
                self.need(h, k)
            self.copies[h, s, 1] = send(self.own(h, k), self.at(h, s, 1), self.axis, s)

        def start(self):
            for h, s, _ in chains(self.n):
                self.first(h, s)

        def arrive(self, h, s, t):
            self.copies[h, s, t].wait_recv()
            if t < self.length[h, s]:
                k = s * (self.length[h, s] - t)
                if self.need:
                    self.need(h, k)
                self.add(self.at(h, s, t), h, k)
                self.copies[h, s, t + 1] = send(self.at(h, s, t), self.at(h, s, t + 1), self.axis, s)

        def last(self, h):
            for s in WAYS:
                self.arrive(h, s, self.length[h, s])
            return [self.at(h, s, self.length[h, s]) for s in WAYS]

    class Gather:
        def __init__(self, axis, part):
            self.axis, self.part = axis, part
            self.n = place[axis][1]
            self.length = {(h, s): length for h, s, length in chains(self.n)}
            self.copies = {}

        def push(self, h, s, t):
            ref = self.part(h, -s * (t - 1))
            self.copies[h, s, t] = send(ref, ref, self.axis, s)

        def start(self):
            for h, s, _ in chains(self.n):
                self.push(h, s, 1)

        def arrive(self, h, s, t):
            self.copies[h, s, t].wait_recv()
            if t < self.length[h, s]:
                self.push(h, s, t + 1)
            return -s * t

    def load_wide(f, h, k):
        if f == 0:
            load((f, h, k), (gg, gu)[h].at[0, at("x", k)], G.at[h, 0, at("x", k)])
        else:
            load((f, h, k), (gg, gu)[h].at[1, :, at("y", k)], G.at[h, 1, :, at("y", k)])

    for h, k in ((0, 2), (1, 2), (1, 1), (0, 3)):
        for f in BOTH:
            load_wide(f, h, k)
    load(("down", 2), pf, PF)
    for i in BOTH:
        load(("down", i), gd.at[i], GR.at[i])
    low = pl.multiple_of(8 * ((11 * d) // 8) - 8 * (d // 127), 8)
    own_w = []

    def load_rest():
        for h, k in ((0, 1), (1, 3), (0, 0), (1, 0)):
            for f in BOTH:
                load_wide(f, h, k)
        load(("back", 0), pb, PB)
        mine = pl.multiple_of(8 * (d // 2), 8)
        pairs = [(w.at[:, pl.ds(mine, 8), :], OW.at[i]) for i, w in enumerate((wg, wu))]
        pairs.append((wd.at[:, pl.ds(low, 24), :], OWD))
        for i, (wide_, deep_) in enumerate((((mg, mu), md), ((vg, vu), vd))):
            pairs += [(wide_[h], IW.at[i, h]) for h in BOTH]
            pairs.append((deep_, ID.at[i]))
        for src, dst in pairs:
            own_w.append(pltpu.make_async_copy(src, dst, wsem.at[len(own_w)]))
            own_w[-1].start()

    ready = set()

    def need(f, n):
        def wait(h, k):
            key = (f, h, k % n)
            if key not in ready:
                ready.add(key)
                loads[key].wait()

        return wait

    pl.semaphore_wait(barrier, 2 * len(place))

    def unit(ref, f, h, k, j):
        return ref.at[h, 0, at("x", k), at("y", j)] if f == 0 else ref.at[h, 1, at("x", j), at("y", k)]

    def by_rows(body):
        loop(2, lambda i: body(pl.ds(pl.multiple_of(i * 16, 16), 16)))

    def first_stage(f, j):
        def add(got, h, k):
            own = unit(G, f, h, k, j)

            def body(rows):
                got[rows] = (got[rows].astype(f32) + own[rows].astype(f32)).astype(bf16)

            by_rows(body)

        return Scatter("xy"[f], lambda h, k: unit(G, f, h, k, j), L1.at[f, j], add, need(f, 4))

    first = [[first_stage(f, j) for j in range(4)] for f in BOTH]

    def end_first(h, j):
        for f in BOTH:
            a, b = first[f][j].last(h)
            need(f, 4)(h, 0)
            own = unit(G, f, h, 0, j)
            place_j = at("yx"[f], j)
            travels = j == 2 or j == (3, 1)[h]

            def body(rows):
                total = own[rows].astype(f32) + a[rows].astype(f32) + b[rows].astype(f32)
                if travels:
                    B1[f, h, place_j, rows] = total.astype(bf16)
                else:
                    F1[f, h, place_j, rows] = total

            by_rows(body)

    def down_stage(j):
        def own(h, k):
            return GD.at[h, at("z", k), at("x", j)]

        def add(got, h, k):
            got[...] = (got[...].astype(f32) + own(h, k)[...].astype(f32)).astype(bf16)

        return Scatter("z", own, LZ.at[j], add)

    down = [down_stage(j) for j in range(X)]

    def end_down(j):
        i = at("x", j)
        for h in BOTH:
            a, b = down[j].last(h)
            DS[h, :88] = GD[h, z, i].astype(f32) + a[...].astype(f32) + b[...].astype(f32)
            for yy in range(Y):
                block = DS[h, 22 * yy : 22 * yy + 24, :]
                YS[i * 4 + yy, h] = block.astype(bf16)
                if j == 0:
                    YF[yy, h] = block
        return send_plane(j, lambda k: YS.at[i * 4 + at("y", k)], lambda k: YL.at[j * 4 + k])

    def second_stage(f):
        axis = "yx"[f]

        def add(got, h, k):
            own = F1.at[f, h, at(axis, k)]

            def body(rows):
                got[rows] = (got[rows].astype(f32) + own[rows]).astype(bf16)

            by_rows(body)

        return Scatter(axis, lambda h, k: B1.at[f, h, at(axis, k)], L2.at[f], add)

    second = [second_stage(f) for f in BOTH]

    def end_second(f, h):
        a, b = second[f].last(h)
        own = F1.at[f, h, at("yx"[f], 0)]

        def body(rows):
            F2[f, h, rows] = own[rows] + a[rows].astype(f32) + b[rows].astype(f32)

        by_rows(body)

    def arrive_pair(ring, t, short=False):
        for h, s in SHORT if short else LONG:
            ring.arrive(h, s, t)

    def begin(which, *js):
        for j in js:
            for f in BOTH:
                first[f][j].first(*which)

    def arrive_first(which, *js):
        for j in js:
            for f in BOTH:
                first[f][j].arrive(*which, 1)

    def begin_second(which):
        for f in BOTH:
            second[f].first(*which)

    def arrive_second(which):
        for f in BOTH:
            second[f].arrive(*which, 1)

    def arrive_down(t, short=False):
        for j in order:
            arrive_pair(down[j], t, short)

    gate_long, up_long = LONG
    up_short, gate_short = SHORT
    gate, up = BOTH
    order = (2, 1, 3, 0)
    u2, u1, u3, u0 = order
    begin(gate_long, *order)
    begin(gate_short, *order)
    begin(up_long, *order)
    load_rest()
    for i in range(3):
        loads["down", i].wait()

    def permute(j):
        i = at("x", j)
        rows = GR[:, pl.ds(pl.multiple_of(i * 352, 32), 352), :].reshape(ROWS, 512)
        out = jnp.dot(PF[...], rows, preferred_element_type=f32)
        for zz in range(Z):
            for h in BOTH:
                GD[h, zz, i] = out[88 * zz : 88 * zz + 88, 256 * h : 256 * h + 256].astype(bf16)

    for j in order:
        permute(j)
        down[j].start()
    arrive_first(gate_long, u2, u1, u3)
    arrive_down(1)
    arrive_first(gate_long, u0)
    for h in BOTH:
        DS[h, 88:] = jnp.zeros((8, 256), f32)
    end_first(gate, u2)
    begin_second(gate_long)
    arrive_down(1, True)
    begin(up_short, u2, u1)
    arrive_first(up_long, u2, u1)
    end_first(gate, u1)
    end_first(gate, u3)
    begin_second(gate_short)
    arrive_first(up_long, u3)
    arrive_down(2)
    end_first(gate, u0)
    arrive_second(gate_long)
    arrive_down(2, True)
    begin(up_short, u3, u0)
    end_first(up, u2)
    begin_second(up_long)
    arrive_first(up_long, u0)
    end_first(up, u1)
    begin_second(up_short)
    arrive_down(3)

    far = (4, 3, 5, 2, 6, 1, 7)
    third, third_down = [], {}

    def begin_third(h):
        for f in BOTH:
            end_second(f, h)
        for j in range(4):
            t0, t1 = (F2[f, h, 8 * j : 8 * j + 8, :] for f in BOTH)
            for i, block in enumerate((jnp.concatenate([t0[:4], t1[:4]], 0), jnp.concatenate([t0[4:], t1[4:]], 0))):
                ZF[2 * j + i, h] = block
                ZS[2 * j + i, h] = block.astype(bf16)
        third.append({k: send(ZS.at[at("z", k), h], ZL.at[k, h], "z", k) for k in far})

    begin_third(gate)
    end_first(up, u3)
    arrive_second(up_long)
    third_down.update(end_down(u2))
    end_first(up, u0)
    for j in (u1, u3):
        third_down.update(end_down(j))
    third_down.update(end_down(u0))
    begin_third(up)
    for copy in third_down.values():
        copy.wait_recv()
    real = lax.broadcasted_iota(jnp.int32, (24, 256), 0) < 22
    squares = jnp.zeros((), f32)
    g_down = []
    for h in BOTH:
        total = YF[y, h]
        for k in range(1, 16):
            total = total + YL[k, h].astype(f32)
        total = jnp.where(real, total, 0.0).astype(bf16).astype(f32)
        g_down.append(total)
        squares += jnp.sum(total * total)
    g_wide = []
    for h in BOTH:
        for copy in third[h].values():
            copy.wait_recv()
        total = ZF[z, h]
        for k in third[h]:
            total = total + ZL[k, h].astype(f32)
        total = total.astype(bf16).astype(f32)
        g_wide.append(total)
        squares += jnp.sum(total * total)

    total = jnp.full((1, 128), squares, f32)
    NS[0] = total
    told = {}
    for i in order:
        told.update(send_plane(i, lambda k: NS.at[0], lambda k: NL.at[i * 4 + k]))
    for copy in told.values():
        copy.wait_recv()
    for k in range(1, 16):
        total = total + NL[k]
    NS[1] = total
    told = {k: send(NS.at[1], NL.at[16 + k], "z", k) for k in far}
    for k in reversed(far):
        told[k].wait_recv()
    for k in range(1, 8):
        total = total + NL[16 + k]
    factor = jnp.minimum(1.0, 0.5 * lax.rsqrt(total / COUNT + 1e-30))[0:1, 0:1]

    def adamw(w, m, v, g):
        m = 0.9 * m + 0.1 * g
        v = 0.95 * v + 0.05 * g * g
        return (w - 0.02 * (m * lax.rsqrt(v + 1e-8) + 0.1 * w)).astype(bf16), m, v

    for copy in own_w:
        copy.wait()
    odd = d % 2 == 1
    wide_z = []
    scattered = len(pending)
    for h in BOTH:
        w = [OW[h, i].astype(f32) for i in BOTH]
        w = jnp.concatenate([jnp.where(odd, one[4:], one[:4]) for one in w], 0)
        m, v = (jnp.concatenate([IW[i, h, 0], IW[i, h, 1]], 0) for i in BOTH)
        WZ[z, h], *new = adamw(w, m, v, g_wide[h] * factor)
        wide_z.append({k: send(WZ.at[z, h], WZ.at[z, h], "z", k) for k in far})
        for i, one in enumerate(new):
            for layer in BOTH:
                MW[i, h, layer] = one[4 * layer : 4 * layer + 4]
    g = jnp.concatenate(g_down, 1) * factor
    for h in BOTH:
        DS[h, :24] = jnp.zeros((24, 256), f32)
    pick = lax.broadcasted_iota(jnp.int32, (24, 24), 1) == lax.broadcasted_iota(jnp.int32, (24, 24), 0) + (11 * d - low)
    pick = jnp.where(pick, 1.0, 0.0).astype(bf16)
    for layer in BOTH:
        w = jnp.dot(pick, OWD[layer], preferred_element_type=f32)[:11]
        w, *new = adamw(w, ID[0, :, layer, :], ID[1, :, layer, :], g[11 * layer : 11 * layer + 11])
        for i, one in enumerate(new):
            MD[i, :, layer, :] = one
        for h in BOTH:
            DS[h, 11 * layer : 11 * layer + 11, :] = w[:, 256 * h : 256 * h + 256].astype(f32)
    for h in BOTH:
        YW[x * 4 + y, h] = DS[h, :24].astype(bf16)

    mine = YW.at[x * 4 + y]
    plane = {}
    spread_order = (0, 2, 1, 3)
    for i in spread_order:
        plane.update(send_plane(i, lambda k: mine, lambda k: mine))
    drain(scattered)
    down = [Gather("z", functools.partial(lambda j, h, k: WD.at[h, at("z", k), at("x", j)], j)) for j in range(X)]

    def begin_down(j):
        for k in range(Y):
            if (j, k) != (0, 0):
                plane[-j % 4, k].wait_recv()
        i = at("x", j)
        for h in BOTH:
            for yy in range(Y):
                DS[h, 22 * yy : 22 * yy + 24, :] = YW[i * 4 + yy, h].astype(f32)
            WD[h, z, i] = DS[h, :88].astype(bf16)
        down[j].start()

    def begin_wide(h):
        for copy in wide_z[h].values():
            copy.wait_recv()
        for layer in BOTH:
            rows = slice(4 * layer, 4 * layer + 4)
            for j in range(2):
                parts = [WZ[4 * j + i, h].astype(f32)[rows] for i in range(4)]
                WG[h, layer, x, y, 16 * j : 16 * j + 16, :] = jnp.concatenate(parts, 0).astype(bf16)

    near = [Gather("yx"[f], functools.partial(lambda f, h, k: unit(WG, f, h, 0, k), f)) for f in BOTH]
    wide = [[Gather("xy"[f], functools.partial(lambda f, j, h, k: unit(WG, f, h, k, j), f, j)) for j in range(4)] for f in BOTH]

    def spread(f, h, j):
        for s in WAYS[:: 1 - 2 * h]:
            wide[f][j % 4].push(h, s, 1)

    def arrive_near(h, t, ways=WAYS):
        for s in ways:
            for f in BOTH:
                spread(f, h, near[f].arrive(h, s, t))

    def arrive_wide(j, h, t=1):
        for f in BOTH:
            wide[f][j].arrive(h, WAYS[h], t)

    def both_down(t, *js):
        for j in js:
            arrive_pair(down[j], t)
            arrive_pair(down[j], t, True)

    begin_down(0)
    for h in BOTH:
        begin_wide(h)
        for f in BOTH:
            for s in WAYS[:: 1 - 2 * h]:
                near[f].push(h, s, 1)
        for f in BOTH:
            spread(f, h, 0)
        if h == 0:
            for j in order[:3]:
                begin_down(j)
    arrive_near(0, 1)
    both_down(1, 0)
    arrive_wide(0, 0)
    both_down(1, 2)
    arrive_near(1, 1)
    both_down(1, 1)
    arrive_wide(0, 1)
    both_down(1, 3)
    arrive_near(0, 2, WAYS[:1])
    both_down(2, 0)
    arrive_wide(3, 0)
    both_down(2, 2)
    arrive_wide(1, 0)
    arrive_near(1, 2, WAYS[1:])
    both_down(2, 1)
    arrive_wide(1, 1)
    both_down(2, 3)
    arrive_wide(3, 1)
    early = len(pending)
    for j in spread_order[:2]:
        arrive_pair(down[j], 3)
    for h in BOTH:
        arrive_wide(2, h)
    for j in spread_order[2:]:
        arrive_pair(down[j], 3)
    drain(early)
    loads["back", 0].wait()
    for j in spread_order:
        arrive_pair(down[j], 3, True)
        arrive_pair(down[j], 4)
        i = at("x", j)
        for h in BOTH:
            rows = WD[h, :, i].astype(f32).reshape(ROWS, 256).astype(bf16)
            out = jnp.dot(PB[...], rows, preferred_element_type=f32).astype(bf16)
            for layer in BOTH:
                OD[layer, pl.ds(pl.multiple_of(i * 352, 32), 352), 256 * h : 256 * h + 256] = out[352 * layer : 352 * layer + 352]
    for j in spread_order:
        for f in BOTH:
            arrive_pair(wide[f][j], 1, True)
        for h in BOTH:
            arrive_wide(j, h, 2)
    drain(len(pending))


def finish(W, OD, MW, MD, *rest):
    sem = rest[-1]
    sources = [W.at[0], W.at[1], OD] + [r for i in BOTH for r in (MW.at[i, 0], MW.at[i, 1], MD.at[i])]
    copies = [pltpu.make_async_copy(src, dst, sem.at[i]) for i, (src, dst) in enumerate(zip(sources, rest))]
    for copy in copies:
        copy.start()
    for copy in copies:
        copy.wait()


def step_kernel(*args):
    hbm, vmem = pl.BlockSpec(memory_space=pl.ANY), pl.BlockSpec(memory_space=pltpu.VMEM)
    wide, deep = (2, 4, F), (11, 2, 512)
    unit, half = (4, 32, F), (4, 88, 256)
    pair, square, whole_down = (2, 2), (4, *unit), (2, 8, *half)
    blocks, small = (8, 2, 8, F), (16, 2, 24, 256)
    shape = jax.ShapeDtypeStruct
    out = pl.pallas_call(
        kernel,
        out_shape=(pltpu.VMEM((*pair, *square), bf16), pltpu.VMEM((2, F, 512), bf16), pltpu.VMEM((*pair, *wide), f32), pltpu.VMEM((2, *deep), f32)),
        in_specs=[hbm] * 14,
        out_specs=(vmem,) * 4,
        scratch_shapes=[
            pltpu.VMEM((*pair, *square), bf16),
            pltpu.VMEM((2, F, 512), bf16),
            pltpu.VMEM(whole_down, bf16),
            pltpu.VMEM((2, 4, 6, *unit[1:]), bf16),
            pltpu.VMEM((*pair, *unit), f32),
            pltpu.VMEM((*pair, *unit), bf16),
            pltpu.VMEM((2, 6, *unit[1:]), bf16),
            pltpu.VMEM((*pair, *unit[1:]), f32),
            pltpu.VMEM(blocks, bf16),
            pltpu.VMEM(blocks, f32),
            pltpu.VMEM(blocks, bf16),
            pltpu.VMEM((4, 14, *half[1:]), bf16),
            pltpu.VMEM((2, 96, 256), f32),
            pltpu.VMEM(small, bf16),
            pltpu.VMEM((4, *small[1:]), f32),
            pltpu.VMEM(small, bf16),
            pltpu.VMEM((2, 1, 128), f32),
            pltpu.VMEM((24, 1, 128), f32),
            pltpu.VMEM(whole_down, bf16),
            pltpu.VMEM(blocks, bf16),
            pltpu.VMEM(small, bf16),
            pltpu.VMEM((ROWS, ROWS), bf16),
            pltpu.VMEM((ROWS, ROWS), bf16),
            pltpu.VMEM((*pair, 8, F), bf16),
            pltpu.VMEM((2, 24, 512), bf16),
            pltpu.VMEM((*pair, *wide), f32),
            pltpu.VMEM((2, *deep), f32),
            pltpu.SemaphoreType.DMA((SEMS,)),
            pltpu.SemaphoreType.DMA((SEMS,)),
            pltpu.SemaphoreType.DMA((LOADS,)),
            pltpu.SemaphoreType.DMA((9,)),
        ],
        compiler_params=pltpu.CompilerParams(collective_id=0, has_side_effects=True, vmem_limit_bytes=50 * 2**20),
        name="clipped_step",
    )(*one_hots(), *args)
    out = [pltpu.with_memory_space_constraint(one, pltpu.VMEM) for one in out]
    return pl.pallas_call(
        finish,
        out_shape=(shape((2, *square), bf16),) * 2 + (shape((2, F, 512), bf16),) + (shape(wide, f32), shape(wide, f32), shape(deep, f32)) * 2,
        in_specs=[vmem] * 4,
        out_specs=(hbm,) * 9,
        scratch_shapes=[pltpu.SemaphoreType.DMA((9,))],
        compiler_params=pltpu.CompilerParams(vmem_limit_bytes=50 * 2**20),
        name="finish",
    )(*out)


def solution(mesh):
    def step(gg, gu, gd, wg, wu, wd, mg, mu, md, vg, vu, vd):
        gg, gu = (g.reshape(2, 4, 4, 32, F) for g in (gg, gu))
        md, vd = (a.transpose(1, 0, 2) for a in (md, vd))
        og, ou, od, omg, omu, omd, ovg, ovu, ovd = step_kernel(gg, gu, gd[0], wg, wu, wd, mg, mu, md, vg, vu, vd)
        og, ou = (o.reshape(2, 512, F) for o in (og, ou))
        omd, ovd = (a.transpose(1, 0, 2) for a in (omd, ovd))
        return og, ou, od, omg, omu, omd, ovg, ovu, ovd

    all_of, cut = P(None, None, None), P(None, "dp", None)
    return jax.shard_map(
        step,
        mesh=mesh,
        in_specs=(P(("rep", "dp"), None, None, None),) * 3 + (all_of,) * 3 + (cut,) * 6,
        out_specs=(P("rep", None, None),) * 3 + (P("rep", "dp", None),) * 6,
        check_vma=False,
    )
```
